256 devices in a mesh: grp: 2 (over y), gx: 16 (over z), gy: 4 (over x), gz: 2 (over core).
Axes of the slice: x: 4, y: 2, z: 16, core: 2. Of those that a mesh axis runs over, the one named last changes fastest.
The devices are a block of a 4x16x16 slice.
Arguments:
- observed: float32 [16384, 4, 256], P(('grp', 'gx', 'gy', 'gz')), parts along dimension 0, may hold values from -12 to 12
- predicted: float32 [16384, 4, 256], P(('grp', 'gx', 'gy', 'gz')), parts along dimension 0, may hold values from -6 to 6
- coherence_mask: int32 [16384, 256], P(('grp', 'gx', 'gy', 'gz')), parts along dimension 0, may hold values 0 or 1
- block_count: int32 [16384], P(('grp', 'gx', 'gy', 'gz')), parts along dimension 0, may hold values from 64 to 256
- block_owner: int32 [16384, 1], P(('grp', 'gx', 'gy', 'gz')), parts along dimension 0, may hold values from 0 to 63; in each aligned block of 64 rows (0 to 63, 64 to 127, ...) at most 4 rows name the same one
- block_matrix_choice: int32 [16384], P(('grp', 'gx', 'gy', 'gz')), parts along dimension 0, may hold values from 0 to 31
- block_patch: int32 [16384], P(('grp', 'gx', 'gy', 'gz')), parts along dimension 0, may hold values from 0 to 31
- look_vector: float32 [4, 3], replicated, may hold values from -1 to 1
- interp_weights: bfloat16 [32, 256, 128], replicated, may hold values from -0.375 to 0.375
- depth_kernel: float32 [64], P(('grp', 'gz')), parts along dimension 0, may hold values from 0.2 to 1
- stiffness: float32 [64, 512, 512], P(('grp', 'gz'), 'gx', 'gy'), parts along dimension 0, may hold values from 0.25 to 4
Outputs:
- adjoint_field: float32 [3, 64, 512, 512], P(None, ('grp', 'gz'), 'gx', 'gy'), parts along dimension 1
- cg_residual: float32 [3, 64, 512, 512], P(None, ('grp', 'gz'), 'gx', 'gy'), parts along dimension 1
The draws below stay inside these ranges and needn't reach their ends.
There are 2 independent parts, one for each index of `grp`. The reference program is written for one: setup_inputs(seed, part) draws one part's arguments, and reference() takes and returns one part's arrays. A program takes and returns all parts, laid end to end along the dimension named above; an argument that names none is the same for every part. Nothing has to cross between parts.
Inputs may be any that keep to these rules, and one draw needn't show every extreme that they name: `block_owner`: the blocks of one device name no column tile more than 4 times; in some devices one tile is named exactly 4 times.
All inputs are finite; a program needn't handle non-finite values. No bound on the sum of `coherence_mask` on one device may be relied on, other than what follows from the above.
Results may differ from the reference program's by a relative error of at most 0.0029.
Values sent between devices are 32-bit elements; how exact they have to be, the bound alone decides.
A program may use at most 64 MiB of HBM per device.

```python
import math
import jax
import jax.numpy as jnp
import numpy as np
from jax import lax

CX = 32
CY = 128
BLK_DEV = 64
NTAB = 32
EPOCHS = 4
BPIX = 256
PATCH_X = 8
PATCH_Y = 16
ITERS = 3
NX = 512
NY = 512
NZ = 32
NBLK = 8192
CAP = 4
NPOS = 32
N_GX = 16
N_GY = 4


def draw_observed(key, part):
    rows = jnp.arange(NBLK, dtype=jnp.float32)
    spread = 1.0 + 2.0 * rows / max(NBLK - 1, 1)
    base = jax.random.truncated_normal(key, -4.0, 4.0, (NBLK, EPOCHS, BPIX), jnp.float32)
    return base * spread[:, None, None]


def place_ends(values, own_key, smallest, largest):
    dims = values.shape
    place = [jax.random.randint(jax.random.fold_in(own_key, axis), (), 0, dims[axis]) for axis in range(len(dims))]
    values = values.at[tuple(place)].set(smallest)
    longest = dims.index(max(dims))
    place[longest] = (place[longest] + 1) % dims[longest]
    return values.at[tuple(place)].set(largest)


def level_of(key, dims, split, low, largest):
    def one(dim, blocks):
        steps = jax.random.uniform(jax.random.fold_in(jax.random.fold_in(key, 6), dim), (blocks,), jnp.float32, low / len(split), largest / len(split))
        return jnp.repeat(jnp.exp(steps), dims[dim] // blocks).reshape((-1,) + (1,) * (len(dims) - dim - 1))

    level = one(*split[0])
    for cut in split[1:]:
        level = level * one(*cut)
    return level


def routed_block(rng, own, number, rows, number_of, top, reach, lean):
    ranking = jax.random.permutation(rng, number_of)
    heavy_load, ordinary = load_shares(number_of, rows * top, reach, lean, True), load_shares(number_of, rows * top, reach, lean, False)
    places = jnp.arange(number_of)

    def named(sizes, offset_by):
        used = int((sizes > 0).sum())
        fixed = max(1, used // 4)
        moved = fixed + (places - fixed + offset_by * (used - fixed)) % max(1, number_of - fixed)
        return jnp.zeros((number_of,), jnp.int32).at[ranking[jnp.where(places < fixed, places, moved)]].set(jnp.asarray(sizes, jnp.int32))

    sizes = jnp.where(number % 4 == 0, named(heavy_load, number // 4), named(ordinary, number - number // 4 - 1))
    mixed = jax.random.permutation(jax.random.fold_in(own, 3), number_of)
    giver, receiver = mixed[0:number_of // 2 * 2:2], mixed[1:number_of // 2 * 2:2]
    room = jnp.minimum(sizes[giver] - 1, reach - sizes[receiver]) // 2
    room = jnp.where((giver == ranking[0]) | (receiver == ranking[0]) | (sizes[receiver] == 0), 0, jnp.maximum(room, 0))
    moved = jax.random.randint(jax.random.fold_in(own, 4), (number_of // 2,), 0, 1 << 20) % (room + 1)
    sizes = sizes.at[giver].add(-moved).at[receiver].add(moved)
    members = jnp.searchsorted(jnp.cumsum(sizes), jnp.arange(rows * top), side="right").astype(jnp.int32)
    table = members.reshape(top, rows).T
    table = table[jax.random.permutation(jax.random.fold_in(own, 1), rows)]
    offset_by = jax.random.randint(jax.random.fold_in(own, 2), (rows, 1), 0, top)
    return jnp.take_along_axis(table, (jnp.arange(top)[None, :] + offset_by) % top, axis=1)


def load_shares(amount, total, bound, lean, full):
    portions = [(1 << 20) // math.isqrt(grade ** lean) + 1 for grade in range(1, amount + 1)]
    largest = bound if full else min(bound, max(-(-total // amount), total * portions[0] // sum(portions)))
    least = 1 if total - largest >= amount - 1 else 0
    counts, surplus = [largest] + [least] * (amount - 1), total - largest - least * (amount - 1)
    while surplus > 0:
        movable = [i for i in range(1, amount) if counts[i] < largest] or [i for i in range(1, amount) if counts[i] < bound]
        pool, budget = sum([portions[i] for i in movable]), surplus
        for i in movable:
            extra = min(bound - counts[i], max(1, budget * portions[i] // pool), surplus)
            counts[i] = counts[i] + extra
            surplus = surplus - extra
    return np.array(counts)


def noise(key, dims, deviation, bound, split=(), kind=jnp.bfloat16):
    level = level_of(key, dims, split, -0.22, 0.18) if split else 1.0
    drawn = jax.random.normal(key, dims, jnp.float32) * deviation * level
    return jnp.minimum(jnp.maximum(drawn, -bound), bound).astype(kind)


def setup_inputs(seed: int = 0, part: int = 0) -> dict:
    splits = jax.random.split(jax.random.key(seed), 12)
    part_splits = jax.random.split(jax.random.fold_in(splits[11], part), 12)
    observed = draw_observed(jax.random.fold_in(jax.random.fold_in(splits[11], part), 71), part)
    predicted = noise(part_splits[1], (NBLK, EPOCHS, BPIX), 1.0, 6.0, ((0, 128),), jnp.float32)
    coherence_mask = place_ends((jax.random.randint(part_splits[2], (NBLK, BPIX), 0, 4) < 3).astype(jnp.int32), jax.random.fold_in(part_splits[2], 1), 0, 1)
    block_count = place_ends(jax.random.randint(part_splits[3], (NBLK,), BPIX // 4, BPIX + 1), jax.random.fold_in(part_splits[3], 1), BPIX // 4, BPIX).astype(jnp.int32)
    block_owner_keys = jax.random.split(jax.random.fold_in(part_splits[4], 1), NBLK // BLK_DEV)
    block_owner_turns = jax.random.permutation(jax.random.fold_in(part_splits[4], 3), NBLK // BLK_DEV)
    block_owner = jax.vmap(lambda own, number: routed_block(jax.random.fold_in(part_splits[4], 2), own, number, BLK_DEV, N_GX * N_GY, 1, CAP, 2))(block_owner_keys, block_owner_turns).reshape((NBLK, 1))
    block_matrix_choice = place_ends(jax.random.randint(part_splits[5], (NBLK,), 0, NTAB), jax.random.fold_in(part_splits[5], 1), 0, NTAB - 1).astype(jnp.int32)
    block_patch = place_ends(jax.random.randint(part_splits[6], (NBLK,), 0, NPOS), jax.random.fold_in(part_splits[6], 1), 0, NPOS - 1).astype(jnp.int32)
    look_vector = jnp.clip(jax.random.uniform(splits[7], (EPOCHS, 3), jnp.float32, -1.0, 1.0), -1.0, 1.0)
    interp_weights = noise(splits[8], (NTAB, BPIX, PATCH_X * PATCH_Y), BPIX ** -0.5, 0.375)
    depth_kernel = jnp.clip(jnp.exp(math.log(1.0) - 1.609438 * jax.random.uniform(part_splits[9], (NZ,), jnp.float32) ** level_of(part_splits[9], (NZ,), ((0, 2),), -0.2, 0.2)), 0.2, 1.0)
    stiffness = jnp.clip(jnp.exp(math.log(4.0) - 2.7725887 * jax.random.uniform(part_splits[10], (NZ, NX, NY), jnp.float32) ** level_of(part_splits[10], (NZ, NX, NY), ((0, 2), (1, 16), (2, 4)), -0.2, 0.2)), 0.25, 4.0)
    return dict(observed=observed, predicted=predicted, coherence_mask=coherence_mask, block_count=block_count, block_owner=block_owner, block_matrix_choice=block_matrix_choice, block_patch=block_patch, look_vector=look_vector, interp_weights=interp_weights, depth_kernel=depth_kernel, stiffness=stiffness)


KAPPA = 0.5
EPS = 1e-06
SPATIAL = (1, 2, 0)

def beside_all(padded):
    total = padded[2:, 1:-1, 1:-1] + padded[:-2, 1:-1, 1:-1]
    total = total + padded[1:-1, 2:, 1:-1] + padded[1:-1, :-2, 1:-1]
    return total + padded[1:-1, 1:-1, 2:] + padded[1:-1, 1:-1, :-2]

def central(padded, axis):
    if axis == 0:
        return 0.5 * (padded[2:, 1:-1, 1:-1] - padded[:-2, 1:-1, 1:-1])
    if axis == 1:
        return 0.5 * (padded[1:-1, 2:, 1:-1] - padded[1:-1, :-2, 1:-1])
    return 0.5 * (padded[1:-1, 1:-1, 2:] - padded[1:-1, 1:-1, :-2])

def operate(field, stiffness):
    padded = jnp.pad(field, ((0, 0), (1, 1), (1, 1), (1, 1)))
    spread = central(padded[0], SPATIAL[0]) + central(padded[1], SPATIAL[1]) + central(padded[2], SPATIAL[2])
    spread_pad = jnp.pad(spread, 1)
    parts = [(6.0 + stiffness) * field[member] - beside_all(padded[member]) - KAPPA * central(spread_pad, SPATIAL[member]) for member in range(3)]
    return jnp.stack(parts)

def project(resid, look_vector):
    return jnp.einsum('ec,nep->ncp', look_vector, resid, precision=lax.Precision.HIGHEST).astype(jnp.bfloat16)

def contribute(coeffs, tables, weights):
    total = coeffs.shape[0]
    group = math.gcd(total, 64)
    coefficient_sets = coeffs.reshape(total // group, group, 3, coeffs.shape[2])
    table_groups = tables.reshape(total // group, group)

    def per_group(both_parts):
        block_coefficient_values, block_tables = both_parts
        selected_entries = jnp.take(weights, block_tables, axis=0).astype(jnp.float32)
        return jnp.einsum('aow,awv->aov', block_coefficient_values.astype(jnp.float32), selected_entries, precision=lax.Precision.HIGHEST)
    result = lax.map(per_group, (coefficient_sets, table_groups))
    return result.reshape(total, 3, weights.shape[2])

def reference(observed, predicted, coherence_mask, block_count, block_owner, block_matrix_choice, block_patch, look_vector, interp_weights, depth_kernel, stiffness):
    column = jnp.arange(BPIX, dtype=jnp.int32)
    valid = coherence_mask.astype(jnp.float32) * (column[None, :] < block_count[:, None]).astype(jnp.float32)
    resid = (predicted - observed) * valid[:, None, :]
    scale = lax.rsqrt(jnp.sum(resid * resid) / (EPOCHS * jnp.sum(valid)) + EPS)
    coeffs = project(resid, look_vector)
    sums = contribute(coeffs, block_matrix_choice, interp_weights)
    owner = block_owner[:, 0]
    tile_y = CY // PATCH_Y
    grid_x = owner // N_GY * (CX // PATCH_X) + block_patch // tile_y
    northing_grid = owner % N_GY * tile_y + block_patch % tile_y
    across_x = NX // PATCH_X
    across_y = NY // PATCH_Y
    placed = jax.ops.segment_sum(sums, (grid_x * across_y + northing_grid).astype(jnp.int32), num_segments=across_x * across_y)
    surface = placed.reshape(across_x, across_y, 3, PATCH_X, PATCH_Y).transpose(2, 0, 3, 1, 4).reshape(3, NX, NY)
    source = scale * depth_kernel[None, :, None, None] * surface[:, None, :, :]
    adjoint_field = jnp.zeros_like(source)
    cg_residual = source
    direction = source
    norm_now = jnp.sum(cg_residual * cg_residual)
    for step in range(ITERS):
        image = operate(direction, stiffness)
        alpha = norm_now / jnp.sum(direction * image)
        adjoint_field = adjoint_field + alpha * direction
        cg_residual = cg_residual - alpha * image
        norm_next = jnp.sum(cg_residual * cg_residual)
        direction = cg_residual + norm_next / norm_now * direction
        norm_now = norm_next
    return (adjoint_field, cg_residual)
```

```python
import jax
import jax.numpy as jnp
from jax import lax
from jax.experimental import pallas as pl
from jax.experimental.pallas import tpu as pltpu
from jax.sharding import PartitionSpec as P

EPOCHS = 4
PATCH_X = 8
PATCH_Y = 16
CAP = 4
EPS = 1e-06

SHIFT = 8.0
PRE = 1024.0
MOMENTS = 6

HIGHEST = lax.Precision.HIGHEST
F32 = jnp.float32


def roll(values, shift, axis):
    return pltpu.roll(values, shift % values.shape[axis], axis)


def ahead(values, axis):
    return roll(values, -1, axis)


def behind(values, axis):
    return roll(values, 1, axis)


def iota(shape, axis):
    return lax.broadcasted_iota(jnp.int32, shape, axis)


def product(first, second, moments):
    total = None
    for i, f in enumerate(first):
        for j, g in enumerate(second):
            term = f * g * moments[i + j]
            total = term if total is None else total + term
    return total


def combined(first, factor, second):
    size = max(len(first), len(second))
    out = []
    for i in range(size):
        value = first[i] if i < len(first) else None
        if i < len(second):
            term = factor * second[i]
            value = term if value is None else value + term
        out.append(value)
    return out


def applied(poly):
    out = []
    for i in range(len(poly) + 1):
        value = None
        for j in (i, i - 1):
            if 0 <= j < len(poly):
                value = poly[j] if value is None else value + poly[j]
        out.append(SHIFT * value)
    return out


def conjugate(moments):
    one = jnp.ones_like(moments[0])
    residual, direction, iterate = [one], [one], []
    now = moments[0]
    for step in range(3):
        image = applied(direction)
        alpha = now / product(direction, image, moments)
        scaled = [alpha * d for d in direction]
        iterate = scaled if not iterate else combined(iterate, one, scaled)
        residual = combined(residual, -alpha, image)
        if step < 2:
            new = product(residual, residual, moments)
            direction = combined(residual, new / now, direction)
            now = new
    return iterate, residual


def kernel(
    slots_ref, choice_ref, part_ref, depth_ref, stiff_ref,
    adj_ref, res_ref,
    got_slots, got_choice, flat_slots, flat_choice,
    surf, surf_other, halo_x, halo_y,
    stiff_x, wide_stiff, strip_out, strip_in, coef,
    depths, table,
    fields, w1, w2, div,
    row_out, row_in, ring_in,
    send_a2a, recv_a2a, send_sem, recv_sem,
):
    gx, gy, gz = lax.axis_index("gx"), lax.axis_index("gy"), lax.axis_index("gz")
    ngx, ngy = lax.axis_size("gx"), lax.axis_size("gy")
    owners = ngx * ngy
    me = gx * ngy + gy
    nz, nx, ny = stiff_ref.shape
    other = 1 - gz
    rows, lanes = nx + 8, 2 * ny
    tall = nx + 16

    def at(x, y, z):
        return {"gx": x, "gy": y, "gz": z}

    def wrap(value, count):
        return lax.rem(value + count, count)

    depths[...] = jnp.zeros(depths.shape, F32)
    depths[pl.ds(pl.multiple_of(8 + nz * gz, 8), nz), :] = depth_ref[...]

    barrier = pltpu.get_barrier_semaphore()

    def greet(k, carry):
        o = lax.rem(me + k, owners)
        pl.semaphore_signal(barrier, inc=1, device_id=at(o // ngy, lax.rem(o, ngy), gz))
        return carry

    lax.fori_loop(1, owners, greet, 0)
    for k in range(ngy):
        pl.semaphore_signal(barrier, inc=1, device_id=at(gx, wrap(gy + k, ngy), other))

    def domain(count):
        r, c = iota((count, lanes), 0), iota((count, lanes), 1)
        half = (count - nx) // 2
        in_x = (r < nx) | ((r < nx + half) & (gx < ngx - 1)) | ((r >= nx + half) & (gx > 0))
        in_y = (c < ny) | ((c < ny + ny // 2) & (gy < ngy - 1)) | ((c >= ny + ny // 2) & (gy > 0))
        return (in_x & in_y).astype(F32)

    zero_plane = jnp.zeros((rows, lanes), F32)
    for edge in (0, 2 * nz + 1):
        div[edge] = zero_plane
        for c in range(3):
            w1[c, edge] = zero_plane
            w2[c, edge] = zero_plane
    pl.semaphore_wait(barrier, owners - 1 + ngy)

    def remote(source, target, index, device):
        return pltpu.make_async_remote_copy(
            src_ref=source, dst_ref=target, send_sem=send_sem.at[index], recv_sem=recv_sem.at[index],
            device_id=device, device_id_type=pl.DeviceIdType.MESH,
        )

    x_up, x_down = wrap(gx + 1, ngx), wrap(gx - 1, ngx)
    y_up, y_down = wrap(gy + 1, ngy), wrap(gy - 1, ngy)
    own_depth = depth_ref
    early = [
        remote(stiff_ref.at[:, pl.ds(0, 8), :], stiff_x.at[0], 0, at(x_down, gy, gz)),
        remote(stiff_ref.at[:, pl.ds(nx - 8, 8), :], stiff_x.at[1], 1, at(x_up, gy, gz)),
        remote(own_depth, depths.at[pl.ds(pl.multiple_of(8 + nz * gz, 8), nz), :], 2, at(gx, gy, other)),
    ]
    for copy in early:
        copy.start()

    def post(k, carry):
        o = lax.rem(me + k, owners)
        device = at(o // ngy, lax.rem(o, ngy), gz)
        pltpu.make_async_remote_copy(
            src_ref=slots_ref.at[o], dst_ref=got_slots.at[me], send_sem=send_a2a.at[0], recv_sem=recv_a2a.at[0],
            device_id=device, device_id_type=pl.DeviceIdType.MESH,
        ).start()
        pltpu.make_async_remote_copy(
            src_ref=choice_ref.at[o], dst_ref=got_choice.at[me], send_sem=send_a2a.at[1], recv_sem=recv_a2a.at[1],
            device_id=device, device_id_type=pl.DeviceIdType.MESH,
        ).start()
        return carry

    lax.fori_loop(1, owners, post, 0)
    got_slots[me] = slots_ref[me]
    got_choice[me] = choice_ref[me]

    for copy in early:
        copy.wait()
    low = iota((8, ny), 0) < 4
    for z in range(nz):
        wide_stiff[z, 0:nx, :] = stiff_ref[z]
        wide_stiff[z, nx:rows, :] = jnp.where(low, stiff_x[0, z], stiff_x[1, z])
    turned = wide_stiff[...].reshape(nz * rows, ny).T
    strip_out[0] = turned[0:8]
    strip_out[1] = turned[ny - 8:ny]
    strips = [
        remote(strip_out.at[0], strip_in.at[0], 3, at(gx, y_down, gz)),
        remote(strip_out.at[1], strip_in.at[1], 4, at(gx, y_up, gz)),
    ]
    for copy in strips:
        copy.start()

    d = depths[...]
    where_z = iota(d.shape, 0)
    inside = ((where_z >= 8) & (where_z < 8 + 2 * nz)).astype(F32)
    d_up, d_down = ahead(d, 0), behind(d, 0)
    q = 0.5 * (d_up - d_down)
    kept_d, kept_q = inside * d, inside * q
    columns = (
        d,
        0.125 * (d_up + d_down),
        q,
        (1.0 / 32.0) * (ahead(kept_d, 0) - behind(kept_d, 0)),
        (1.0 / 32.0) * (ahead(kept_q, 0) - behind(kept_q, 0)),
    )
    for k, values in enumerate(columns):
        for z in range(2 * nz):
            table[k, z] = values[z + 8:z + 9]

    for copy in strips:
        copy.wait()
    filler = jnp.zeros((ny - 16, nz * rows), F32)
    beside = jnp.concatenate([strip_in[0], filler, strip_in[1]], axis=0).T.reshape(nz, rows, ny)
    base = nz * gz
    for z in range(nz):
        coef[base + z, :, 0:ny] = 0.125 * wide_stiff[z] - 0.25
        coef[base + z, :, ny:lanes] = 0.125 * beside[z] - 0.25
    passed = pl.ds((nz - 4) + 4 * gz, 4)
    layers = remote(coef.at[passed], coef.at[passed], 5, at(gx, gy, other))
    layers.start()

    for message, buffer in enumerate((slots_ref, choice_ref)):
        part = buffer.at[pl.ds(0, owners - 1)]
        pltpu.make_async_copy(part, part, send_a2a.at[message]).wait()
    for message, buffer in enumerate((got_slots, got_choice)):
        part = buffer.at[pl.ds(0, owners - 1)]
        pltpu.make_async_copy(part, part, recv_a2a.at[message]).wait()
    own_slot = iota((CAP, ny), 1) // (ny // CAP) == iota((CAP, ny), 0)
    for o in range(owners):
        for c in range(3):
            flat_slots[c, CAP * o:CAP * (o + 1), :] = got_slots[o, c]
        flat_choice[CAP * o:CAP * (o + 1), :] = jnp.where(own_slot, got_choice[o], 0.0)
    picked = flat_choice[...]
    tiles = []
    for c in range(3):
        spread = lax.dot_general(
            picked, flat_slots[c], (((0,), (0,)), ((), ())), precision=HIGHEST, preferred_element_type=F32
        )
        depth_places = ny // CAP
        placed = spread[0:depth_places]
        for j in range(1, CAP):
            placed = placed + spread[j * depth_places:(j + 1) * depth_places]
        tiles.append(placed)
    tile = jnp.concatenate(tiles, axis=0)
    sub = lax.rem(iota(tile.shape, 0), 8)
    chunk = iota(tile.shape, 1) // PATCH_Y
    for bit in (1, 2, 4):
        row_set, chunk_set = (sub // bit) % 2 == 1, (chunk // bit) % 2 == 1
        from_below = roll(roll(tile, -bit, 0), bit * PATCH_Y, 1)
        from_above = roll(roll(tile, bit, 0), -bit * PATCH_Y, 1)
        tile = jnp.where(row_set == chunk_set, tile, jnp.where(row_set, from_above, from_below))
    surf[0] = tile.reshape(3, nx, ny)
    swap = remote(surf.at[0], surf_other, 6, at(gx, gy, other))
    swap.start()
    swap.wait()
    surf[1] = surf[0] + surf_other[...]

    first, last = pl.ds(0, 8), pl.ds(nx - 8, 8)
    whole = surf.at[1]
    halos = [
        remote(whole.at[:, first, :], halo_x.at[0], 7, at(x_down, gy, gz)),
        remote(whole.at[:, last, :], halo_x.at[1], 8, at(x_up, gy, gz)),
        remote(whole.at[:, first, :], halo_x.at[2], 9, at(x_down, y_down, gz)),
        remote(whole.at[:, first, :], halo_x.at[3], 10, at(x_down, y_up, gz)),
        remote(whole.at[:, last, :], halo_x.at[4], 11, at(x_up, y_down, gz)),
        remote(whole.at[:, last, :], halo_x.at[5], 12, at(x_up, y_up, gz)),
        remote(whole, halo_y.at[0], 13, at(gx, y_down, gz)),
        remote(whole, halo_y.at[1], 14, at(gx, y_up, gz)),
    ]
    for copy in halos:
        copy.start()
    for copy in halos:
        copy.wait()
    mask_tall = domain(tall)
    mask = domain(rows)
    left = iota((1, ny), 1) < ny // 2
    low_rows = iota((8, lanes), 0) < 4

    def packed(values):
        return jnp.concatenate(
            [values[0:nx], jnp.where(low_rows, values[nx:nx + 8], values[nx + 8:nx + 16])], axis=0
        )

    around = []
    for c in range(3):
        main = jnp.concatenate([surf[1, c], halo_x[0, c], halo_x[1, c]], axis=0)
        side = jnp.concatenate(
            [
                jnp.where(left, halo_y[0, c], halo_y[1, c]),
                jnp.where(left, halo_x[2, c], halo_x[3, c]),
                jnp.where(left, halo_x[4, c], halo_x[5, c]),
            ],
            axis=0,
        )
        around.append(mask_tall * jnp.concatenate([main, side], axis=1))
    flux = mask_tall * (
        0.5 * ((ahead(around[0], 0) - behind(around[0], 0)) + (ahead(around[1], 1) - behind(around[1], 1)))
    )
    for c in range(3):
        s = around[c]
        beside_xy = (ahead(s, 0) + behind(s, 0)) + (ahead(s, 1) + behind(s, 1))
        fields[c] = packed(s)
        if c < 2:
            drop = 0.125 * beside_xy + (1.0 / 32.0) * (ahead(flux, c) - behind(flux, c))
            fields[3 + c] = mask * packed(drop)
            fields[6 + c] = mask * packed((1.0 / 32.0) * (ahead(around[2], c) - behind(around[2], c)))
        else:
            fields[3 + c] = mask * packed(0.125 * beside_xy)
    fields[8] = packed(flux)

    layers.wait()

    def first_layer(i, carry):
        z = (nz - 4) * gz + i
        value = [table[k, z] for k in range(5)]
        own = coef[z] * value[0] - value[1]
        for c in range(2):
            w1[c, z + 1] = mask * (fields[c] * own) - value[0] * fields[3 + c] - value[2] * fields[6 + c]
        w1[2, z + 1] = mask * (fields[2] * (own - value[4])) - value[0] * fields[5] - value[3] * fields[8]
        return carry

    lax.fori_loop(0, nz + 4, first_layer, 0)

    def spread_of(source, start, amount):
        def layer(i, carry):
            z = start + i
            x, y = source[0, z + 1], source[1, z + 1]
            div[z + 1] = mask * (
                ((ahead(x, 0) - behind(x, 0)) + (ahead(y, 1) - behind(y, 1)))
                + (source[2, z + 2] - source[2, z])
            )
            return carry

        lax.fori_loop(0, amount, layer, 0)

    spread_of(w1, (nz - 3) * gz, nz + 3)

    def second_layer(i, carry):
        z = (nz - 2) * gz + i
        own = coef[z]
        here = div[z + 1]
        for c in range(3):
            v = w1[c, z + 1]
            total = (ahead(v, 0) + behind(v, 0)) + (ahead(v, 1) + behind(v, 1))
            total = total + (w1[c, z + 2] + w1[c, z])
            slope = (ahead(here, c) - behind(here, c)) if c < 2 else (div[z + 2] - div[z])
            w2[c, z + 1] = mask * (own * v - 0.125 * total - (1.0 / 64.0) * slope)
        return carry

    lax.fori_loop(0, nz + 2, second_layer, 0)

    spread_of(w2, (nz - 1) * gz, nz + 1)

    def folded(values):
        total = values[0:8]
        for k in range(8, nx, 8):
            total = total + values[k:k + 8]
        return total

    def third_layer(i, sums):
        z = nz * gz + i
        own = coef[z, 0:nx, 0:ny]
        here_x, here_y = div[z + 1, :, 0:ny], div[z + 1, 0:nx, :]
        d_now = table[0, z, :, 0:ny]
        sums = list(sums)
        for c in range(3):
            v = w2[c, z + 1, 0:nx, 0:ny]
            vx, vy = w2[c, z + 1, :, 0:ny], w2[c, z + 1, 0:nx, :]
            total = (ahead(vx, 0) + behind(vx, 0))[0:nx] + (ahead(vy, 1) + behind(vy, 1))[:, 0:ny]
            total = total + (w2[c, z + 2, 0:nx, 0:ny] + w2[c, z, 0:nx, 0:ny])
            if c == 0:
                slope = (ahead(here_x, 0) - behind(here_x, 0))[0:nx]
            elif c == 1:
                slope = (ahead(here_y, 1) - behind(here_y, 1))[:, 0:ny]
            else:
                slope = div[z + 2, 0:nx, 0:ny] - div[z, 0:nx, 0:ny]
            third = own * v - 0.125 * total - (1.0 / 64.0) * slope
            res_ref[c, i] = third
            zeroth = d_now * fields[c, 0:nx, 0:ny]
            one = w1[c, z + 1, 0:nx, 0:ny]
            for k, term in enumerate(
                (zeroth * zeroth, zeroth * one, one * one, one * v, v * v, v * third)
            ):
                sums[k] = sums[k] + folded(term)
        return tuple(sums)

    sums = lax.fori_loop(0, nz, third_layer, tuple(jnp.zeros((8, ny), F32) for _ in range(MOMENTS)))

    lane = iota((1, ny), 1)
    message = part_ref[...]
    for k in range(MOMENTS):
        amount = jnp.sum(jnp.sum(sums[k], axis=0, keepdims=True), axis=1, keepdims=True)
        message = message + jnp.where(lane == k, amount, 0.0)
    row_out[0] = message
    slot = gy * 2 + gz
    row_in[slot] = message
    copies = []
    for k in range(1, ngy):
        copies.append((wrap(gy + k, ngy), gz))
    for k in range(ngy):
        copies.append((wrap(gy + k, ngy), other))
    started = []
    for k, (y, z) in enumerate(copies):
        copy = remote(row_out.at[0], row_in.at[slot], 15 + k, at(gx, y, z))
        copy.start()
        started.append(copy)
    for copy in started:
        copy.wait()
    message = row_in[0]
    for k in range(1, 2 * ngy):
        message = message + row_in[k]
    row_out[1] = message
    ring_in[gx] = message
    first_index = 15 + len(copies)
    started = []
    for k in range(1, ngx):
        copy = remote(row_out.at[1], ring_in.at[gx], first_index + k - 1, at(wrap(gx + k, ngx), gy, gz))
        copy.start()
        started.append(copy)
    for copy in started:
        copy.wait()
    message = ring_in[0]
    for k in range(1, ngx):
        message = message + ring_in[k]
    parts = [jnp.sum(jnp.where(lane == k, message, 0.0), axis=1, keepdims=True) for k in range(MOMENTS + 2)]

    scale = lax.rsqrt(parts[MOMENTS] / (EPOCHS * parts[MOMENTS + 1]) + EPS) * (1.0 / PRE)
    iterate, residual = conjugate(parts[0:MOMENTS])
    iterate = [scale * value for value in iterate]
    residual = [scale * value for value in residual]

    def finish(i, carry):
        z = nz * gz + i
        d_now = table[0, z, :, 0:ny]
        for c in range(3):
            zeroth = d_now * fields[c, 0:nx, 0:ny]
            one, two = w1[c, z + 1, 0:nx, 0:ny], w2[c, z + 1, 0:nx, 0:ny]
            third = res_ref[c, i]
            adj_ref[c, i] = iterate[0] * zeroth + iterate[1] * one + iterate[2] * two
            res_ref[c, i] = residual[0] * zeroth + residual[1] * one + residual[2] * two + residual[3] * third
        return carry

    lax.fori_loop(0, nz, finish, 0)


def project(resid, look_vector):
    return jnp.einsum("ec,nep->ncp", look_vector, resid, precision=HIGHEST).astype(jnp.bfloat16)


def per_device(
    observed,
    predicted,
    coherence_mask,
    block_count,
    block_owner,
    block_matrix_choice,
    block_patch,
    look_vector,
    interp_weights,
    depth_kernel,
    stiffness,
):
    blocks, _, pixels = observed.shape
    cells = PATCH_X * PATCH_Y
    ngx, ngy = lax.axis_size("gx"), lax.axis_size("gy")
    owners = ngx * ngy
    nz, nx, ny = stiffness.shape
    places = (nx // PATCH_X) * (ny // PATCH_Y)

    column = lax.broadcasted_iota(jnp.int32, (blocks, pixels), 1)
    valid = coherence_mask.astype(F32) * (column < block_count[:, None]).astype(F32)
    resid = (predicted - observed) * valid[:, None, :]
    lane = jnp.arange(ny)
    part = jnp.where(lane == MOMENTS, jnp.sum(resid * resid), 0.0) + jnp.where(
        lane == MOMENTS + 1, jnp.sum(valid), 0.0
    )

    owner = block_owner[:, 0]
    order = lax.broadcasted_iota(jnp.int32, (blocks, blocks), 0)
    before = lax.broadcasted_iota(jnp.int32, (blocks, blocks), 1)
    earlier = (owner[:, None] == owner[None, :]) & (before < order)
    rank = jnp.sum(earlier.astype(jnp.int32), axis=1)
    slot = owner * CAP + rank
    select = (lax.broadcasted_iota(jnp.int32, (blocks, owners * CAP), 1) == slot[:, None]).astype(F32)
    at_owner = (lax.broadcasted_iota(jnp.int32, (blocks, owners), 1) == owner[:, None]).astype(F32)
    at_lane = (lax.broadcasted_iota(jnp.int32, (blocks, CAP * places), 1) == (rank * places + block_patch)[:, None])
    choice = jnp.einsum("bo,bl->ol", at_owner, at_lane.astype(F32))

    coeffs = project(resid, look_vector)
    picked = jnp.take(interp_weights, block_matrix_choice, axis=0)
    sums = jnp.einsum("aow,awv->aov", coeffs, picked, preferred_element_type=F32)
    slots = jnp.einsum(
        "bos,bcp->ocsp", select.reshape(blocks, owners, CAP), sums, precision=HIGHEST
    )

    depth = jnp.broadcast_to((PRE * depth_kernel)[:, None], (nz, 2 * ny))
    rows, lanes = nx + 8, 2 * ny
    out = jax.ShapeDtypeStruct((3, nz, nx, ny), F32)
    vmem = pl.BlockSpec(memory_space=pltpu.VMEM)
    copies = 15 + (2 * ngy - 1) + (ngx - 1)
    return pl.pallas_call(
        kernel,
        out_shape=(out, out),
        in_specs=[vmem] * 5,
        out_specs=(vmem, vmem),
        scratch_shapes=[
            pltpu.VMEM((owners, 3, CAP, cells), F32),
            pltpu.VMEM((owners, 1, cells), F32),
            pltpu.VMEM((3, owners * CAP, cells), F32),
            pltpu.VMEM((owners * CAP, cells), F32),
            pltpu.VMEM((2, 3, nx, ny), F32),
            pltpu.VMEM((3, nx, ny), F32),
            pltpu.VMEM((6, 3, 8, ny), F32),
            pltpu.VMEM((2, 3, nx, ny), F32),
            pltpu.VMEM((2, nz, 8, ny), F32),
            pltpu.VMEM((nz, rows, ny), F32),
            pltpu.VMEM((2, 8, nz * rows), F32),
            pltpu.VMEM((2, 8, nz * rows), F32),
            pltpu.VMEM((2 * nz, rows, lanes), F32),
            pltpu.VMEM((2 * nz + 16, lanes), F32),
            pltpu.VMEM((5, 2 * nz, 1, lanes), F32),
            pltpu.VMEM((9, rows, lanes), F32),
            pltpu.VMEM((3, 2 * nz + 2, rows, lanes), F32),
            pltpu.VMEM((3, 2 * nz + 2, rows, lanes), F32),
            pltpu.VMEM((2 * nz + 2, rows, lanes), F32),
            pltpu.VMEM((2, 1, ny), F32),
            pltpu.VMEM((2 * ngy, 1, ny), F32),
            pltpu.VMEM((ngx, 1, ny), F32),
            pltpu.SemaphoreType.DMA((2,)),
            pltpu.SemaphoreType.DMA((2,)),
            pltpu.SemaphoreType.DMA((copies,)),
            pltpu.SemaphoreType.DMA((copies,)),
        ],
        compiler_params=pltpu.CompilerParams(
            collective_id=0, has_side_effects=True, vmem_limit_bytes=48 * 1024 * 1024
        ),
    )(slots, choice[:, None, :], part[None, :], depth, stiffness)


def solution(mesh):
    in_specs = (
        P(("grp", "gx", "gy", "gz"), None, None),
        P(("grp", "gx", "gy", "gz"), None, None),
        P(("grp", "gx", "gy", "gz"), None),
        P(("grp", "gx", "gy", "gz")),
        P(("grp", "gx", "gy", "gz"), None),
        P(("grp", "gx", "gy", "gz")),
        P(("grp", "gx", "gy", "gz")),
        P(),
        P(),
        P(("grp", "gz")),
        P(("grp", "gz"), "gx", "gy"),
    )
    out_specs = (P(None, ("grp", "gz"), "gx", "gy"), P(None, ("grp", "gz"), "gx", "gy"))
    return jax.shard_map(
        per_device, mesh=mesh, in_specs=in_specs, out_specs=out_specs, check_vma=False
    )
```

```python
import jax
import jax.numpy as jnp
from jax import lax
from jax.experimental import pallas as pl
from jax.experimental.pallas import tpu as pltpu
from jax.sharding import PartitionSpec as P

EPOCHS = 4
PATCH_X = 8
PATCH_Y = 16
CAP = 4
EPS = 1e-06

SHIFT = 8.0
PRE = 1024.0
MOMENTS = 6

HIGHEST = lax.Precision.HIGHEST
F32 = jnp.float32


def roll(values, shift, axis):
    return pltpu.roll(values, shift % values.shape[axis], axis)


def ahead(values, axis):
    return roll(values, -1, axis)


def behind(values, axis):
    return roll(values, 1, axis)


def iota(shape, axis):
    return lax.broadcasted_iota(jnp.int32, shape, axis)


def product(first, second, moments):
    total = None
    for i, f in enumerate(first):
        for j, g in enumerate(second):
            term = f * g * moments[i + j]
            total = term if total is None else total + term
    return total


def combined(first, factor, second):
    size = max(len(first), len(second))
    out = []
    for i in range(size):
        value = first[i] if i < len(first) else None
        if i < len(second):
            term = factor * second[i]
            value = term if value is None else value + term
        out.append(value)
    return out


def applied(poly):
    out = []
    for i in range(len(poly) + 1):
        value = None
        for j in (i, i - 1):
            if 0 <= j < len(poly):
                value = poly[j] if value is None else value + poly[j]
        out.append(SHIFT * value)
    return out


def conjugate(moments):
    one = jnp.ones_like(moments[0])
    residual, direction, iterate = [one], [one], []
    now = moments[0]
    for step in range(3):
        image = applied(direction)
        alpha = now / product(direction, image, moments)
        scaled = [alpha * d for d in direction]
        iterate = scaled if not iterate else combined(iterate, one, scaled)
        residual = combined(residual, -alpha, image)
        if step < 2:
            new = product(residual, residual, moments)
            direction = combined(residual, new / now, direction)
            now = new
    return iterate, residual


def kernel(
    observed_hbm, predicted_hbm, coherence_hbm, count_hbm, owner_hbm, table_hbm, patch_hbm, look_hbm,
    weights_hbm, depth_hbm, stiff_hbm,
    adj_ref, res_ref,
    observed_ref, predicted_ref, coherence_ref, count_ref, owner_ref, table_ref, patch_ref, look_ref,
    weights, depth_ref, stiff_ref,
    numbers, valid, resid, coeffs, slots_ref, choice_ref,
    got_slots, got_choice, flat_slots, flat_choice,
    surf, surf_other, halo_x, halo_y,
    stiff_x, wide_stiff, strip_out, strip_in, coef,
    depths, table,
    fields, w1, w2, div,
    row_out, row_in, ring_in,
    send_a2a, recv_a2a, send_sem, recv_sem, local_sem,
):
    pairs = (
        (depth_hbm, depth_ref), (count_hbm, count_ref), (owner_hbm, owner_ref), (table_hbm, table_ref),
        (patch_hbm, patch_ref), (look_hbm, look_ref), (coherence_hbm, coherence_ref),
        (predicted_hbm, predicted_ref), (observed_hbm, observed_ref), (weights_hbm, weights), (stiff_hbm, stiff_ref),
    )
    fetches = [pltpu.make_async_copy(a, b, local_sem.at[i]) for i, (a, b) in enumerate(pairs)]
    for fetch in fetches:
        fetch.start()
    gx, gy, gz = lax.axis_index("gx"), lax.axis_index("gy"), lax.axis_index("gz")
    ngx, ngy = lax.axis_size("gx"), lax.axis_size("gy")
    owners = ngx * ngy
    me = gx * ngy + gy
    nz, nx, ny = stiff_ref.shape
    other = 1 - gz
    rows, lanes = nx + 8, 2 * ny
    tall = nx + 16

    def at(x, y, z):
        return {"gx": x, "gy": y, "gz": z}

    def wrap(value, count):
        return lax.rem(value + count, count)

    depths[...] = jnp.zeros(depths.shape, F32)
    own_layers = pl.ds(pl.multiple_of(8 + nz * gz, 8), nz)
    fetches[0].wait()
    layer = iota((nz, lanes), 0)
    own_depths = jnp.zeros((nz, lanes), F32)
    for z in range(nz):
        own_depths = jnp.where(layer == z, PRE * depth_ref[z], own_depths)
    depths[own_layers, :] = own_depths

    barrier = pltpu.get_barrier_semaphore()

    def greet(k, carry):
        o = lax.rem(me + k, owners)
        pl.semaphore_signal(barrier, inc=1, device_id=at(o // ngy, lax.rem(o, ngy), gz))
        return carry

    lax.fori_loop(1, owners, greet, 0)
    for k in range(ngy):
        pl.semaphore_signal(barrier, inc=1, device_id=at(gx, wrap(gy + k, ngy), other))

    def domain(count):
        r, c = iota((count, lanes), 0), iota((count, lanes), 1)
        half = (count - nx) // 2
        in_x = (r < nx) | ((r < nx + half) & (gx < ngx - 1)) | ((r >= nx + half) & (gx > 0))
        in_y = (c < ny) | ((c < ny + ny // 2) & (gy < ngy - 1)) | ((c >= ny + ny // 2) & (gy > 0))
        return (in_x & in_y).astype(F32)

    zero_plane = jnp.zeros((rows, lanes), F32)
    for edge in (0, 2 * nz + 1):
        div[edge] = zero_plane
        for c in range(3):
            w1[c, edge] = zero_plane
            w2[c, edge] = zero_plane
    blocks, epochs, pixels = observed_ref.shape
    for fetch in fetches[1:9]:
        fetch.wait()
    for b in range(blocks):
        for k, source in enumerate((count_ref, table_ref, patch_ref, owner_ref)):
            numbers[k, b:b + 1, :] = jnp.full((1, ny), source[b], jnp.int32)
    in_scene = iota((blocks, ny), 1)
    for k in range(0, pixels, ny):
        kept = (in_scene + k < numbers[0]).astype(F32)
        valid[:, k:k + ny] = coherence_ref[:, k:k + ny].astype(F32) * kept
    for b in range(blocks):
        resid[epochs * b:epochs * (b + 1), :] = (predicted_ref[b] - observed_ref[b]) * valid[b:b + 1, :]
    res = resid[...]
    row_block, row_place = iota((blocks, epochs * blocks), 0), iota((blocks, epochs * blocks), 1)
    own_rows = row_place // epochs == row_block
    for c in range(3):
        mix = jnp.zeros((blocks, epochs * blocks), F32)
        for e in range(epochs):
            mix = jnp.where(own_rows & (row_place % epochs == e), look_ref[e, c], mix)
        coeffs[c * blocks:(c + 1) * blocks, :] = jnp.dot(
            mix, res, precision=HIGHEST, preferred_element_type=F32
        )
    mass = jnp.sum(jnp.sum(res * res, axis=0, keepdims=True), axis=1, keepdims=True)
    weight = jnp.sum(jnp.sum(valid[...], axis=0, keepdims=True), axis=1, keepdims=True)

    lane_owner = iota((blocks, owners), 1)
    at_owner = (lane_owner == numbers[3, :, 0:owners]).astype(F32)
    before = (iota((blocks, blocks), 1) < iota((blocks, blocks), 0)).astype(F32)
    ahead_of = jnp.dot(before, at_owner, preferred_element_type=F32)
    rank = jnp.sum(ahead_of * at_owner, axis=1, keepdims=True).astype(jnp.int32)
    slot_of = numbers[3, :, 0:1] * CAP + rank
    select = (iota((blocks, owners * CAP), 1) == slot_of).astype(F32)
    at_lane = (iota((blocks, ny), 1) == rank * (ny // CAP) + numbers[2]).astype(F32)
    marks = lax.dot_general(at_owner, at_lane, (((0,), (0,)), ((), ())), preferred_element_type=F32)
    for o in range(owners):
        choice_ref[o] = marks[o:o + 1]

    rounded = coeffs[...].astype(jnp.bfloat16).astype(F32)
    which = jnp.concatenate([numbers[1]] * 3, axis=0)
    which = jnp.concatenate([which] * (pixels // ny), axis=1)
    fetches[9].wait()
    total_sums = jnp.zeros((3 * blocks, ny), F32)
    for t in range(weights.shape[0]):
        taken = jnp.where(which == t, rounded, 0.0).astype(jnp.bfloat16)
        total_sums = total_sums + jnp.dot(taken, weights[t], preferred_element_type=F32)
    for c in range(3):
        chosen = lax.dot_general(
            select, total_sums[c * blocks:(c + 1) * blocks], (((0,), (0,)), ((), ())),
            precision=HIGHEST, preferred_element_type=F32,
        )
        for o in range(owners):
            slots_ref[o, c] = chosen[CAP * o:CAP * (o + 1)]

    fetches[10].wait()
    pl.semaphore_wait(barrier, owners - 1 + ngy)

    def remote(source, target, index, device):
        return pltpu.make_async_remote_copy(
            src_ref=source, dst_ref=target, send_sem=send_sem.at[index], recv_sem=recv_sem.at[index],
            device_id=device, device_id_type=pl.DeviceIdType.MESH,
        )

    x_up, x_down = wrap(gx + 1, ngx), wrap(gx - 1, ngx)
    y_up, y_down = wrap(gy + 1, ngy), wrap(gy - 1, ngy)
    early = [
        remote(stiff_ref.at[:, pl.ds(0, 8), :], stiff_x.at[0], 0, at(x_down, gy, gz)),
        remote(stiff_ref.at[:, pl.ds(nx - 8, 8), :], stiff_x.at[1], 1, at(x_up, gy, gz)),
        remote(depths.at[own_layers, :], depths.at[own_layers, :], 2, at(gx, gy, other)),
    ]
    for copy in early:
        copy.start()

    def post(k, carry):
        o = lax.rem(me + k, owners)
        device = at(o // ngy, lax.rem(o, ngy), gz)
        pltpu.make_async_remote_copy(
            src_ref=slots_ref.at[o], dst_ref=got_slots.at[me], send_sem=send_a2a.at[0], recv_sem=recv_a2a.at[0],
            device_id=device, device_id_type=pl.DeviceIdType.MESH,
        ).start()
        pltpu.make_async_remote_copy(
            src_ref=choice_ref.at[o], dst_ref=got_choice.at[me], send_sem=send_a2a.at[1], recv_sem=recv_a2a.at[1],
            device_id=device, device_id_type=pl.DeviceIdType.MESH,
        ).start()
        return carry

    lax.fori_loop(1, owners, post, 0)
    got_slots[me] = slots_ref[me]
    got_choice[me] = choice_ref[me]

    for copy in early:
        copy.wait()
    low = iota((8, ny), 0) < 4
    for z in range(nz):
        wide_stiff[z, 0:nx, :] = stiff_ref[z]
        wide_stiff[z, nx:rows, :] = jnp.where(low, stiff_x[0, z], stiff_x[1, z])
    turned = wide_stiff[...].reshape(nz * rows, ny).T
    strip_out[0] = turned[0:8]
    strip_out[1] = turned[ny - 8:ny]
    strips = [
        remote(strip_out.at[0], strip_in.at[0], 3, at(gx, y_down, gz)),
        remote(strip_out.at[1], strip_in.at[1], 4, at(gx, y_up, gz)),
    ]
    for copy in strips:
        copy.start()

    d = depths[...]
    where_z = iota(d.shape, 0)
    inside = ((where_z >= 8) & (where_z < 8 + 2 * nz)).astype(F32)
    d_up, d_down = ahead(d, 0), behind(d, 0)
    q = 0.5 * (d_up - d_down)
    kept_d, kept_q = inside * d, inside * q
    columns = (
        d,
        0.125 * (d_up + d_down),
        q,
        (1.0 / 32.0) * (ahead(kept_d, 0) - behind(kept_d, 0)),
        (1.0 / 32.0) * (ahead(kept_q, 0) - behind(kept_q, 0)),
    )
    for k, values in enumerate(columns):
        for z in range(2 * nz):
            table[k, z] = values[z + 8:z + 9]

    for copy in strips:
        copy.wait()
    filler = jnp.zeros((ny - 16, nz * rows), F32)
    beside = jnp.concatenate([strip_in[0], filler, strip_in[1]], axis=0).T.reshape(nz, rows, ny)
    base = nz * gz
    for z in range(nz):
        coef[base + z, :, 0:ny] = 0.125 * wide_stiff[z] - 0.25
        coef[base + z, :, ny:lanes] = 0.125 * beside[z] - 0.25
    passed = pl.ds((nz - 4) + 4 * gz, 4)
    layers = remote(coef.at[passed], coef.at[passed], 5, at(gx, gy, other))
    layers.start()

    for message, buffer in enumerate((slots_ref, choice_ref)):
        part = buffer.at[pl.ds(0, owners - 1)]
        pltpu.make_async_copy(part, part, send_a2a.at[message]).wait()
    for message, buffer in enumerate((got_slots, got_choice)):
        part = buffer.at[pl.ds(0, owners - 1)]
        pltpu.make_async_copy(part, part, recv_a2a.at[message]).wait()
    own_slot = iota((CAP, ny), 1) // (ny // CAP) == iota((CAP, ny), 0)
    for o in range(owners):
        for c in range(3):
            flat_slots[c, CAP * o:CAP * (o + 1), :] = got_slots[o, c]
        flat_choice[CAP * o:CAP * (o + 1), :] = jnp.where(own_slot, got_choice[o], 0.0)
    picked = flat_choice[...]
    tiles = []
    for c in range(3):
        spread = lax.dot_general(
            picked, flat_slots[c], (((0,), (0,)), ((), ())), precision=HIGHEST, preferred_element_type=F32
        )
        depth_places = ny // CAP
        placed = spread[0:depth_places]
        for j in range(1, CAP):
            placed = placed + spread[j * depth_places:(j + 1) * depth_places]
        tiles.append(placed)
    tile = jnp.concatenate(tiles, axis=0)
    sub = lax.rem(iota(tile.shape, 0), 8)
    chunk = iota(tile.shape, 1) // PATCH_Y
    for bit in (1, 2, 4):
        row_set, chunk_set = (sub // bit) % 2 == 1, (chunk // bit) % 2 == 1
        from_below = roll(roll(tile, -bit, 0), bit * PATCH_Y, 1)
        from_above = roll(roll(tile, bit, 0), -bit * PATCH_Y, 1)
        tile = jnp.where(row_set == chunk_set, tile, jnp.where(row_set, from_above, from_below))
    surf[0] = tile.reshape(3, nx, ny)
    swap = remote(surf.at[0], surf_other, 6, at(gx, gy, other))
    swap.start()
    swap.wait()
    surf[1] = surf[0] + surf_other[...]

    first, last = pl.ds(0, 8), pl.ds(nx - 8, 8)
    whole = surf.at[1]
    halos = [
        remote(whole.at[:, first, :], halo_x.at[0], 7, at(x_down, gy, gz)),
        remote(whole.at[:, last, :], halo_x.at[1], 8, at(x_up, gy, gz)),
        remote(whole.at[:, first, :], halo_x.at[2], 9, at(x_down, y_down, gz)),
        remote(whole.at[:, first, :], halo_x.at[3], 10, at(x_down, y_up, gz)),
        remote(whole.at[:, last, :], halo_x.at[4], 11, at(x_up, y_down, gz)),
        remote(whole.at[:, last, :], halo_x.at[5], 12, at(x_up, y_up, gz)),
        remote(whole, halo_y.at[0], 13, at(gx, y_down, gz)),
        remote(whole, halo_y.at[1], 14, at(gx, y_up, gz)),
    ]
    for copy in halos:
        copy.start()
    for copy in halos:
        copy.wait()
    mask_tall = domain(tall)
    mask = domain(rows)
    left = iota((1, ny), 1) < ny // 2
    low_rows = iota((8, lanes), 0) < 4

    def packed(values):
        return jnp.concatenate(
            [values[0:nx], jnp.where(low_rows, values[nx:nx + 8], values[nx + 8:nx + 16])], axis=0
        )

    around = []
    for c in range(3):
        main = jnp.concatenate([surf[1, c], halo_x[0, c], halo_x[1, c]], axis=0)
        side = jnp.concatenate(
            [
                jnp.where(left, halo_y[0, c], halo_y[1, c]),
                jnp.where(left, halo_x[2, c], halo_x[3, c]),
                jnp.where(left, halo_x[4, c], halo_x[5, c]),
            ],
            axis=0,
        )
        around.append(mask_tall * jnp.concatenate([main, side], axis=1))
    flux = mask_tall * (
        0.5 * ((ahead(around[0], 0) - behind(around[0], 0)) + (ahead(around[1], 1) - behind(around[1], 1)))
    )
    for c in range(3):
        s = around[c]
        beside_xy = (ahead(s, 0) + behind(s, 0)) + (ahead(s, 1) + behind(s, 1))
        fields[c] = packed(s)
        if c < 2:
            drop = 0.125 * beside_xy + (1.0 / 32.0) * (ahead(flux, c) - behind(flux, c))
            fields[3 + c] = mask * packed(drop)
            fields[6 + c] = mask * packed((1.0 / 32.0) * (ahead(around[2], c) - behind(around[2], c)))
        else:
            fields[3 + c] = mask * packed(0.125 * beside_xy)
    fields[8] = packed(flux)

    layers.wait()

    def first_layer(i, carry):
        z = (nz - 4) * gz + i
        value = [table[k, z] for k in range(5)]
        own = coef[z] * value[0] - value[1]
        for c in range(2):
            w1[c, z + 1] = mask * (fields[c] * own) - value[0] * fields[3 + c] - value[2] * fields[6 + c]
        w1[2, z + 1] = mask * (fields[2] * (own - value[4])) - value[0] * fields[5] - value[3] * fields[8]
        return carry

    lax.fori_loop(0, nz + 4, first_layer, 0)

    def spread_of(source, start, amount):
        def layer(i, carry):
            z = start + i
            x, y = source[0, z + 1], source[1, z + 1]
            div[z + 1] = mask * (
                ((ahead(x, 0) - behind(x, 0)) + (ahead(y, 1) - behind(y, 1)))
                + (source[2, z + 2] - source[2, z])
            )
            return carry

        lax.fori_loop(0, amount, layer, 0)

    spread_of(w1, (nz - 3) * gz, nz + 3)

    def second_layer(i, carry):
        z = (nz - 2) * gz + i
        own = coef[z]
        here = div[z + 1]
        for c in range(3):
            v = w1[c, z + 1]
            total = (ahead(v, 0) + behind(v, 0)) + (ahead(v, 1) + behind(v, 1))
            total = total + (w1[c, z + 2] + w1[c, z])
            slope = (ahead(here, c) - behind(here, c)) if c < 2 else (div[z + 2] - div[z])
            w2[c, z + 1] = mask * (own * v - 0.125 * total - (1.0 / 64.0) * slope)
        return carry

    lax.fori_loop(0, nz + 2, second_layer, 0)

    spread_of(w2, (nz - 1) * gz, nz + 1)

    def folded(values):
        total = values[0:8]
        for k in range(8, nx, 8):
            total = total + values[k:k + 8]
        return total

    def third_layer(i, sums):
        z = nz * gz + i
        own = coef[z, 0:nx, 0:ny]
        here_x, here_y = div[z + 1, :, 0:ny], div[z + 1, 0:nx, :]
        d_now = table[0, z, :, 0:ny]
        sums = list(sums)
        for c in range(3):
            v = w2[c, z + 1, 0:nx, 0:ny]
            vx, vy = w2[c, z + 1, :, 0:ny], w2[c, z + 1, 0:nx, :]
            total = (ahead(vx, 0) + behind(vx, 0))[0:nx] + (ahead(vy, 1) + behind(vy, 1))[:, 0:ny]
            total = total + (w2[c, z + 2, 0:nx, 0:ny] + w2[c, z, 0:nx, 0:ny])
            if c == 0:
                slope = (ahead(here_x, 0) - behind(here_x, 0))[0:nx]
            elif c == 1:
                slope = (ahead(here_y, 1) - behind(here_y, 1))[:, 0:ny]
            else:
                slope = div[z + 2, 0:nx, 0:ny] - div[z, 0:nx, 0:ny]
            third = own * v - 0.125 * total - (1.0 / 64.0) * slope
            res_ref[c, i] = third
            zeroth = d_now * fields[c, 0:nx, 0:ny]
            one = w1[c, z + 1, 0:nx, 0:ny]
            for k, term in enumerate(
                (zeroth * zeroth, zeroth * one, one * one, one * v, v * v, v * third)
            ):
                sums[k] = sums[k] + folded(term)
        return tuple(sums)

    sums = lax.fori_loop(0, nz, third_layer, tuple(jnp.zeros((8, ny), F32) for _ in range(MOMENTS)))

    lane = iota((1, ny), 1)
    message = jnp.where(lane == MOMENTS, mass, 0.0) + jnp.where(lane == MOMENTS + 1, weight, 0.0)
    for k in range(MOMENTS):
        amount = jnp.sum(jnp.sum(sums[k], axis=0, keepdims=True), axis=1, keepdims=True)
        message = message + jnp.where(lane == k, amount, 0.0)
    row_out[0] = message
    slot = gy * 2 + gz
    row_in[slot] = message
    copies = []
    for k in range(1, ngy):
        copies.append((wrap(gy + k, ngy), gz))
    for k in range(ngy):
        copies.append((wrap(gy + k, ngy), other))
    started = []
    for k, (y, z) in enumerate(copies):
        copy = remote(row_out.at[0], row_in.at[slot], 15 + k, at(gx, y, z))
        copy.start()
        started.append(copy)
    for copy in started:
        copy.wait()
    message = row_in[0]
    for k in range(1, 2 * ngy):
        message = message + row_in[k]
    row_out[1] = message
    ring_in[gx] = message
    first_index = 15 + len(copies)
    started = []
    for k in range(1, ngx):
        copy = remote(row_out.at[1], ring_in.at[gx], first_index + k - 1, at(wrap(gx + k, ngx), gy, gz))
        copy.start()
        started.append(copy)
    for copy in started:
        copy.wait()
    message = ring_in[0]
    for k in range(1, ngx):
        message = message + ring_in[k]
    parts = [jnp.sum(jnp.where(lane == k, message, 0.0), axis=1, keepdims=True) for k in range(MOMENTS + 2)]

    scale = lax.rsqrt(parts[MOMENTS] / (EPOCHS * parts[MOMENTS + 1]) + EPS) * (1.0 / PRE)
    iterate, residual = conjugate(parts[0:MOMENTS])
    iterate = [scale * value for value in iterate]
    residual = [scale * value for value in residual]

    def finish(i, carry):
        z = nz * gz + i
        d_now = table[0, z, :, 0:ny]
        for c in range(3):
            zeroth = d_now * fields[c, 0:nx, 0:ny]
            one, two = w1[c, z + 1, 0:nx, 0:ny], w2[c, z + 1, 0:nx, 0:ny]
            third = res_ref[c, i]
            adj_ref[c, i] = iterate[0] * zeroth + iterate[1] * one + iterate[2] * two
            res_ref[c, i] = residual[0] * zeroth + residual[1] * one + residual[2] * two + residual[3] * third
        return carry

    lax.fori_loop(0, nz, finish, 0)


def per_device(
    observed,
    predicted,
    coherence_mask,
    block_count,
    block_owner,
    block_matrix_choice,
    block_patch,
    look_vector,
    interp_weights,
    depth_kernel,
    stiffness,
):
    blocks, epochs, pixels = observed.shape
    cells = PATCH_X * PATCH_Y
    ngx, ngy = lax.axis_size("gx"), lax.axis_size("gy")
    owners = ngx * ngy
    nz, nx, ny = stiffness.shape

    rows, lanes = nx + 8, 2 * ny
    out = jax.ShapeDtypeStruct((3, nz, nx, ny), F32)
    vmem = pl.BlockSpec(memory_space=pltpu.VMEM)
    far = pl.BlockSpec(memory_space=pltpu.HBM)
    copies = 15 + (2 * ngy - 1) + (ngx - 1)
    return pl.pallas_call(
        kernel,
        out_shape=(out, out),
        in_specs=[far] * 11,
        out_specs=(vmem, vmem),
        scratch_shapes=[
            pltpu.VMEM(observed.shape, F32),
            pltpu.VMEM(predicted.shape, F32),
            pltpu.VMEM(coherence_mask.shape, jnp.int32),
            pltpu.SMEM((blocks,), jnp.int32),
            pltpu.SMEM((blocks,), jnp.int32),
            pltpu.SMEM((blocks,), jnp.int32),
            pltpu.SMEM((blocks,), jnp.int32),
            pltpu.SMEM(look_vector.shape, F32),
            pltpu.VMEM(interp_weights.shape, interp_weights.dtype),
            pltpu.SMEM((nz,), F32),
            pltpu.VMEM(stiffness.shape, F32),
            pltpu.VMEM((4, blocks, ny), jnp.int32),
            pltpu.VMEM((blocks, pixels), F32),
            pltpu.VMEM((epochs * blocks, pixels), F32),
            pltpu.VMEM((3 * blocks, pixels), F32),
            pltpu.VMEM((owners, 3, CAP, cells), F32),
            pltpu.VMEM((owners, 1, cells), F32),
            pltpu.VMEM((owners, 3, CAP, cells), F32),
            pltpu.VMEM((owners, 1, cells), F32),
            pltpu.VMEM((3, owners * CAP, cells), F32),
            pltpu.VMEM((owners * CAP, cells), F32),
            pltpu.VMEM((2, 3, nx, ny), F32),
            pltpu.VMEM((3, nx, ny), F32),
            pltpu.VMEM((6, 3, 8, ny), F32),
            pltpu.VMEM((2, 3, nx, ny), F32),
            pltpu.VMEM((2, nz, 8, ny), F32),
            pltpu.VMEM((nz, rows, ny), F32),
            pltpu.VMEM((2, 8, nz * rows), F32),
            pltpu.VMEM((2, 8, nz * rows), F32),
            pltpu.VMEM((2 * nz, rows, lanes), F32),
            pltpu.VMEM((2 * nz + 16, lanes), F32),
            pltpu.VMEM((5, 2 * nz, 1, lanes), F32),
            pltpu.VMEM((9, rows, lanes), F32),
            pltpu.VMEM((3, 2 * nz + 2, rows, lanes), F32),
            pltpu.VMEM((3, 2 * nz + 2, rows, lanes), F32),
            pltpu.VMEM((2 * nz + 2, rows, lanes), F32),
            pltpu.VMEM((2, 1, ny), F32),
            pltpu.VMEM((2 * ngy, 1, ny), F32),
            pltpu.VMEM((ngx, 1, ny), F32),
            pltpu.SemaphoreType.DMA((2,)),
            pltpu.SemaphoreType.DMA((2,)),
            pltpu.SemaphoreType.DMA((copies,)),
            pltpu.SemaphoreType.DMA((copies,)),
            pltpu.SemaphoreType.DMA((11,)),
        ],
        compiler_params=pltpu.CompilerParams(
            collective_id=0, has_side_effects=True, vmem_limit_bytes=67043328
        ),
    )(
        observed, predicted, coherence_mask, block_count, block_owner[:, 0], block_matrix_choice, block_patch,
        look_vector, interp_weights, depth_kernel, stiffness,
    )


def solution(mesh):
    in_specs = (
        P(("grp", "gx", "gy", "gz"), None, None),
        P(("grp", "gx", "gy", "gz"), None, None),
        P(("grp", "gx", "gy", "gz"), None),
        P(("grp", "gx", "gy", "gz")),
        P(("grp", "gx", "gy", "gz"), None),
        P(("grp", "gx", "gy", "gz")),
        P(("grp", "gx", "gy", "gz")),
        P(),
        P(),
        P(("grp", "gz")),
        P(("grp", "gz"), "gx", "gy"),
    )
    out_specs = (P(None, ("grp", "gz"), "gx", "gy"), P(None, ("grp", "gz"), "gx", "gy"))
    return jax.shard_map(
        per_device, mesh=mesh, in_specs=in_specs, out_specs=out_specs, check_vma=False
    )
```

```python
import jax
import jax.numpy as jnp
from jax import lax
from jax.experimental import pallas as pl
from jax.experimental.pallas import tpu as pltpu
from jax.sharding import PartitionSpec as P

EPOCHS = 4
PATCH_X = 8
PATCH_Y = 16
CAP = 4
EPS = 1e-06

SHIFT = 8.0
PRE = 1024.0
MOMENTS = 6

HIGHEST = lax.Precision.HIGHEST
F32 = jnp.float32


def roll(values, shift, axis):
    return pltpu.roll(values, shift % values.shape[axis], axis)


def ahead(values, axis):
    return roll(values, -1, axis)


def behind(values, axis):
    return roll(values, 1, axis)


def iota(shape, axis):
    return lax.broadcasted_iota(jnp.int32, shape, axis)


def product(first, second, moments):
    total = None
    for i, f in enumerate(first):
        for j, g in enumerate(second):
            term = f * g * moments[i + j]
            total = term if total is None else total + term
    return total


def combined(first, factor, second):
    size = max(len(first), len(second))
    out = []
    for i in range(size):
        value = first[i] if i < len(first) else None
        if i < len(second):
            term = factor * second[i]
            value = term if value is None else value + term
        out.append(value)
    return out


def applied(poly):
    out = []
    for i in range(len(poly) + 1):
        value = None
        for j in (i, i - 1):
            if 0 <= j < len(poly):
                value = poly[j] if value is None else value + poly[j]
        out.append(SHIFT * value)
    return out


def conjugate(moments):
    one = jnp.ones_like(moments[0])
    residual, direction, iterate = [one], [one], []
    now = moments[0]
    for step in range(3):
        image = applied(direction)
        alpha = now / product(direction, image, moments)
        scaled = [alpha * d for d in direction]
        iterate = scaled if not iterate else combined(iterate, one, scaled)
        residual = combined(residual, -alpha, image)
        if step < 2:
            new = product(residual, residual, moments)
            direction = combined(residual, new / now, direction)
            now = new
    return iterate, residual


def kernel(
    observed_hbm, predicted_hbm, coherence_hbm, count_hbm, owner_hbm, table_hbm, patch_hbm, look_hbm,
    weights_hbm, depth_hbm, stiff_hbm,
    adj_ref, res_ref,
    observed_ref, predicted_ref, coherence_ref, count_ref, owner_ref, table_ref, patch_ref, look_ref,
    weights, depth_ref, stiff_ref,
    numbers, valid, resid, coeffs, slots_ref, choice_ref,
    got_slots, got_choice, flat_slots, flat_choice,
    surf, surf_other, border, halo_x, halo_y,
    stiff_x, wide_stiff, strip_out, strip_in, coef,
    depths, table,
    fields, w1, w2, div,
    row_out, row_in, ring_in,
    send_a2a, recv_a2a, send_sem, recv_sem, local_sem, chain, entered,
):
    pairs = (
        (depth_hbm, depth_ref), (count_hbm, count_ref), (owner_hbm, owner_ref), (table_hbm, table_ref),
        (patch_hbm, patch_ref), (look_hbm, look_ref), (coherence_hbm, coherence_ref),
        (predicted_hbm, predicted_ref), (observed_hbm, observed_ref), (weights_hbm, weights), (stiff_hbm, stiff_ref),
    )
    fetches = [pltpu.make_async_copy(a, b, local_sem.at[i]) for i, (a, b) in enumerate(pairs)]
    for fetch in fetches:
        fetch.start()
    gx, gy, gz = lax.axis_index("gx"), lax.axis_index("gy"), lax.axis_index("gz")
    ngx, ngy = lax.axis_size("gx"), lax.axis_size("gy")
    owners = ngx * ngy
    me = gx * ngy + gy
    nz, nx, ny = stiff_ref.shape
    other = 1 - gz
    rows, lanes = nx + 8, 2 * ny
    tall = nx + 16

    def at(x, y, z):
        return {"gx": x, "gy": y, "gz": z}

    def wrap(value, count):
        return lax.rem(value + count, count)

    depths[...] = jnp.zeros(depths.shape, F32)
    own_layers = pl.ds(pl.multiple_of(8 + nz * gz, 8), nz)
    fetches[0].wait()
    layer = iota((nz, lanes), 0)
    own_depths = jnp.zeros((nz, lanes), F32)
    for z in range(nz):
        own_depths = jnp.where(layer == z, PRE * depth_ref[z], own_depths)
    depths[own_layers, :] = own_depths
    stiff_x[...] = jnp.zeros(stiff_x.shape, F32)

    barrier = pltpu.get_barrier_semaphore()
    peers = [(wrap(gy + k, ngy), gz) for k in range(1, ngy)] + [(wrap(gy + k, ngy), other) for k in range(ngy)]
    below, above = gx > 0, gx < ngx - 1
    for y, z in peers:
        pl.semaphore_signal(barrier, inc=1, device_id=at(gx, y, z))

    @pl.when(below)
    def _():
        pl.semaphore_signal(barrier, inc=1, device_id=at(gx - 1, gy, gz))

    @pl.when(above)
    def _():
        pl.semaphore_signal(barrier, inc=1, device_id=at(gx + 1, gy, gz))

    def domain(count):
        r, c = iota((count, lanes), 0), iota((count, lanes), 1)
        half = (count - nx) // 2
        in_x = (r < nx) | ((r < nx + half) & (gx < ngx - 1)) | ((r >= nx + half) & (gx > 0))
        in_y = (c < ny) | ((c < ny + ny // 2) & (gy < ngy - 1)) | ((c >= ny + ny // 2) & (gy > 0))
        return (in_x & in_y).astype(F32)

    zero_plane = jnp.zeros((rows, lanes), F32)
    for edge in (0, 2 * nz + 1):
        div[edge] = zero_plane
        for c in range(3):
            w1[c, edge] = zero_plane
            w2[c, edge] = zero_plane
    blocks, epochs, pixels = observed_ref.shape
    for fetch in fetches[1:9]:
        fetch.wait()

    pl.semaphore_wait(barrier, len(peers) + below.astype(jnp.int32) + above.astype(jnp.int32))

    @pl.when(below)
    def _():
        pl.semaphore_wait(chain, 1)

    @pl.when(above)
    def _():
        pl.semaphore_signal(chain, inc=1, device_id=at(gx + 1, gy, gz))

    def announce(j, carry):
        pl.semaphore_signal(entered.at[gx], inc=1, device_id=at(j, gy, gz))
        return carry

    lax.fori_loop(0, gx, announce, 0)

    for b in range(blocks):
        for k, source in enumerate((count_ref, table_ref, patch_ref, owner_ref)):
            numbers[k, b:b + 1, :] = jnp.full((1, ny), source[b], jnp.int32)
    in_scene = iota((blocks, ny), 1)
    for k in range(0, pixels, ny):
        kept = (in_scene + k < numbers[0]).astype(F32)
        valid[:, k:k + ny] = coherence_ref[:, k:k + ny].astype(F32) * kept
    for b in range(blocks):
        resid[epochs * b:epochs * (b + 1), :] = (predicted_ref[b] - observed_ref[b]) * valid[b:b + 1, :]
    res = resid[...]
    row_block, row_place = iota((blocks, epochs * blocks), 0), iota((blocks, epochs * blocks), 1)
    own_rows = row_place // epochs == row_block
    for c in range(3):
        mix = jnp.zeros((blocks, epochs * blocks), F32)
        for e in range(epochs):
            mix = jnp.where(own_rows & (row_place % epochs == e), look_ref[e, c], mix)
        coeffs[c * blocks:(c + 1) * blocks, :] = jnp.dot(
            mix, res, precision=HIGHEST, preferred_element_type=F32
        )
    mass = jnp.sum(jnp.sum(res * res, axis=0, keepdims=True), axis=1, keepdims=True)
    weight = jnp.sum(jnp.sum(valid[...], axis=0, keepdims=True), axis=1, keepdims=True)

    lane_owner = iota((blocks, owners), 1)
    at_owner = (lane_owner == numbers[3, :, 0:owners]).astype(F32)
    before = (iota((blocks, blocks), 1) < iota((blocks, blocks), 0)).astype(F32)
    ahead_of = jnp.dot(before, at_owner, preferred_element_type=F32)
    rank = jnp.sum(ahead_of * at_owner, axis=1, keepdims=True).astype(jnp.int32)
    slot_of = numbers[3, :, 0:1] * CAP + rank
    select = (iota((blocks, owners * CAP), 1) == slot_of).astype(F32)
    at_lane = (iota((blocks, ny), 1) == rank * (ny // CAP) + numbers[2]).astype(F32)
    marks = lax.dot_general(at_owner, at_lane, (((0,), (0,)), ((), ())), preferred_element_type=F32)
    for o in range(owners):
        choice_ref[o] = marks[o:o + 1]

    rounded = coeffs[...].astype(jnp.bfloat16).astype(F32)
    which = jnp.concatenate([numbers[1]] * 3, axis=0)
    which = jnp.concatenate([which] * (pixels // ny), axis=1)
    fetches[9].wait()
    total_sums = jnp.zeros((3 * blocks, ny), F32)
    for t in range(weights.shape[0]):
        taken = jnp.where(which == t, rounded, 0.0).astype(jnp.bfloat16)
        total_sums = total_sums + jnp.dot(taken, weights[t], preferred_element_type=F32)
    for c in range(3):
        chosen = lax.dot_general(
            select, total_sums[c * blocks:(c + 1) * blocks], (((0,), (0,)), ((), ())),
            precision=HIGHEST, preferred_element_type=F32,
        )
        for o in range(owners):
            slots_ref[o, c] = chosen[CAP * o:CAP * (o + 1)]

    fetches[10].wait()

    def remote(source, target, index, device, arrival=None):
        return pltpu.make_async_remote_copy(
            src_ref=source, dst_ref=target, send_sem=send_sem.at[index],
            recv_sem=recv_sem.at[index if arrival is None else arrival],
            device_id=device, device_id_type=pl.DeviceIdType.MESH,
        )

    def post(j, first):
        for k in range(first, ngy):
            y = wrap(gy + k, ngy)
            o = j * ngy + y
            for message, (source, target) in enumerate(((slots_ref, got_slots), (choice_ref, got_choice))):
                pltpu.make_async_remote_copy(
                    src_ref=source.at[o], dst_ref=target.at[me],
                    send_sem=send_a2a.at[message], recv_sem=recv_a2a.at[message],
                    device_id=at(j, y, gz), device_id_type=pl.DeviceIdType.MESH,
                ).start()

    def post_known(i, carry):
        d = ngx // 2 - i
        down, up = wrap(gx - d, ngx), wrap(gx + d, ngx)

        @pl.when(down < gx)
        def _():
            post(down, 0)

        @pl.when((up < gx) & (d < ngx // 2))
        def _():
            post(up, 0)

        return carry

    lax.fori_loop(0, ngx // 2, post_known, 0)
    post(gx, 1)

    x_up, x_down = wrap(gx + 1, ngx), wrap(gx - 1, ngx)
    y_up, y_down = wrap(gy + 1, ngy), wrap(gy - 1, ngy)
    to_down = remote(stiff_ref.at[:, pl.ds(0, 8), :], stiff_x.at[0], 0, at(x_down, gy, gz))
    to_up = remote(stiff_ref.at[:, pl.ds(nx - 8, 8), :], stiff_x.at[1], 1, at(x_up, gy, gz))
    to_other = remote(depths.at[own_layers, :], depths.at[own_layers, :], 2, at(gx, gy, other))
    to_other.start()

    @pl.when(below)
    def _():
        to_down.start()

    @pl.when(above)
    def _():
        to_up.start()

    got_slots[me] = slots_ref[me]
    got_choice[me] = choice_ref[me]

    @pl.when(below)
    def _():
        to_down.wait_send()
        to_up.wait_recv()

    @pl.when(above)
    def _():
        to_up.wait_send()
        to_down.wait_recv()

    to_other.wait()
    low = iota((8, ny), 0) < 4
    for z in range(nz):
        wide_stiff[z, 0:nx, :] = stiff_ref[z]
        wide_stiff[z, nx:rows, :] = jnp.where(low, stiff_x[0, z], stiff_x[1, z])
    turned = wide_stiff[...].reshape(nz * rows, ny).T
    strip_out[0] = turned[0:8]
    strip_out[1] = turned[ny - 8:ny]
    strips = [
        remote(strip_out.at[0], strip_in.at[0], 3, at(gx, y_down, gz)),
        remote(strip_out.at[1], strip_in.at[1], 4, at(gx, y_up, gz)),
    ]
    for copy in strips:
        copy.start()

    d = depths[...]
    where_z = iota(d.shape, 0)
    inside = ((where_z >= 8) & (where_z < 8 + 2 * nz)).astype(F32)
    d_up, d_down = ahead(d, 0), behind(d, 0)
    q = 0.5 * (d_up - d_down)
    kept_d, kept_q = inside * d, inside * q
    columns = (
        d,
        0.125 * (d_up + d_down),
        q,
        (1.0 / 32.0) * (ahead(kept_d, 0) - behind(kept_d, 0)),
        (1.0 / 32.0) * (ahead(kept_q, 0) - behind(kept_q, 0)),
    )
    for k, values in enumerate(columns):
        for z in range(2 * nz):
            table[k, z] = values[z + 8:z + 9]

    for copy in strips:
        copy.wait()
    filler = jnp.zeros((ny - 16, nz * rows), F32)
    beside = jnp.concatenate([strip_in[0], filler, strip_in[1]], axis=0).T.reshape(nz, rows, ny)
    base = nz * gz
    for z in range(nz):
        coef[base + z, :, 0:ny] = 0.125 * wide_stiff[z] - 0.25
        coef[base + z, :, ny:lanes] = 0.125 * beside[z] - 0.25
    passed = pl.ds((nz - 4) + 4 * gz, 4)
    layers = remote(coef.at[passed], coef.at[passed], 5, at(gx, gy, other))
    layers.start()

    def post_later(j, carry):
        pl.semaphore_wait(entered.at[j], 1)
        post(j, 0)
        return carry

    lax.fori_loop(gx + 1, ngx, post_later, 0)

    for message, buffer in enumerate((slots_ref, choice_ref)):
        part = buffer.at[pl.ds(0, owners - 1)]
        pltpu.make_async_copy(part, part, send_a2a.at[message]).wait()
    for message, buffer in enumerate((got_slots, got_choice)):
        part = buffer.at[pl.ds(0, owners - 1)]
        pltpu.make_async_copy(part, part, recv_a2a.at[message]).wait()
    own_slot = iota((CAP, ny), 1) // (ny // CAP) == iota((CAP, ny), 0)
    for o in range(owners):
        for c in range(3):
            flat_slots[c, CAP * o:CAP * (o + 1), :] = got_slots[o, c]
        flat_choice[CAP * o:CAP * (o + 1), :] = jnp.where(own_slot, got_choice[o], 0.0)
    picked = flat_choice[...]
    tiles = []
    for c in range(3):
        spread = lax.dot_general(
            picked, flat_slots[c], (((0,), (0,)), ((), ())), precision=HIGHEST, preferred_element_type=F32
        )
        depth_places = ny // CAP
        placed = spread[0:depth_places]
        for j in range(1, CAP):
            placed = placed + spread[j * depth_places:(j + 1) * depth_places]
        tiles.append(placed)
    tile = jnp.concatenate(tiles, axis=0)
    sub = lax.rem(iota(tile.shape, 0), 8)
    chunk = iota(tile.shape, 1) // PATCH_Y
    for bit in (1, 2, 4):
        row_set, chunk_set = (sub // bit) % 2 == 1, (chunk // bit) % 2 == 1
        from_below = roll(roll(tile, -bit, 0), bit * PATCH_Y, 1)
        from_above = roll(roll(tile, bit, 0), -bit * PATCH_Y, 1)
        tile = jnp.where(row_set == chunk_set, tile, jnp.where(row_set, from_above, from_below))
    surf[...] = tile.reshape(3, nx, ny)
    turned = tile.T
    border[0] = turned[0:8]
    border[1] = turned[ny - 8:ny]

    swap = remote(surf, surf_other, 6, at(gx, gy, other))
    swap.start()
    first, last = pl.ds(0, 8), pl.ds(nx - 8, 8)
    ways = (
        (surf.at[:, first, :], halo_x, 0, x_down, gy),
        (surf.at[:, last, :], halo_x, 1, x_up, gy),
        (border.at[0], halo_y, 0, gx, y_down),
        (border.at[1], halo_y, 1, gx, y_up),
        (border.at[0], halo_y, 2, x_down, y_down),
        (border.at[1], halo_y, 3, x_down, y_up),
        (border.at[0], halo_y, 4, x_up, y_down),
        (border.at[1], halo_y, 5, x_up, y_up),
    )
    count = len(ways)
    started = []
    for k in reversed(range(count)):
        source, target, place, x, y = ways[k]
        for i, z in enumerate((gz, other)):
            copy = remote(source, target.at[gz, place], 7 + i * count + k, at(x, y, z), 7 + gz * count + k)
            copy.start()
            started.append(copy)
    swap.wait()
    for k, (source, target, place, x, y) in enumerate(ways):
        for i in range(2):
            remote(source, target.at[i, place], 7 + i * count + k, at(x, y, gz)).wait_recv()
    for copy in started:
        copy.wait_send()
    mask_tall = domain(tall)
    mask = domain(rows)
    low_rows = iota((8, lanes), 0) < 4

    def packed(values):
        return jnp.concatenate(
            [values[0:nx], jnp.where(low_rows, values[nx:nx + 8], values[nx + 8:nx + 16])], axis=0
        )

    blank = jnp.zeros((ny - 16, 3 * nx), F32)

    def columns_of(place):
        low_side, high_side = halo_y[0, place] + halo_y[1, place], halo_y[0, place + 1] + halo_y[1, place + 1]
        return jnp.concatenate([low_side, blank, high_side], axis=0).T.reshape(3, nx, ny)

    near, upper, lower = columns_of(0), columns_of(2), columns_of(4)
    around = []
    for c in range(3):
        main = jnp.concatenate(
            [surf[c] + surf_other[c], halo_x[0, 0, c] + halo_x[1, 0, c], halo_x[0, 1, c] + halo_x[1, 1, c]], axis=0
        )
        side = jnp.concatenate([near[c], upper[c, 0:8], lower[c, nx - 8:nx]], axis=0)
        around.append(mask_tall * jnp.concatenate([main, side], axis=1))
    flux = mask_tall * (
        0.5 * ((ahead(around[0], 0) - behind(around[0], 0)) + (ahead(around[1], 1) - behind(around[1], 1)))
    )
    for c in range(3):
        s = around[c]
        beside_xy = (ahead(s, 0) + behind(s, 0)) + (ahead(s, 1) + behind(s, 1))
        fields[c] = packed(s)
        if c < 2:
            drop = 0.125 * beside_xy + (1.0 / 32.0) * (ahead(flux, c) - behind(flux, c))
            fields[3 + c] = mask * packed(drop)
            fields[6 + c] = mask * packed((1.0 / 32.0) * (ahead(around[2], c) - behind(around[2], c)))
        else:
            fields[3 + c] = mask * packed(0.125 * beside_xy)
    fields[8] = packed(flux)

    layers.wait()

    def first_layer(i, carry):
        z = (nz - 4) * gz + i
        value = [table[k, z] for k in range(5)]
        own = coef[z] * value[0] - value[1]
        for c in range(2):
            w1[c, z + 1] = mask * (fields[c] * own) - value[0] * fields[3 + c] - value[2] * fields[6 + c]
        w1[2, z + 1] = mask * (fields[2] * (own - value[4])) - value[0] * fields[5] - value[3] * fields[8]
        return carry

    lax.fori_loop(0, nz + 4, first_layer, 0)

    def spread_of(source, start, amount):
        def layer(i, carry):
            z = start + i
            x, y = source[0, z + 1], source[1, z + 1]
            div[z + 1] = mask * (
                ((ahead(x, 0) - behind(x, 0)) + (ahead(y, 1) - behind(y, 1)))
                + (source[2, z + 2] - source[2, z])
            )
            return carry

        lax.fori_loop(0, amount, layer, 0)

    spread_of(w1, (nz - 3) * gz, nz + 3)

    def second_layer(i, carry):
        z = (nz - 2) * gz + i
        own = coef[z]
        here = div[z + 1]
        for c in range(3):
            v = w1[c, z + 1]
            total = (ahead(v, 0) + behind(v, 0)) + (ahead(v, 1) + behind(v, 1))
            total = total + (w1[c, z + 2] + w1[c, z])
            slope = (ahead(here, c) - behind(here, c)) if c < 2 else (div[z + 2] - div[z])
            w2[c, z + 1] = mask * (own * v - 0.125 * total - (1.0 / 64.0) * slope)
        return carry

    lax.fori_loop(0, nz + 2, second_layer, 0)

    spread_of(w2, (nz - 1) * gz, nz + 1)

    def folded(values):
        total = values[0:8]
        for k in range(8, nx, 8):
            total = total + values[k:k + 8]
        return total

    def gather_moments(i, sums):
        z = nz * gz + i
        own = coef[z, 0:nx, 0:ny]
        d_now = table[0, z, :, 0:ny]
        here = div[z + 1, 0:nx, 0:ny]
        terms = [None] * MOMENTS
        terms[MOMENTS - 1] = (1.0 / 64.0) * (here * here)
        for c in range(3):
            v = w2[c, z + 1, 0:nx, 0:ny]
            total = ahead(w2[c, z + 1, :, 0:ny], 0)[0:nx] + ahead(w2[c, z + 1, 0:nx, :], 1)[:, 0:ny]
            total = total + w2[c, z + 2, 0:nx, 0:ny]
            zeroth = d_now * fields[c, 0:nx, 0:ny]
            one = w1[c, z + 1, 0:nx, 0:ny]
            for k, term in enumerate(
                (zeroth * zeroth, zeroth * one, one * one, one * v, v * v, v * (own * v - 0.25 * total))
            ):
                terms[k] = term if terms[k] is None else terms[k] + term
        return tuple(s + folded(t) for s, t in zip(sums, terms))

    sums = lax.fori_loop(0, nz, gather_moments, tuple(jnp.zeros((8, ny), F32) for _ in range(MOMENTS)))

    def third_layer(i, carry):
        z = nz * gz + i
        own = coef[z, 0:nx, 0:ny]
        here_x, here_y = div[z + 1, :, 0:ny], div[z + 1, 0:nx, :]
        for c in range(3):
            v = w2[c, z + 1, 0:nx, 0:ny]
            vx, vy = w2[c, z + 1, :, 0:ny], w2[c, z + 1, 0:nx, :]
            total = (ahead(vx, 0) + behind(vx, 0))[0:nx] + (ahead(vy, 1) + behind(vy, 1))[:, 0:ny]
            total = total + (w2[c, z + 2, 0:nx, 0:ny] + w2[c, z, 0:nx, 0:ny])
            if c == 0:
                slope = (ahead(here_x, 0) - behind(here_x, 0))[0:nx]
            elif c == 1:
                slope = (ahead(here_y, 1) - behind(here_y, 1))[:, 0:ny]
            else:
                slope = div[z + 2, 0:nx, 0:ny] - div[z, 0:nx, 0:ny]
            res_ref[c, i] = own * v - 0.125 * total - (1.0 / 64.0) * slope
        return carry

    early_layers = (3 * nz) // 8

    lane = iota((1, ny), 1)
    message = jnp.where(lane == MOMENTS, mass, 0.0) + jnp.where(lane == MOMENTS + 1, weight, 0.0)
    for k in range(MOMENTS):
        amount = jnp.sum(jnp.sum(sums[k], axis=0, keepdims=True), axis=1, keepdims=True)
        message = message + jnp.where(lane == k, amount, 0.0)
    row_out[0] = message
    slot = gy * 2 + gz
    row_in[slot] = message
    base = 7 + 2 * count
    started = []
    for k, (y, z) in enumerate(peers):
        copy = remote(row_out.at[0], row_in.at[slot], base + k, at(gx, y, z))
        copy.start()
        started.append(copy)
    lax.fori_loop(0, early_layers, third_layer, 0)
    for copy in started:
        copy.wait()
    message = row_in[0]
    for k in range(1, 2 * ngy):
        message = message + row_in[k]
    row_out[1] = message
    ring_in[gx] = message
    first_index = base + len(peers)
    started = []
    for k in range(1, ngx):
        copy = remote(row_out.at[1], ring_in.at[gx], first_index + k - 1, at(wrap(gx + k, ngx), gy, gz))
        copy.start()
        started.append(copy)
    lax.fori_loop(early_layers, nz, third_layer, 0)
    for copy in started:
        copy.wait()
    message = ring_in[0]
    for k in range(1, ngx):
        message = message + ring_in[k]
    parts = [jnp.sum(jnp.where(lane == k, message, 0.0), axis=1, keepdims=True) for k in range(MOMENTS + 2)]

    scale = lax.rsqrt(parts[MOMENTS] / (EPOCHS * parts[MOMENTS + 1]) + EPS) * (1.0 / PRE)
    iterate, residual = conjugate(parts[0:MOMENTS])
    iterate = [scale * value for value in iterate]
    residual = [scale * value for value in residual]

    def finish(i, carry):
        z = nz * gz + i
        d_now = table[0, z, :, 0:ny]
        for c in range(3):
            zeroth = d_now * fields[c, 0:nx, 0:ny]
            one, two = w1[c, z + 1, 0:nx, 0:ny], w2[c, z + 1, 0:nx, 0:ny]
            third = res_ref[c, i]
            adj_ref[c, i] = iterate[0] * zeroth + iterate[1] * one + iterate[2] * two
            res_ref[c, i] = residual[0] * zeroth + residual[1] * one + residual[2] * two + residual[3] * third
        return carry

    lax.fori_loop(0, nz, finish, 0)


def per_device(
    observed,
    predicted,
    coherence_mask,
    block_count,
    block_owner,
    block_matrix_choice,
    block_patch,
    look_vector,
    interp_weights,
    depth_kernel,
    stiffness,
):
    blocks, epochs, pixels = observed.shape
    cells = PATCH_X * PATCH_Y
    ngx, ngy = lax.axis_size("gx"), lax.axis_size("gy")
    owners = ngx * ngy
    nz, nx, ny = stiffness.shape

    rows, lanes = nx + 8, 2 * ny
    out = pltpu.VMEM((3, nz, nx, ny), F32)
    vmem = pl.BlockSpec(memory_space=pltpu.VMEM)
    far = pl.BlockSpec(memory_space=pltpu.HBM)
    copies = 23 + (2 * ngy - 1) + (ngx - 1)
    return pl.pallas_call(
        kernel,
        out_shape=(out, out),
        in_specs=[far] * 11,
        out_specs=(vmem, vmem),
        scratch_shapes=[
            pltpu.VMEM(observed.shape, F32),
            pltpu.VMEM(predicted.shape, F32),
            pltpu.VMEM(coherence_mask.shape, jnp.int32),
            pltpu.SMEM((blocks,), jnp.int32),
            pltpu.SMEM((blocks,), jnp.int32),
            pltpu.SMEM((blocks,), jnp.int32),
            pltpu.SMEM((blocks,), jnp.int32),
            pltpu.SMEM(look_vector.shape, F32),
            pltpu.VMEM(interp_weights.shape, interp_weights.dtype),
            pltpu.SMEM((nz,), F32),
            pltpu.VMEM(stiffness.shape, F32),
            pltpu.VMEM((4, blocks, ny), jnp.int32),
            pltpu.VMEM((blocks, pixels), F32),
            pltpu.VMEM((epochs * blocks, pixels), F32),
            pltpu.VMEM((3 * blocks, pixels), F32),
            pltpu.VMEM((owners, 3, CAP, cells), F32),
            pltpu.VMEM((owners, 1, cells), F32),
            pltpu.VMEM((owners, 3, CAP, cells), F32),
            pltpu.VMEM((owners, 1, cells), F32),
            pltpu.VMEM((3, owners * CAP, cells), F32),
            pltpu.VMEM((owners * CAP, cells), F32),
            pltpu.VMEM((3, nx, ny), F32),
            pltpu.VMEM((3, nx, ny), F32),
            pltpu.VMEM((2, 8, 3 * nx), F32),
            pltpu.VMEM((2, 2, 3, 8, ny), F32),
            pltpu.VMEM((2, 6, 8, 3 * nx), F32),
            pltpu.VMEM((2, nz, 8, ny), F32),
            pltpu.VMEM((nz, rows, ny), F32),
            pltpu.VMEM((2, 8, nz * rows), F32),
            pltpu.VMEM((2, 8, nz * rows), F32),
            pltpu.VMEM((2 * nz, rows, lanes), F32),
            pltpu.VMEM((2 * nz + 16, lanes), F32),
            pltpu.VMEM((5, 2 * nz, 1, lanes), F32),
            pltpu.VMEM((9, rows, lanes), F32),
            pltpu.VMEM((3, 2 * nz + 2, rows, lanes), F32),
            pltpu.VMEM((3, 2 * nz + 2, rows, lanes), F32),
            pltpu.VMEM((2 * nz + 2, rows, lanes), F32),
            pltpu.VMEM((2, 1, ny), F32),
            pltpu.VMEM((2 * ngy, 1, ny), F32),
            pltpu.VMEM((ngx, 1, ny), F32),
            pltpu.SemaphoreType.DMA((2,)),
            pltpu.SemaphoreType.DMA((2,)),
            pltpu.SemaphoreType.DMA((copies,)),
            pltpu.SemaphoreType.DMA((copies,)),
            pltpu.SemaphoreType.DMA((11,)),
            pltpu.SemaphoreType.REGULAR,
            pltpu.SemaphoreType.REGULAR((ngx,)),
        ],
        compiler_params=pltpu.CompilerParams(
            collective_id=0, has_side_effects=True, vmem_limit_bytes=60000000
        ),
    )(
        observed, predicted, coherence_mask, block_count, block_owner[:, 0], block_matrix_choice, block_patch,
        look_vector, interp_weights, depth_kernel, stiffness,
    )


def solution(mesh):
    in_specs = (
        P(("grp", "gx", "gy", "gz"), None, None),
        P(("grp", "gx", "gy", "gz"), None, None),
        P(("grp", "gx", "gy", "gz"), None),
        P(("grp", "gx", "gy", "gz")),
        P(("grp", "gx", "gy", "gz"), None),
        P(("grp", "gx", "gy", "gz")),
        P(("grp", "gx", "gy", "gz")),
        P(),
        P(),
        P(("grp", "gz")),
        P(("grp", "gz"), "gx", "gy"),
    )
    out_specs = (P(None, ("grp", "gz"), "gx", "gy"), P(None, ("grp", "gz"), "gx", "gy"))
    return jax.shard_map(
        per_device, mesh=mesh, in_specs=in_specs, out_specs=out_specs, check_vma=False
    )
```

```python
import jax
import jax.numpy as jnp
from jax import lax
from jax.experimental import pallas as pl
from jax.experimental.pallas import tpu as pltpu
from jax.sharding import PartitionSpec as P

EPOCHS = 4
PATCH_X = 8
PATCH_Y = 16
CAP = 4
EPS = 1e-06

SHIFT = 8.0
PRE = 1024.0
MOMENTS = 6

HIGHEST = lax.Precision.HIGHEST
F32 = jnp.float32


def roll(values, shift, axis):
    return pltpu.roll(values, shift % values.shape[axis], axis)


def ahead(values, axis):
    return roll(values, -1, axis)


def behind(values, axis):
    return roll(values, 1, axis)


def iota(shape, axis):
    return lax.broadcasted_iota(jnp.int32, shape, axis)


def product(first, second, moments):
    total = None
    for i, f in enumerate(first):
        for j, g in enumerate(second):
            term = f * g * moments[i + j]
            total = term if total is None else total + term
    return total


def combined(first, factor, second):
    size = max(len(first), len(second))
    out = []
    for i in range(size):
        value = first[i] if i < len(first) else None
        if i < len(second):
            term = factor * second[i]
            value = term if value is None else value + term
        out.append(value)
    return out


def applied(poly):
    out = []
    for i in range(len(poly) + 1):
        value = None
        for j in (i, i - 1):
            if 0 <= j < len(poly):
                value = poly[j] if value is None else value + poly[j]
        out.append(SHIFT * value)
    return out


def conjugate(moments):
    one = jnp.ones_like(moments[0])
    residual, direction, iterate = [one], [one], []
    now = moments[0]
    for step in range(3):
        image = applied(direction)
        alpha = now / product(direction, image, moments)
        scaled = [alpha * d for d in direction]
        iterate = scaled if not iterate else combined(iterate, one, scaled)
        residual = combined(residual, -alpha, image)
        if step < 2:
            new = product(residual, residual, moments)
            direction = combined(residual, new / now, direction)
            now = new
    return iterate, residual


def kernel(
    observed_hbm, predicted_hbm, coherence_hbm, count_hbm, owner_hbm, table_hbm, patch_hbm, look_hbm,
    weights_hbm, depth_hbm, stiff_hbm,
    adj_ref, res_ref,
    observed_ref, predicted_ref, coherence_ref, count_ref, owner_ref, table_ref, patch_ref, look_ref,
    weights, depth_ref, stiff_ref,
    numbers, valid, resid, coeffs, slots_ref, choice_ref,
    got_slots, got_choice, flat_slots, flat_choice,
    surf, surf_other, border, halo_x, halo_y,
    stiff_x, wide_stiff, strip_out, strip_in, coef,
    depths, table,
    fields, w1, w2, div,
    row_out, row_in, ring_in,
    send_a2a, recv_a2a, send_sem, recv_sem, local_sem,
):
    pairs = (
        (depth_hbm, depth_ref), (count_hbm, count_ref), (owner_hbm, owner_ref), (table_hbm, table_ref),
        (patch_hbm, patch_ref), (look_hbm, look_ref), (coherence_hbm, coherence_ref),
        (predicted_hbm, predicted_ref), (observed_hbm, observed_ref), (weights_hbm, weights), (stiff_hbm, stiff_ref),
    )
    fetches = [pltpu.make_async_copy(a, b, local_sem.at[i]) for i, (a, b) in enumerate(pairs)]
    for fetch in fetches:
        fetch.start()
    gx, gy, gz = lax.axis_index("gx"), lax.axis_index("gy"), lax.axis_index("gz")
    ngx, ngy = lax.axis_size("gx"), lax.axis_size("gy")
    owners = ngx * ngy
    me = gx * ngy + gy
    nz, nx, ny = stiff_ref.shape
    other = 1 - gz
    rows, lanes = nx + 8, 2 * ny
    tall = nx + 16

    def at(x, y, z):
        return {"gx": x, "gy": y, "gz": z}

    def wrap(value, count):
        return lax.rem(value + count, count)

    depths[...] = jnp.zeros(depths.shape, F32)
    own_layers = pl.ds(pl.multiple_of(8 + nz * gz, 8), nz)
    fetches[0].wait()
    layer = iota((nz, lanes), 0)
    own_depths = jnp.zeros((nz, lanes), F32)
    for z in range(nz):
        own_depths = jnp.where(layer == z, PRE * depth_ref[z], own_depths)
    depths[own_layers, :] = own_depths

    barrier = pltpu.get_barrier_semaphore()
    peers = [(wrap(gy + k, ngy), gz) for k in range(1, ngy)] + [(wrap(gy + k, ngy), other) for k in range(ngy)]

    def greet(k, carry):
        j = wrap(gx - k, ngx)
        for y in range(ngy):
            pl.semaphore_signal(barrier, inc=1, device_id=at(j, y, gz))
        return carry

    lax.fori_loop(1, ngx, greet, 0)
    for y, z in peers:
        pl.semaphore_signal(barrier, inc=1, device_id=at(gx, y, z))

    def domain(count):
        r, c = iota((count, lanes), 0), iota((count, lanes), 1)
        half = (count - nx) // 2
        in_x = (r < nx) | ((r < nx + half) & (gx < ngx - 1)) | ((r >= nx + half) & (gx > 0))
        in_y = (c < ny) | ((c < ny + ny // 2) & (gy < ngy - 1)) | ((c >= ny + ny // 2) & (gy > 0))
        return (in_x & in_y).astype(F32)

    zero_plane = jnp.zeros((rows, lanes), F32)
    for edge in (0, 2 * nz + 1):
        div[edge] = zero_plane
        for c in range(3):
            w1[c, edge] = zero_plane
            w2[c, edge] = zero_plane
    blocks, epochs, pixels = observed_ref.shape
    for fetch in fetches[1:9]:
        fetch.wait()

    for b in range(blocks):
        for k, source in enumerate((count_ref, table_ref, patch_ref, owner_ref)):
            numbers[k, b:b + 1, :] = jnp.full((1, ny), source[b], jnp.int32)
    in_scene = iota((blocks, ny), 1)
    for k in range(0, pixels, ny):
        kept = (in_scene + k < numbers[0]).astype(F32)
        valid[:, k:k + ny] = coherence_ref[:, k:k + ny].astype(F32) * kept
    for b in range(blocks):
        resid[epochs * b:epochs * (b + 1), :] = (predicted_ref[b] - observed_ref[b]) * valid[b:b + 1, :]
    res = resid[...]
    row_block, row_place = iota((blocks, epochs * blocks), 0), iota((blocks, epochs * blocks), 1)
    own_rows = row_place // epochs == row_block
    for c in range(3):
        mix = jnp.zeros((blocks, epochs * blocks), F32)
        for e in range(epochs):
            mix = jnp.where(own_rows & (row_place % epochs == e), look_ref[e, c], mix)
        coeffs[c * blocks:(c + 1) * blocks, :] = jnp.dot(
            mix, res, precision=HIGHEST, preferred_element_type=F32
        )
    mass = jnp.sum(jnp.sum(res * res, axis=0, keepdims=True), axis=1, keepdims=True)
    weight = jnp.sum(jnp.sum(valid[...], axis=0, keepdims=True), axis=1, keepdims=True)

    lane_owner = iota((blocks, owners), 1)
    at_owner = (lane_owner == numbers[3, :, 0:owners]).astype(F32)
    before = (iota((blocks, blocks), 1) < iota((blocks, blocks), 0)).astype(F32)
    ahead_of = jnp.dot(before, at_owner, preferred_element_type=F32)
    rank = jnp.sum(ahead_of * at_owner, axis=1, keepdims=True).astype(jnp.int32)
    slot_of = numbers[3, :, 0:1] * CAP + rank
    select = (iota((blocks, owners * CAP), 1) == slot_of).astype(F32)
    at_lane = (iota((blocks, ny), 1) == rank * (ny // CAP) + numbers[2]).astype(F32)
    marks = lax.dot_general(at_owner, at_lane, (((0,), (0,)), ((), ())), preferred_element_type=F32)
    for o in range(owners):
        choice_ref[o] = marks[o:o + 1]

    rounded = coeffs[...].astype(jnp.bfloat16).astype(F32)
    which = jnp.concatenate([numbers[1]] * 3, axis=0)
    which = jnp.concatenate([which] * (pixels // ny), axis=1)
    fetches[9].wait()
    total_sums = jnp.zeros((3 * blocks, ny), F32)
    for t in range(weights.shape[0]):
        taken = jnp.where(which == t, rounded, 0.0).astype(jnp.bfloat16)
        total_sums = total_sums + jnp.dot(taken, weights[t], preferred_element_type=F32)
    for c in range(3):
        chosen = lax.dot_general(
            select, total_sums[c * blocks:(c + 1) * blocks], (((0,), (0,)), ((), ())),
            precision=HIGHEST, preferred_element_type=F32,
        )
        for o in range(owners):
            slots_ref[o, c] = chosen[CAP * o:CAP * (o + 1)]

    fetches[10].wait()
    pl.semaphore_wait(barrier, (ngx - 1) * ngy + len(peers))

    def remote(source, target, index, device, arrival=None):
        return pltpu.make_async_remote_copy(
            src_ref=source, dst_ref=target, send_sem=send_sem.at[index],
            recv_sem=recv_sem.at[index if arrival is None else arrival],
            device_id=device, device_id_type=pl.DeviceIdType.MESH,
        )

    def post(j, first):
        for k in range(first, ngy):
            y = wrap(gy + k, ngy)
            o = j * ngy + y
            for message, (source, target) in enumerate(((slots_ref, got_slots), (choice_ref, got_choice))):
                pltpu.make_async_remote_copy(
                    src_ref=source.at[o], dst_ref=target.at[me],
                    send_sem=send_a2a.at[message], recv_sem=recv_a2a.at[message],
                    device_id=at(j, y, gz), device_id_type=pl.DeviceIdType.MESH,
                ).start()

    def post_pair(i, carry):
        d = ngx // 2 - i
        post(wrap(gx - d, ngx), 0)

        @pl.when(d < ngx // 2)
        def _():
            post(wrap(gx + d, ngx), 0)

        return carry

    lax.fori_loop(0, ngx // 2, post_pair, 0)
    post(gx, 1)

    x_up, x_down = wrap(gx + 1, ngx), wrap(gx - 1, ngx)
    y_up, y_down = wrap(gy + 1, ngy), wrap(gy - 1, ngy)
    to_down = remote(stiff_ref.at[:, pl.ds(0, 8), :], stiff_x.at[0], 0, at(x_down, gy, gz))
    to_up = remote(stiff_ref.at[:, pl.ds(nx - 8, 8), :], stiff_x.at[1], 1, at(x_up, gy, gz))
    to_other = remote(depths.at[own_layers, :], depths.at[own_layers, :], 2, at(gx, gy, other))
    to_other.start()

    to_down.start()
    to_up.start()
    got_slots[me] = slots_ref[me]
    got_choice[me] = choice_ref[me]

    to_down.wait()
    to_up.wait()
    to_other.wait()
    low = iota((8, ny), 0) < 4
    for z in range(nz):
        wide_stiff[z, 0:nx, :] = stiff_ref[z]
        wide_stiff[z, nx:rows, :] = jnp.where(low, stiff_x[0, z], stiff_x[1, z])
    turned = wide_stiff[...].reshape(nz * rows, ny).T
    strip_out[0] = turned[0:8]
    strip_out[1] = turned[ny - 8:ny]
    strips = [
        remote(strip_out.at[0], strip_in.at[0], 3, at(gx, y_down, gz)),
        remote(strip_out.at[1], strip_in.at[1], 4, at(gx, y_up, gz)),
    ]
    for copy in strips:
        copy.start()

    d = depths[...]
    where_z = iota(d.shape, 0)
    inside = ((where_z >= 8) & (where_z < 8 + 2 * nz)).astype(F32)
    d_up, d_down = ahead(d, 0), behind(d, 0)
    q = 0.5 * (d_up - d_down)
    kept_d, kept_q = inside * d, inside * q
    columns = (
        d,
        0.125 * (d_up + d_down),
        q,
        (1.0 / 32.0) * (ahead(kept_d, 0) - behind(kept_d, 0)),
        (1.0 / 32.0) * (ahead(kept_q, 0) - behind(kept_q, 0)),
    )
    for k, values in enumerate(columns):
        for z in range(2 * nz):
            table[k, z] = values[z + 8:z + 9]

    for copy in strips:
        copy.wait()
    filler = jnp.zeros((ny - 16, nz * rows), F32)
    beside = jnp.concatenate([strip_in[0], filler, strip_in[1]], axis=0).T.reshape(nz, rows, ny)
    base = nz * gz
    for z in range(nz):
        coef[base + z, :, 0:ny] = 0.125 * wide_stiff[z] - 0.25
        coef[base + z, :, ny:lanes] = 0.125 * beside[z] - 0.25
    passed = pl.ds((nz - 4) + 4 * gz, 4)
    layers = remote(coef.at[passed], coef.at[passed], 5, at(gx, gy, other))
    layers.start()

    for message, buffer in enumerate((slots_ref, choice_ref)):
        part = buffer.at[pl.ds(0, owners - 1)]
        pltpu.make_async_copy(part, part, send_a2a.at[message]).wait()
    for message, buffer in enumerate((got_slots, got_choice)):
        part = buffer.at[pl.ds(0, owners - 1)]
        pltpu.make_async_copy(part, part, recv_a2a.at[message]).wait()
    own_slot = iota((CAP, ny), 1) // (ny // CAP) == iota((CAP, ny), 0)
    for o in range(owners):
        for c in range(3):
            flat_slots[c, CAP * o:CAP * (o + 1), :] = got_slots[o, c]
        flat_choice[CAP * o:CAP * (o + 1), :] = jnp.where(own_slot, got_choice[o], 0.0)
    picked = flat_choice[...]
    tiles = []
    for c in range(3):
        spread = lax.dot_general(
            picked, flat_slots[c], (((0,), (0,)), ((), ())), precision=HIGHEST, preferred_element_type=F32
        )
        depth_places = ny // CAP
        placed = spread[0:depth_places]
        for j in range(1, CAP):
            placed = placed + spread[j * depth_places:(j + 1) * depth_places]
        tiles.append(placed)
    tile = jnp.concatenate(tiles, axis=0)
    sub = lax.rem(iota(tile.shape, 0), 8)
    chunk = iota(tile.shape, 1) // PATCH_Y
    for bit in (1, 2, 4):
        row_set, chunk_set = (sub // bit) % 2 == 1, (chunk // bit) % 2 == 1
        from_below = roll(roll(tile, -bit, 0), bit * PATCH_Y, 1)
        from_above = roll(roll(tile, bit, 0), -bit * PATCH_Y, 1)
        tile = jnp.where(row_set == chunk_set, tile, jnp.where(row_set, from_above, from_below))
    surf[...] = tile.reshape(3, nx, ny)
    turned = jnp.concatenate([tile, jnp.zeros((ny - 3 * nx, ny), F32)], axis=0).T
    border[0] = turned[0:8]
    border[1] = turned[ny - 8:ny]

    swap = remote(surf, surf_other, 6, at(gx, gy, other))
    swap.start()
    first, last = pl.ds(0, 8), pl.ds(nx - 8, 8)
    ways = (
        (surf.at[:, first, :], halo_x, 0, x_down, gy),
        (surf.at[:, last, :], halo_x, 1, x_up, gy),
        (border.at[0], halo_y, 0, gx, y_down),
        (border.at[1], halo_y, 1, gx, y_up),
        (border.at[0], halo_y, 2, x_down, y_down),
        (border.at[1], halo_y, 3, x_down, y_up),
        (border.at[0], halo_y, 4, x_up, y_down),
        (border.at[1], halo_y, 5, x_up, y_up),
    )
    count = len(ways)
    started = []
    for k in reversed(range(count)):
        source, target, place, x, y = ways[k]
        for i, z in enumerate((gz, other)):
            copy = remote(source, target.at[gz, place], 7 + i * count + k, at(x, y, z), 7 + gz * count + k)
            copy.start()
            started.append(copy)
    swap.wait()
    for k, (source, target, place, x, y) in enumerate(ways):
        for i in range(2):
            remote(source, target.at[i, place], 7 + i * count + k, at(x, y, gz)).wait_recv()
    for copy in started:
        copy.wait_send()
    mask_tall = domain(tall)
    mask = domain(rows)
    low_rows = iota((8, lanes), 0) < 4

    def packed(values):
        return jnp.concatenate(
            [values[0:nx], jnp.where(low_rows, values[nx:nx + 8], values[nx + 8:nx + 16])], axis=0
        )

    blank = jnp.zeros((ny - 16, ny), F32)

    def columns_of(place):
        low_side, high_side = halo_y[0, place] + halo_y[1, place], halo_y[0, place + 1] + halo_y[1, place + 1]
        return jnp.concatenate([low_side, blank, high_side], axis=0).T[0:3 * nx].reshape(3, nx, ny)

    near, upper, lower = columns_of(0), columns_of(2), columns_of(4)
    around = []
    for c in range(3):
        main = jnp.concatenate(
            [surf[c] + surf_other[c], halo_x[0, 0, c] + halo_x[1, 0, c], halo_x[0, 1, c] + halo_x[1, 1, c]], axis=0
        )
        side = jnp.concatenate([near[c], upper[c, 0:8], lower[c, nx - 8:nx]], axis=0)
        around.append(mask_tall * jnp.concatenate([main, side], axis=1))
    flux = mask_tall * (
        0.5 * ((ahead(around[0], 0) - behind(around[0], 0)) + (ahead(around[1], 1) - behind(around[1], 1)))
    )
    for c in range(3):
        s = around[c]
        beside_xy = (ahead(s, 0) + behind(s, 0)) + (ahead(s, 1) + behind(s, 1))
        fields[c] = packed(s)
        if c < 2:
            drop = 0.125 * beside_xy + (1.0 / 32.0) * (ahead(flux, c) - behind(flux, c))
            fields[3 + c] = mask * packed(drop)
            fields[6 + c] = mask * packed((1.0 / 32.0) * (ahead(around[2], c) - behind(around[2], c)))
        else:
            fields[3 + c] = mask * packed(0.125 * beside_xy)
    fields[8] = packed(flux)

    layers.wait()

    def first_layer(i, carry):
        z = (nz - 4) * gz + i
        value = [table[k, z] for k in range(5)]
        own = coef[z] * value[0] - value[1]
        for c in range(2):
            w1[c, z + 1] = mask * (fields[c] * own) - value[0] * fields[3 + c] - value[2] * fields[6 + c]
        w1[2, z + 1] = mask * (fields[2] * (own - value[4])) - value[0] * fields[5] - value[3] * fields[8]
        return carry

    lax.fori_loop(0, nz + 4, first_layer, 0)

    def spread_of(source, start, amount):
        def layer(i, carry):
            z = start + i
            x, y = source[0, z + 1], source[1, z + 1]
            div[z + 1] = mask * (
                ((ahead(x, 0) - behind(x, 0)) + (ahead(y, 1) - behind(y, 1)))
                + (source[2, z + 2] - source[2, z])
            )
            return carry

        lax.fori_loop(0, amount, layer, 0)

    spread_of(w1, (nz - 3) * gz, nz + 3)

    def second_layer(i, carry):
        z = (nz - 2) * gz + i
        own = coef[z]
        here = div[z + 1]
        for c in range(3):
            v = w1[c, z + 1]
            total = (ahead(v, 0) + behind(v, 0)) + (ahead(v, 1) + behind(v, 1))
            total = total + (w1[c, z + 2] + w1[c, z])
            slope = (ahead(here, c) - behind(here, c)) if c < 2 else (div[z + 2] - div[z])
            w2[c, z + 1] = mask * (own * v - 0.125 * total - (1.0 / 64.0) * slope)
        return carry

    lax.fori_loop(0, nz + 2, second_layer, 0)

    spread_of(w2, (nz - 1) * gz, nz + 1)

    def folded(values):
        total = values[0:8]
        for k in range(8, nx, 8):
            total = total + values[k:k + 8]
        return total

    def gather_moments(i, sums):
        z = nz * gz + i
        own = coef[z, 0:nx, 0:ny]
        d_now = table[0, z, :, 0:ny]
        here = div[z + 1, 0:nx, 0:ny]
        terms = [None] * MOMENTS
        terms[MOMENTS - 1] = (1.0 / 64.0) * (here * here)
        for c in range(3):
            v = w2[c, z + 1, 0:nx, 0:ny]
            total = ahead(w2[c, z + 1, :, 0:ny], 0)[0:nx] + ahead(w2[c, z + 1, 0:nx, :], 1)[:, 0:ny]
            total = total + w2[c, z + 2, 0:nx, 0:ny]
            zeroth = d_now * fields[c, 0:nx, 0:ny]
            one = w1[c, z + 1, 0:nx, 0:ny]
            for k, term in enumerate(
                (zeroth * zeroth, zeroth * one, one * one, one * v, v * v, v * (own * v - 0.25 * total))
            ):
                terms[k] = term if terms[k] is None else terms[k] + term
        return tuple(s + folded(t) for s, t in zip(sums, terms))

    sums = lax.fori_loop(0, nz, gather_moments, tuple(jnp.zeros((8, ny), F32) for _ in range(MOMENTS)))

    def third_layer(i, carry):
        z = nz * gz + i
        own = coef[z, 0:nx, 0:ny]
        here_x, here_y = div[z + 1, :, 0:ny], div[z + 1, 0:nx, :]
        for c in range(3):
            v = w2[c, z + 1, 0:nx, 0:ny]
            vx, vy = w2[c, z + 1, :, 0:ny], w2[c, z + 1, 0:nx, :]
            total = (ahead(vx, 0) + behind(vx, 0))[0:nx] + (ahead(vy, 1) + behind(vy, 1))[:, 0:ny]
            total = total + (w2[c, z + 2, 0:nx, 0:ny] + w2[c, z, 0:nx, 0:ny])
            if c == 0:
                slope = (ahead(here_x, 0) - behind(here_x, 0))[0:nx]
            elif c == 1:
                slope = (ahead(here_y, 1) - behind(here_y, 1))[:, 0:ny]
            else:
                slope = div[z + 2, 0:nx, 0:ny] - div[z, 0:nx, 0:ny]
            res_ref[c, i] = own * v - 0.125 * total - (1.0 / 64.0) * slope
        return carry

    early_layers = (3 * nz) // 8

    lane = iota((1, ny), 1)
    message = jnp.where(lane == MOMENTS, mass, 0.0) + jnp.where(lane == MOMENTS + 1, weight, 0.0)
    for k in range(MOMENTS):
        amount = jnp.sum(jnp.sum(sums[k], axis=0, keepdims=True), axis=1, keepdims=True)
        message = message + jnp.where(lane == k, amount, 0.0)
    row_out[0] = message
    slot = gy * 2 + gz
    row_in[slot] = message
    base = 7 + 2 * count
    started = []
    for k, (y, z) in enumerate(peers):
        copy = remote(row_out.at[0], row_in.at[slot], base + k, at(gx, y, z))
        copy.start()
        started.append(copy)
    lax.fori_loop(0, early_layers, third_layer, 0)
    for copy in started:
        copy.wait()
    message = row_in[0]
    for k in range(1, 2 * ngy):
        message = message + row_in[k]
    row_out[1] = message
    ring_in[gx] = message
    first_index = base + len(peers)
    started = []
    for k in range(1, ngx):
        copy = remote(row_out.at[1], ring_in.at[gx], first_index + k - 1, at(wrap(gx + k, ngx), gy, gz))
        copy.start()
        started.append(copy)
    lax.fori_loop(early_layers, nz, third_layer, 0)
    for copy in started:
        copy.wait()
    message = ring_in[0]
    for k in range(1, ngx):
        message = message + ring_in[k]
    parts = [jnp.sum(jnp.where(lane == k, message, 0.0), axis=1, keepdims=True) for k in range(MOMENTS + 2)]

    scale = lax.rsqrt(parts[MOMENTS] / (EPOCHS * parts[MOMENTS + 1]) + EPS) * (1.0 / PRE)
    iterate, residual = conjugate(parts[0:MOMENTS])
    iterate = [scale * value for value in iterate]
    residual = [scale * value for value in residual]

    def finish(i, carry):
        z = nz * gz + i
        d_now = table[0, z, :, 0:ny]
        for c in range(3):
            zeroth = d_now * fields[c, 0:nx, 0:ny]
            one, two = w1[c, z + 1, 0:nx, 0:ny], w2[c, z + 1, 0:nx, 0:ny]
            third = res_ref[c, i]
            adj_ref[c, i] = iterate[0] * zeroth + iterate[1] * one + iterate[2] * two
            res_ref[c, i] = residual[0] * zeroth + residual[1] * one + residual[2] * two + residual[3] * third
        return carry

    lax.fori_loop(0, nz, finish, 0)


def per_device(
    observed,
    predicted,
    coherence_mask,
    block_count,
    block_owner,
    block_matrix_choice,
    block_patch,
    look_vector,
    interp_weights,
    depth_kernel,
    stiffness,
):
    blocks, epochs, pixels = observed.shape
    cells = PATCH_X * PATCH_Y
    ngx, ngy = lax.axis_size("gx"), lax.axis_size("gy")
    owners = ngx * ngy
    nz, nx, ny = stiffness.shape

    rows, lanes = nx + 8, 2 * ny
    out = pltpu.VMEM((3, nz, nx, ny), F32)
    vmem = pl.BlockSpec(memory_space=pltpu.VMEM)
    far = pl.BlockSpec(memory_space=pltpu.HBM)
    copies = 23 + (2 * ngy - 1) + (ngx - 1)
    return pl.pallas_call(
        kernel,
        out_shape=(out, out),
        in_specs=[far] * 11,
        out_specs=(vmem, vmem),
        scratch_shapes=[
            pltpu.VMEM(observed.shape, F32),
            pltpu.VMEM(predicted.shape, F32),
            pltpu.VMEM(coherence_mask.shape, jnp.int32),
            pltpu.SMEM((blocks,), jnp.int32),
            pltpu.SMEM((blocks,), jnp.int32),
            pltpu.SMEM((blocks,), jnp.int32),
            pltpu.SMEM((blocks,), jnp.int32),
            pltpu.SMEM(look_vector.shape, F32),
            pltpu.VMEM(interp_weights.shape, interp_weights.dtype),
            pltpu.SMEM((nz,), F32),
            pltpu.VMEM(stiffness.shape, F32),
            pltpu.VMEM((4, blocks, ny), jnp.int32),
            pltpu.VMEM((blocks, pixels), F32),
            pltpu.VMEM((epochs * blocks, pixels), F32),
            pltpu.VMEM((3 * blocks, pixels), F32),
            pltpu.VMEM((owners, 3, CAP, cells), F32),
            pltpu.VMEM((owners, 1, cells), F32),
            pltpu.VMEM((owners, 3, CAP, cells), F32),
            pltpu.VMEM((owners, 1, cells), F32),
            pltpu.VMEM((3, owners * CAP, cells), F32),
            pltpu.VMEM((owners * CAP, cells), F32),
            pltpu.VMEM((3, nx, ny), F32),
            pltpu.VMEM((3, nx, ny), F32),
            pltpu.VMEM((2, 8, ny), F32),
            pltpu.VMEM((2, 2, 3, 8, ny), F32),
            pltpu.VMEM((2, 6, 8, ny), F32),
            pltpu.VMEM((2, nz, 8, ny), F32),
            pltpu.VMEM((nz, rows, ny), F32),
            pltpu.VMEM((2, 8, nz * rows), F32),
            pltpu.VMEM((2, 8, nz * rows), F32),
            pltpu.VMEM((2 * nz, rows, lanes), F32),
            pltpu.VMEM((2 * nz + 16, lanes), F32),
            pltpu.VMEM((5, 2 * nz, 1, lanes), F32),
            pltpu.VMEM((9, rows, lanes), F32),
            pltpu.VMEM((3, 2 * nz + 2, rows, lanes), F32),
            pltpu.VMEM((3, 2 * nz + 2, rows, lanes), F32),
            pltpu.VMEM((2 * nz + 2, rows, lanes), F32),
            pltpu.VMEM((2, 1, ny), F32),
            pltpu.VMEM((2 * ngy, 1, ny), F32),
            pltpu.VMEM((ngx, 1, ny), F32),
            pltpu.SemaphoreType.DMA((2,)),
            pltpu.SemaphoreType.DMA((2,)),
            pltpu.SemaphoreType.DMA((copies,)),
            pltpu.SemaphoreType.DMA((copies,)),
            pltpu.SemaphoreType.DMA((11,)),
        ],
        compiler_params=pltpu.CompilerParams(
            collective_id=0, has_side_effects=True, vmem_limit_bytes=60000000
        ),
    )(
        observed, predicted, coherence_mask, block_count, block_owner[:, 0], block_matrix_choice, block_patch,
        look_vector, interp_weights, depth_kernel, stiffness,
    )


def solution(mesh):
    in_specs = (
        P(("grp", "gx", "gy", "gz"), None, None),
        P(("grp", "gx", "gy", "gz"), None, None),
        P(("grp", "gx", "gy", "gz"), None),
        P(("grp", "gx", "gy", "gz")),
        P(("grp", "gx", "gy", "gz"), None),
        P(("grp", "gx", "gy", "gz")),
        P(("grp", "gx", "gy", "gz")),
        P(),
        P(),
        P(("grp", "gz")),
        P(("grp", "gz"), "gx", "gy"),
    )
    out_specs = (P(None, ("grp", "gz"), "gx", "gy"), P(None, ("grp", "gz"), "gx", "gy"))
    return jax.shard_map(
        per_device, mesh=mesh, in_specs=in_specs, out_specs=out_specs, check_vma=False
    )
```

```python
import jax
import jax.numpy as jnp
from jax import lax
from jax.experimental import pallas as pl
from jax.experimental.pallas import tpu as pltpu
from jax.sharding import PartitionSpec as P

EPOCHS = 4
PATCH_X = 8
PATCH_Y = 16
CAP = 4
EPS = 1e-06

SHIFT = 8.0
PRE = 1024.0
MOMENTS = 6

HIGHEST = lax.Precision.HIGHEST
F32 = jnp.float32


def roll(values, shift, axis):
    return pltpu.roll(values, shift % values.shape[axis], axis)


def ahead(values, axis):
    return roll(values, -1, axis)


def behind(values, axis):
    return roll(values, 1, axis)


def iota(shape, axis):
    return lax.broadcasted_iota(jnp.int32, shape, axis)


def pairwise(start, stop, body):
    def trip(k, carry):
        body(start + 2 * k, None)
        body(start + 2 * k + 1, None)
        return carry

    lax.fori_loop(0, (stop - start) // 2, trip, 0)
    if (stop - start) % 2:
        body(stop - 1, None)


def product(first, second, moments):
    total = None
    for i, f in enumerate(first):
        for j, g in enumerate(second):
            term = f * g * moments[i + j]
            total = term if total is None else total + term
    return total


def combined(first, factor, second):
    size = max(len(first), len(second))
    out = []
    for i in range(size):
        value = first[i] if i < len(first) else None
        if i < len(second):
            term = factor * second[i]
            value = term if value is None else value + term
        out.append(value)
    return out


def applied(poly):
    out = []
    for i in range(len(poly) + 1):
        value = None
        for j in (i, i - 1):
            if 0 <= j < len(poly):
                value = poly[j] if value is None else value + poly[j]
        out.append(SHIFT * value)
    return out


def conjugate(moments):
    one = jnp.ones_like(moments[0])
    residual, direction, iterate = [one], [one], []
    now = moments[0]
    for step in range(3):
        image = applied(direction)
        alpha = now / product(direction, image, moments)
        scaled = [alpha * d for d in direction]
        iterate = scaled if not iterate else combined(iterate, one, scaled)
        residual = combined(residual, -alpha, image)
        if step < 2:
            new = product(residual, residual, moments)
            direction = combined(residual, new / now, direction)
            now = new
    return iterate, residual


def kernel(
    observed_hbm, predicted_hbm, coherence_hbm, count_hbm, owner_hbm, table_hbm, patch_hbm, look_hbm,
    weights_hbm, depth_hbm, stiff_hbm,
    adj_ref, res_ref,
    observed_ref, predicted_ref, coherence_ref, count_ref, owner_ref, table_ref, patch_ref, look_ref,
    weights, depth_ref, stiff_ref,
    numbers, valid, resid, coeffs, slots_ref, choice_ref,
    got_slots, got_choice, flat_slots, flat_choice,
    surf, surf_other, border, halo_x, halo_y,
    stiff_x, wide_stiff, strip_out, strip_in, coef,
    depths, table,
    fields, w1, w2, div,
    row_out, row_in, ring_in,
    send_a2a, recv_a2a, send_sem, recv_sem, local_sem,
):
    pairs = (
        (depth_hbm, depth_ref), (count_hbm, count_ref), (owner_hbm, owner_ref), (table_hbm, table_ref),
        (patch_hbm, patch_ref), (look_hbm, look_ref), (coherence_hbm, coherence_ref),
        (predicted_hbm, predicted_ref), (observed_hbm, observed_ref), (weights_hbm, weights), (stiff_hbm, stiff_ref),
    )
    fetches = [pltpu.make_async_copy(a, b, local_sem.at[i]) for i, (a, b) in enumerate(pairs)]
    for fetch in fetches:
        fetch.start()
    gx, gy, gz = lax.axis_index("gx"), lax.axis_index("gy"), lax.axis_index("gz")
    ngx, ngy = lax.axis_size("gx"), lax.axis_size("gy")
    owners = ngx * ngy
    me = gx * ngy + gy
    nz, nx, ny = stiff_ref.shape
    other = 1 - gz
    rows, lanes = nx + 8, 2 * ny
    tall = nx + 16

    def at(x, y, z):
        return {"gx": x, "gy": y, "gz": z}

    def wrap(value, count):
        return lax.rem(value + count, count)

    depths[...] = jnp.zeros(depths.shape, F32)
    own_layers = pl.ds(pl.multiple_of(8 + nz * gz, 8), nz)
    fetches[0].wait()
    layer = iota((nz, lanes), 0)
    own_depths = jnp.zeros((nz, lanes), F32)
    for z in range(nz):
        own_depths = jnp.where(layer == z, PRE * depth_ref[z], own_depths)
    depths[own_layers, :] = own_depths

    barrier = pltpu.get_barrier_semaphore()
    peers = [(wrap(gy + k, ngy), gz) for k in range(1, ngy)] + [(wrap(gy + k, ngy), other) for k in range(ngy)]

    def greet(k, carry):
        j = wrap(gx - k, ngx)
        for y in range(ngy):
            pl.semaphore_signal(barrier, inc=1, device_id=at(j, y, gz))
        return carry

    lax.fori_loop(1, ngx, greet, 0)
    for y, z in peers:
        pl.semaphore_signal(barrier, inc=1, device_id=at(gx, y, z))

    def domain(count):
        r, c = iota((count, lanes), 0), iota((count, lanes), 1)
        half = (count - nx) // 2
        in_x = (r < nx) | ((r < nx + half) & (gx < ngx - 1)) | ((r >= nx + half) & (gx > 0))
        in_y = (c < ny) | ((c < ny + ny // 2) & (gy < ngy - 1)) | ((c >= ny + ny // 2) & (gy > 0))
        return (in_x & in_y).astype(F32)

    zero_plane = jnp.zeros((rows, lanes), F32)
    for edge in (0, 2 * nz + 1):
        div[edge] = zero_plane
        for c in range(3):
            w1[c, edge] = zero_plane
            w2[c, edge] = zero_plane
    blocks, epochs, pixels = observed_ref.shape
    for fetch in fetches[1:9]:
        fetch.wait()

    for b in range(blocks):
        for k, source in enumerate((count_ref, table_ref, patch_ref, owner_ref)):
            numbers[k, b:b + 1, :] = jnp.full((1, ny), source[b], jnp.int32)
    in_scene = iota((blocks, ny), 1)
    for k in range(0, pixels, ny):
        kept = (in_scene + k < numbers[0]).astype(F32)
        valid[:, k:k + ny] = coherence_ref[:, k:k + ny].astype(F32) * kept
    for b in range(blocks):
        resid[epochs * b:epochs * (b + 1), :] = (predicted_ref[b] - observed_ref[b]) * valid[b:b + 1, :]
    res = resid[...]
    row_block, row_place = iota((blocks, epochs * blocks), 0), iota((blocks, epochs * blocks), 1)
    own_rows = row_place // epochs == row_block
    mixes = []
    for c in range(3):
        mix = jnp.zeros((blocks, epochs * blocks), F32)
        for e in range(epochs):
            mix = jnp.where(own_rows & (row_place % epochs == e), look_ref[e, c], mix)
        mixes.append(mix)
    coeffs[...] = jnp.dot(
        jnp.concatenate(mixes, axis=0), res, precision=HIGHEST, preferred_element_type=F32
    )
    mass = jnp.sum(jnp.sum(res * res, axis=0, keepdims=True), axis=1, keepdims=True)
    weight = jnp.sum(jnp.sum(valid[...], axis=0, keepdims=True), axis=1, keepdims=True)

    lane_owner = iota((blocks, owners), 1)
    at_owner = (lane_owner == numbers[3, :, 0:owners]).astype(F32)
    before = (iota((blocks, blocks), 1) < iota((blocks, blocks), 0)).astype(F32)
    ahead_of = jnp.dot(before, at_owner, preferred_element_type=F32)
    rank = jnp.sum(ahead_of * at_owner, axis=1, keepdims=True).astype(jnp.int32)
    slot_of = numbers[3, :, 0:1] * CAP + rank
    select = (iota((blocks, owners * CAP), 1) == slot_of).astype(F32)
    at_lane = (iota((blocks, ny), 1) == rank * (ny // CAP) + numbers[2]).astype(F32)
    marks = lax.dot_general(at_owner, at_lane, (((0,), (0,)), ((), ())), preferred_element_type=F32)
    for o in range(owners):
        choice_ref[o] = marks[o:o + 1]

    rounded = coeffs[...].astype(jnp.bfloat16).astype(F32)
    which = jnp.concatenate([numbers[1]] * 3, axis=0)
    which = jnp.concatenate([which] * (pixels // ny), axis=1)
    fetches[9].wait()
    total_sums = jnp.zeros((3 * blocks, ny), F32)
    for t in range(weights.shape[0]):
        taken = jnp.where(which == t, rounded, 0.0).astype(jnp.bfloat16)
        total_sums = total_sums + jnp.dot(taken, weights[t], preferred_element_type=F32)
    chosen = lax.dot_general(
        select, jnp.concatenate([total_sums[c * blocks:(c + 1) * blocks] for c in range(3)], axis=1),
        (((0,), (0,)), ((), ())), precision=HIGHEST, preferred_element_type=F32,
    )
    for c in range(3):
        for o in range(owners):
            slots_ref[o, c] = chosen[CAP * o:CAP * (o + 1), c * ny:(c + 1) * ny]

    fetches[10].wait()
    pl.semaphore_wait(barrier, (ngx - 1) * ngy + len(peers))

    def remote(source, target, index, device, arrival=None):
        return pltpu.make_async_remote_copy(
            src_ref=source, dst_ref=target, send_sem=send_sem.at[index],
            recv_sem=recv_sem.at[index if arrival is None else arrival],
            device_id=device, device_id_type=pl.DeviceIdType.MESH,
        )

    x_up, x_down = wrap(gx + 1, ngx), wrap(gx - 1, ngx)
    y_up, y_down = wrap(gy + 1, ngy), wrap(gy - 1, ngy)
    to_down = remote(stiff_ref.at[:, pl.ds(0, 8), :], stiff_x.at[0], 0, at(x_down, gy, gz))
    to_up = remote(stiff_ref.at[:, pl.ds(nx - 8, 8), :], stiff_x.at[1], 1, at(x_up, gy, gz))
    to_other = remote(depths.at[own_layers, :], depths.at[own_layers, :], 2, at(gx, gy, other))
    to_other.start()

    to_down.start()
    to_up.start()
    def post(j, first):
        for k in range(first, ngy):
            y = wrap(gy + k, ngy)
            o = j * ngy + y
            for message, (source, target) in enumerate(((slots_ref, got_slots), (choice_ref, got_choice))):
                pltpu.make_async_remote_copy(
                    src_ref=source.at[o], dst_ref=target.at[me],
                    send_sem=send_a2a.at[message], recv_sem=recv_a2a.at[message],
                    device_id=at(j, y, gz), device_id_type=pl.DeviceIdType.MESH,
                ).start()

    def post_pair(i, carry):
        d = ngx // 2 - i
        post(wrap(gx - d, ngx), 0)

        @pl.when(d < ngx // 2)
        def _():
            post(wrap(gx + d, ngx), 0)

        return carry

    lax.fori_loop(0, ngx // 2, post_pair, 0)
    post(gx, 1)

    got_slots[me] = slots_ref[me]
    got_choice[me] = choice_ref[me]

    to_down.wait_recv()
    to_up.wait_recv()
    to_other.wait_recv()
    sent = [to_down, to_up, to_other]
    low = iota((8, ny), 0) < 4
    for z in range(nz):
        wide_stiff[z, 0:nx, :] = stiff_ref[z]
        wide_stiff[z, nx:rows, :] = jnp.where(low, stiff_x[0, z], stiff_x[1, z])
    turned = wide_stiff[...].reshape(nz * rows, ny).T
    strip_out[0] = turned[0:8]
    strip_out[1] = turned[ny - 8:ny]
    strips = [
        remote(strip_out.at[0], strip_in.at[0], 3, at(gx, y_down, gz)),
        remote(strip_out.at[1], strip_in.at[1], 4, at(gx, y_up, gz)),
    ]
    for copy in strips:
        copy.start()

    d = depths[...]
    where_z = iota(d.shape, 0)
    inside = ((where_z >= 8) & (where_z < 8 + 2 * nz)).astype(F32)
    d_up, d_down = ahead(d, 0), behind(d, 0)
    q = 0.5 * (d_up - d_down)
    kept_d, kept_q = inside * d, inside * q
    columns = (
        d,
        0.125 * (d_up + d_down),
        q,
        (1.0 / 32.0) * (ahead(kept_d, 0) - behind(kept_d, 0)),
        (1.0 / 32.0) * (ahead(kept_q, 0) - behind(kept_q, 0)),
    )
    for k, values in enumerate(columns):
        for z in range(2 * nz):
            table[k, z] = values[z + 8:z + 9]

    for copy in strips:
        copy.wait_recv()
    sent = sent + strips
    filler = jnp.zeros((ny - 16, nz * rows), F32)
    beside = jnp.concatenate([strip_in[0], filler, strip_in[1]], axis=0).T.reshape(nz, rows, ny)
    base = nz * gz
    for z in range(nz):
        coef[base + z, :, 0:ny] = 0.125 * wide_stiff[z] - 0.25
        coef[base + z, :, ny:lanes] = 0.125 * beside[z] - 0.25
    passed = pl.ds((nz - 4) + 4 * gz, 4)
    layers = remote(coef.at[passed], coef.at[passed], 5, at(gx, gy, other))
    layers.start()

    for message, buffer in enumerate((got_slots, got_choice)):
        part = buffer.at[pl.ds(0, owners - 1)]
        pltpu.make_async_copy(part, part, recv_a2a.at[message]).wait()
    own_slot = iota((CAP, ny), 1) // (ny // CAP) == iota((CAP, ny), 0)
    for o in range(owners):
        for c in range(3):
            flat_slots[CAP * o:CAP * (o + 1), c * ny:(c + 1) * ny] = got_slots[o, c]
        flat_choice[CAP * o:CAP * (o + 1), :] = jnp.where(own_slot, got_choice[o], 0.0)
    picked = flat_choice[...]
    spread = lax.dot_general(
        picked, flat_slots[...], (((0,), (0,)), ((), ())), precision=HIGHEST, preferred_element_type=F32
    )
    depth_places = ny // CAP
    tiles = []
    for c in range(3):
        placed = spread[0:depth_places, c * ny:(c + 1) * ny]
        for j in range(1, CAP):
            placed = placed + spread[j * depth_places:(j + 1) * depth_places, c * ny:(c + 1) * ny]
        tiles.append(placed)
    tile = jnp.concatenate(tiles, axis=0)
    sub = lax.rem(iota(tile.shape, 0), 8)
    chunk = iota(tile.shape, 1) // PATCH_Y
    for bit in (1, 2, 4):
        row_set, chunk_set = (sub // bit) % 2 == 1, (chunk // bit) % 2 == 1
        from_below = roll(roll(tile, -bit, 0), bit * PATCH_Y, 1)
        from_above = roll(roll(tile, bit, 0), -bit * PATCH_Y, 1)
        tile = jnp.where(row_set == chunk_set, tile, jnp.where(row_set, from_above, from_below))
    surf[...] = tile.reshape(3, nx, ny)
    turned = jnp.concatenate([tile, jnp.zeros((ny - 3 * nx, ny), F32)], axis=0).T
    border[0] = turned[0:8]
    border[1] = turned[ny - 8:ny]

    swap = remote(surf, surf_other, 6, at(gx, gy, other))
    swap.start()
    first, last = pl.ds(0, 8), pl.ds(nx - 8, 8)
    ways = (
        (surf.at[:, first, :], halo_x, 0, x_down, gy),
        (surf.at[:, last, :], halo_x, 1, x_up, gy),
        (border.at[0], halo_y, 0, gx, y_down),
        (border.at[1], halo_y, 1, gx, y_up),
        (border.at[0], halo_y, 2, x_down, y_down),
        (border.at[1], halo_y, 3, x_down, y_up),
        (border.at[0], halo_y, 4, x_up, y_down),
        (border.at[1], halo_y, 5, x_up, y_up),
    )
    count = len(ways)
    started = []
    for k in reversed(range(count)):
        source, target, place, x, y = ways[k]
        for i, z in enumerate((gz, other)):
            copy = remote(source, target.at[gz, place], 7 + i * count + k, at(x, y, z), 7 + gz * count + k)
            copy.start()
            started.append(copy)
    swap.wait_recv()
    for k, (source, target, place, x, y) in enumerate(ways):
        for i in range(2):
            remote(source, target.at[i, place], 7 + i * count + k, at(x, y, gz)).wait_recv()
    sent = sent + [swap] + started
    mask_tall = domain(tall)
    mask = domain(rows)
    low_rows = iota((8, lanes), 0) < 4

    def packed(values):
        return jnp.concatenate(
            [values[0:nx], jnp.where(low_rows, values[nx:nx + 8], values[nx + 8:nx + 16])], axis=0
        )

    blank = jnp.zeros((ny - 16, ny), F32)

    def columns_of(place):
        low_side, high_side = halo_y[0, place] + halo_y[1, place], halo_y[0, place + 1] + halo_y[1, place + 1]
        return jnp.concatenate([low_side, blank, high_side], axis=0).T[0:3 * nx].reshape(3, nx, ny)

    near, upper, lower = columns_of(0), columns_of(2), columns_of(4)
    around = []
    for c in range(3):
        main = jnp.concatenate(
            [surf[c] + surf_other[c], halo_x[0, 0, c] + halo_x[1, 0, c], halo_x[0, 1, c] + halo_x[1, 1, c]], axis=0
        )
        side = jnp.concatenate([near[c], upper[c, 0:8], lower[c, nx - 8:nx]], axis=0)
        around.append(mask_tall * jnp.concatenate([main, side], axis=1))
    flux = mask_tall * (
        0.5 * ((ahead(around[0], 0) - behind(around[0], 0)) + (ahead(around[1], 1) - behind(around[1], 1)))
    )
    for c in range(3):
        s = around[c]
        beside_xy = (ahead(s, 0) + behind(s, 0)) + (ahead(s, 1) + behind(s, 1))
        fields[c] = packed(s)
        if c < 2:
            drop = 0.125 * beside_xy + (1.0 / 32.0) * (ahead(flux, c) - behind(flux, c))
            fields[3 + c] = mask * packed(drop)
            fields[6 + c] = mask * packed((1.0 / 32.0) * (ahead(around[2], c) - behind(around[2], c)))
        else:
            fields[3 + c] = mask * packed(0.125 * beside_xy)
    fields[8] = packed(flux)

    layers.wait_recv()
    sent = sent + [layers]

    def first_layer(i, carry):
        z = (nz - 4) * gz + i
        value = [table[k, z] for k in range(5)]
        own = coef[z] * value[0] - value[1]
        for c in range(2):
            w1[c, z + 1] = mask * (fields[c] * own) - value[0] * fields[3 + c] - value[2] * fields[6 + c]
        w1[2, z + 1] = mask * (fields[2] * (own - value[4])) - value[0] * fields[5] - value[3] * fields[8]
        return carry

    pairwise(0, nz + 4, first_layer)

    def spread_of(source, start, amount):
        def layer(i, carry):
            z = start + i
            x, y = source[0, z + 1], source[1, z + 1]
            div[z + 1] = mask * (
                ((ahead(x, 0) - behind(x, 0)) + (ahead(y, 1) - behind(y, 1)))
                + (source[2, z + 2] - source[2, z])
            )
            return carry

        pairwise(0, amount, layer)

    spread_of(w1, (nz - 3) * gz, nz + 3)

    def second_layer(i, carry):
        z = (nz - 2) * gz + i
        own = coef[z]
        here = div[z + 1]
        for c in range(3):
            v = w1[c, z + 1]
            total = (ahead(v, 0) + behind(v, 0)) + (ahead(v, 1) + behind(v, 1))
            total = total + (w1[c, z + 2] + w1[c, z])
            slope = (ahead(here, c) - behind(here, c)) if c < 2 else (div[z + 2] - div[z])
            w2[c, z + 1] = mask * (own * v - 0.125 * total - (1.0 / 64.0) * slope)
        return carry

    pairwise(0, nz + 2, second_layer)

    spread_of(w2, (nz - 1) * gz, nz + 1)

    def folded(values):
        total = values[0:8]
        for k in range(8, nx, 8):
            total = total + values[k:k + 8]
        return total

    def gather_moments(i, sums):
        z = nz * gz + i
        own = coef[z, 0:nx, 0:ny]
        d_now = table[0, z, :, 0:ny]
        here = div[z + 1, 0:nx, 0:ny]
        terms = [None] * MOMENTS
        terms[MOMENTS - 1] = (1.0 / 64.0) * (here * here)
        for c in range(3):
            v = w2[c, z + 1, 0:nx, 0:ny]
            total = ahead(w2[c, z + 1, :, 0:ny], 0)[0:nx] + ahead(w2[c, z + 1, 0:nx, :], 1)[:, 0:ny]
            total = total + w2[c, z + 2, 0:nx, 0:ny]
            zeroth = d_now * fields[c, 0:nx, 0:ny]
            one = w1[c, z + 1, 0:nx, 0:ny]
            for k, term in enumerate(
                (zeroth * zeroth, zeroth * one, one * one, one * v, v * v, v * (own * v - 0.25 * total))
            ):
                terms[k] = term if terms[k] is None else terms[k] + term
        return tuple(s + folded(t) for s, t in zip(sums, terms))

    sums = lax.fori_loop(0, nz, gather_moments, tuple(jnp.zeros((8, ny), F32) for _ in range(MOMENTS)))

    def third_layer(i, carry):
        z = nz * gz + i
        own = coef[z, 0:nx, 0:ny]
        here_x, here_y = div[z + 1, :, 0:ny], div[z + 1, 0:nx, :]
        for c in range(3):
            v = w2[c, z + 1, 0:nx, 0:ny]
            vx, vy = w2[c, z + 1, :, 0:ny], w2[c, z + 1, 0:nx, :]
            total = (ahead(vx, 0) + behind(vx, 0))[0:nx] + (ahead(vy, 1) + behind(vy, 1))[:, 0:ny]
            total = total + (w2[c, z + 2, 0:nx, 0:ny] + w2[c, z, 0:nx, 0:ny])
            if c == 0:
                slope = (ahead(here_x, 0) - behind(here_x, 0))[0:nx]
            elif c == 1:
                slope = (ahead(here_y, 1) - behind(here_y, 1))[:, 0:ny]
            else:
                slope = div[z + 2, 0:nx, 0:ny] - div[z, 0:nx, 0:ny]
            res_ref[c, i] = own * v - 0.125 * total - (1.0 / 64.0) * slope
        return carry

    early_layers = (3 * nz) // 8

    lane = iota((1, ny), 1)
    message = jnp.where(lane == MOMENTS, mass, 0.0) + jnp.where(lane == MOMENTS + 1, weight, 0.0)
    for k in range(MOMENTS):
        amount = jnp.sum(jnp.sum(sums[k], axis=0, keepdims=True), axis=1, keepdims=True)
        message = message + jnp.where(lane == k, amount, 0.0)
    row_out[0] = message
    slot = gy * 2 + gz
    row_in[slot] = message
    base = 7 + 2 * count
    started = []
    for k, (y, z) in enumerate(peers):
        copy = remote(row_out.at[0], row_in.at[slot], base + k, at(gx, y, z))
        copy.start()
        started.append(copy)
    pairwise(0, early_layers, third_layer)
    for copy in started:
        copy.wait_recv()
    sent = sent + started
    message = row_in[0]
    for k in range(1, 2 * ngy):
        message = message + row_in[k]
    row_out[1] = message
    ring_in[gx] = message
    first_index = base + len(peers)
    started = []
    for k in range(1, ngx):
        copy = remote(row_out.at[1], ring_in.at[gx], first_index + k - 1, at(wrap(gx + k, ngx), gy, gz))
        copy.start()
        started.append(copy)
    pairwise(early_layers, nz, third_layer)
    for copy in started:
        copy.wait_recv()
    sent = sent + started
    message = ring_in[0]
    for k in range(1, ngx):
        message = message + ring_in[k]
    parts = [jnp.sum(jnp.where(lane == k, message, 0.0), axis=1, keepdims=True) for k in range(MOMENTS + 2)]

    scale = lax.rsqrt(parts[MOMENTS] / (EPOCHS * parts[MOMENTS + 1]) + EPS) * (1.0 / PRE)
    iterate, residual = conjugate(parts[0:MOMENTS])
    iterate = [scale * value for value in iterate]
    residual = [scale * value for value in residual]

    def finish(i, carry):
        z = nz * gz + i
        d_now = table[0, z, :, 0:ny]
        for c in range(3):
            zeroth = d_now * fields[c, 0:nx, 0:ny]
            one, two = w1[c, z + 1, 0:nx, 0:ny], w2[c, z + 1, 0:nx, 0:ny]
            third = res_ref[c, i]
            adj_ref[c, i] = iterate[0] * zeroth + iterate[1] * one + iterate[2] * two
            res_ref[c, i] = residual[0] * zeroth + residual[1] * one + residual[2] * two + residual[3] * third
        return carry

    pairwise(0, nz, finish)
    for copy in sent:
        copy.wait_send()
    for message, buffer in enumerate((slots_ref, choice_ref)):
        part = buffer.at[pl.ds(0, owners - 1)]
        pltpu.make_async_copy(part, part, send_a2a.at[message]).wait()


def per_device(
    observed,
    predicted,
    coherence_mask,
    block_count,
    block_owner,
    block_matrix_choice,
    block_patch,
    look_vector,
    interp_weights,
    depth_kernel,
    stiffness,
):
    blocks, epochs, pixels = observed.shape
    cells = PATCH_X * PATCH_Y
    ngx, ngy = lax.axis_size("gx"), lax.axis_size("gy")
    owners = ngx * ngy
    nz, nx, ny = stiffness.shape

    rows, lanes = nx + 8, 2 * ny
    out = pltpu.VMEM((3, nz, nx, ny), F32)
    vmem = pl.BlockSpec(memory_space=pltpu.VMEM)
    far = pl.BlockSpec(memory_space=pltpu.HBM)
    copies = 23 + (2 * ngy - 1) + (ngx - 1)
    return pl.pallas_call(
        kernel,
        out_shape=(out, out),
        in_specs=[far] * 11,
        out_specs=(vmem, vmem),
        scratch_shapes=[
            pltpu.VMEM(observed.shape, F32),
            pltpu.VMEM(predicted.shape, F32),
            pltpu.VMEM(coherence_mask.shape, jnp.int32),
            pltpu.SMEM((blocks,), jnp.int32),
            pltpu.SMEM((blocks,), jnp.int32),
            pltpu.SMEM((blocks,), jnp.int32),
            pltpu.SMEM((blocks,), jnp.int32),
            pltpu.SMEM(look_vector.shape, F32),
            pltpu.VMEM(interp_weights.shape, interp_weights.dtype),
            pltpu.SMEM((nz,), F32),
            pltpu.VMEM(stiffness.shape, F32),
            pltpu.VMEM((4, blocks, ny), jnp.int32),
            pltpu.VMEM((blocks, pixels), F32),
            pltpu.VMEM((epochs * blocks, pixels), F32),
            pltpu.VMEM((3 * blocks, pixels), F32),
            pltpu.VMEM((owners, 3, CAP, cells), F32),
            pltpu.VMEM((owners, 1, cells), F32),
            pltpu.VMEM((owners, 3, CAP, cells), F32),
            pltpu.VMEM((owners, 1, cells), F32),
            pltpu.VMEM((owners * CAP, 3 * cells), F32),
            pltpu.VMEM((owners * CAP, cells), F32),
            pltpu.VMEM((3, nx, ny), F32),
            pltpu.VMEM((3, nx, ny), F32),
            pltpu.VMEM((2, 8, ny), F32),
            pltpu.VMEM((2, 2, 3, 8, ny), F32),
            pltpu.VMEM((2, 6, 8, ny), F32),
            pltpu.VMEM((2, nz, 8, ny), F32),
            pltpu.VMEM((nz, rows, ny), F32),
            pltpu.VMEM((2, 8, nz * rows), F32),
            pltpu.VMEM((2, 8, nz * rows), F32),
            pltpu.VMEM((2 * nz, rows, lanes), F32),
            pltpu.VMEM((2 * nz + 16, lanes), F32),
            pltpu.VMEM((5, 2 * nz, 1, lanes), F32),
            pltpu.VMEM((9, rows, lanes), F32),
            pltpu.VMEM((3, 2 * nz + 2, rows, lanes), F32),
            pltpu.VMEM((3, 2 * nz + 2, rows, lanes), F32),
            pltpu.VMEM((2 * nz + 2, rows, lanes), F32),
            pltpu.VMEM((2, 1, ny), F32),
            pltpu.VMEM((2 * ngy, 1, ny), F32),
            pltpu.VMEM((ngx, 1, ny), F32),
            pltpu.SemaphoreType.DMA((2,)),
            pltpu.SemaphoreType.DMA((2,)),
            pltpu.SemaphoreType.DMA((copies,)),
            pltpu.SemaphoreType.DMA((copies,)),
            pltpu.SemaphoreType.DMA((11,)),
        ],
        compiler_params=pltpu.CompilerParams(
            collective_id=0, has_side_effects=True, vmem_limit_bytes=60000000
        ),
    )(
        observed, predicted, coherence_mask, block_count, block_owner[:, 0], block_matrix_choice, block_patch,
        look_vector, interp_weights, depth_kernel, stiffness,
    )


def solution(mesh):
    in_specs = (
        P(("grp", "gx", "gy", "gz"), None, None),
        P(("grp", "gx", "gy", "gz"), None, None),
        P(("grp", "gx", "gy", "gz"), None),
        P(("grp", "gx", "gy", "gz")),
        P(("grp", "gx", "gy", "gz"), None),
        P(("grp", "gx", "gy", "gz")),
        P(("grp", "gx", "gy", "gz")),
        P(),
        P(),
        P(("grp", "gz")),
        P(("grp", "gz"), "gx", "gy"),
    )
    out_specs = (P(None, ("grp", "gz"), "gx", "gy"), P(None, ("grp", "gz"), "gx", "gy"))
    return jax.shard_map(
        per_device, mesh=mesh, in_specs=in_specs, out_specs=out_specs, check_vma=False
    )
```

```python
import jax
import jax.numpy as jnp
from jax import lax
from jax.experimental import pallas as pl
from jax.experimental.pallas import tpu as pltpu
from jax.sharding import PartitionSpec as P

EPOCHS = 4
PATCH_X = 8
PATCH_Y = 16
CAP = 4
EPS = 1e-06

SHIFT = 8.0
PRE = 1024.0
MOMENTS = 6

HIGHEST = lax.Precision.HIGHEST
F32 = jnp.float32


def roll(values, shift, axis):
    return pltpu.roll(values, shift % values.shape[axis], axis)


def ahead(values, axis):
    return roll(values, -1, axis)


def behind(values, axis):
    return roll(values, 1, axis)


def iota(shape, axis):
    return lax.broadcasted_iota(jnp.int32, shape, axis)


def pairwise(start, stop, body):
    def trip(k, carry):
        body(start + 2 * k, None)
        body(start + 2 * k + 1, None)
        return carry

    lax.fori_loop(0, (stop - start) // 2, trip, 0)
    if (stop - start) % 2:
        body(stop - 1, None)


def product(first, second, moments):
    total = None
    for i, f in enumerate(first):
        for j, g in enumerate(second):
            term = f * g * moments[i + j]
            total = term if total is None else total + term
    return total


def combined(first, factor, second):
    size = max(len(first), len(second))
    out = []
    for i in range(size):
        value = first[i] if i < len(first) else None
        if i < len(second):
            term = factor * second[i]
            value = term if value is None else value + term
        out.append(value)
    return out


def applied(poly):
    out = []
    for i in range(len(poly) + 1):
        value = None
        for j in (i, i - 1):
            if 0 <= j < len(poly):
                value = poly[j] if value is None else value + poly[j]
        out.append(SHIFT * value)
    return out


def conjugate(moments):
    one = jnp.ones_like(moments[0])
    residual, direction, iterate = [one], [one], []
    now = moments[0]
    for step in range(3):
        image = applied(direction)
        alpha = now / product(direction, image, moments)
        scaled = [alpha * d for d in direction]
        iterate = scaled if not iterate else combined(iterate, one, scaled)
        residual = combined(residual, -alpha, image)
        if step < 2:
            new = product(residual, residual, moments)
            direction = combined(residual, new / now, direction)
            now = new
    return iterate, residual


def kernel(
    observed_hbm, predicted_hbm, coherence_hbm, count_hbm, owner_hbm, table_hbm, patch_hbm, look_hbm,
    weights_hbm, depth_hbm, stiff_hbm,
    adj_ref, res_ref,
    observed_ref, predicted_ref, coherence_ref, count_ref, owner_ref, table_ref, patch_ref, look_ref,
    weights, depth_ref, stiff_ref,
    numbers, valid, resid, coeffs, slots_ref, choice_ref,
    got_slots, got_choice, flat_slots, flat_choice,
    surf, surf_other, border, halo_x, halo_y,
    stiff_edge, stiff_x, wide_stiff, strip_out, strip_in, coef,
    depths, table,
    fields, w1, w2, div,
    row_out, row_in, ring_in,
    send_a2a, recv_a2a, send_sem, recv_sem, local_sem,
):
    pairs = (
        (depth_hbm, depth_ref), (count_hbm, count_ref), (owner_hbm, owner_ref), (table_hbm, table_ref),
        (patch_hbm, patch_ref), (look_hbm, look_ref), (coherence_hbm, coherence_ref),
        (predicted_hbm, predicted_ref), (observed_hbm, observed_ref), (weights_hbm, weights), (stiff_hbm, stiff_ref),
    )
    fetches = [pltpu.make_async_copy(a, b, local_sem.at[i]) for i, (a, b) in enumerate(pairs)]
    for fetch in fetches:
        fetch.start()
    gx, gy, gz = lax.axis_index("gx"), lax.axis_index("gy"), lax.axis_index("gz")
    ngx, ngy = lax.axis_size("gx"), lax.axis_size("gy")
    owners = ngx * ngy
    me = gx * ngy + gy
    nz, nx, ny = stiff_ref.shape
    other = 1 - gz
    rows, lanes = nx + 8, 2 * ny
    tall = nx + 16

    def at(x, y, z):
        return {"gx": x, "gy": y, "gz": z}

    def wrap(value, count):
        return lax.rem(value + count, count)

    depths[...] = jnp.zeros(depths.shape, F32)

    barrier = pltpu.get_barrier_semaphore()
    peers = [(wrap(gy + k, ngy), gz) for k in range(1, ngy)] + [(wrap(gy + k, ngy), other) for k in range(ngy)]

    def greet(k, carry):
        j = wrap(gx - k, ngx)
        for y in range(ngy):
            pl.semaphore_signal(barrier, inc=1, device_id=at(j, y, gz))
        return carry

    lax.fori_loop(1, ngx, greet, 0)
    for y, z in peers:
        pl.semaphore_signal(barrier, inc=1, device_id=at(gx, y, z))

    own_layers = pl.ds(pl.multiple_of(8 + nz * gz, 8), nz)
    fetches[0].wait()
    layer = iota((nz, lanes), 0)
    own_depths = jnp.zeros((nz, lanes), F32)
    for z in range(nz):
        own_depths = jnp.where(layer == z, PRE * depth_ref[z], own_depths)
    depths[own_layers, :] = own_depths

    def domain(count):
        r, c = iota((count, lanes), 0), iota((count, lanes), 1)
        half = (count - nx) // 2
        in_x = (r < nx) | ((r < nx + half) & (gx < ngx - 1)) | ((r >= nx + half) & (gx > 0))
        in_y = (c < ny) | ((c < ny + ny // 2) & (gy < ngy - 1)) | ((c >= ny + ny // 2) & (gy > 0))
        return (in_x & in_y).astype(F32)

    zero_plane = jnp.zeros((rows, lanes), F32)
    for edge in (0, 2 * nz + 1):
        div[edge] = zero_plane
        for c in range(3):
            w1[c, edge] = zero_plane
            w2[c, edge] = zero_plane
    blocks, epochs, pixels = observed_ref.shape
    for fetch in fetches[1:9]:
        fetch.wait()

    for b in range(blocks):
        for k, source in enumerate((count_ref, table_ref, patch_ref, owner_ref)):
            numbers[k, b:b + 1, :] = jnp.full((1, ny), source[b], jnp.int32)
    in_scene = iota((blocks, ny), 1)
    for k in range(0, pixels, ny):
        kept = (in_scene + k < numbers[0]).astype(F32)
        valid[:, k:k + ny] = coherence_ref[:, k:k + ny].astype(F32) * kept
    for b in range(blocks):
        resid[epochs * b:epochs * (b + 1), :] = (predicted_ref[b] - observed_ref[b]) * valid[b:b + 1, :]
    res = resid[...]
    row_block, row_place = iota((blocks, epochs * blocks), 0), iota((blocks, epochs * blocks), 1)
    own_rows = row_place // epochs == row_block
    mixes = []
    for c in range(3):
        mix = jnp.zeros((blocks, epochs * blocks), F32)
        for e in range(epochs):
            mix = jnp.where(own_rows & (row_place % epochs == e), look_ref[e, c], mix)
        mixes.append(mix)
    coeffs[...] = jnp.dot(
        jnp.concatenate(mixes, axis=0), res, precision=HIGHEST, preferred_element_type=F32
    )
    mass = jnp.sum(jnp.sum(res * res, axis=0, keepdims=True), axis=1, keepdims=True)
    weight = jnp.sum(jnp.sum(valid[...], axis=0, keepdims=True), axis=1, keepdims=True)

    lane_owner = iota((blocks, owners), 1)
    at_owner = (lane_owner == numbers[3, :, 0:owners]).astype(F32)
    before = (iota((blocks, blocks), 1) < iota((blocks, blocks), 0)).astype(F32)
    ahead_of = jnp.dot(before, at_owner, preferred_element_type=F32)
    rank = jnp.sum(ahead_of * at_owner, axis=1, keepdims=True).astype(jnp.int32)
    slot_of = numbers[3, :, 0:1] * CAP + rank
    select = (iota((blocks, owners * CAP), 1) == slot_of).astype(F32)
    at_lane = (iota((blocks, ny), 1) == rank * (ny // CAP) + numbers[2]).astype(F32)
    marks = lax.dot_general(at_owner, at_lane, (((0,), (0,)), ((), ())), preferred_element_type=F32)
    for o in range(owners):
        choice_ref[o] = marks[o:o + 1]

    rounded = coeffs[...].astype(jnp.bfloat16).astype(F32)
    which = jnp.concatenate([numbers[1]] * 3, axis=0)
    which = jnp.concatenate([which] * (pixels // ny), axis=1)
    fetches[9].wait()
    fetches[10].wait()
    for z in range(nz):
        stiff_edge[0, z] = stiff_ref[z, 0:4]
        stiff_edge[1, z] = stiff_ref[z, nx - 4:nx]
    total_sums = jnp.zeros((3 * blocks, ny), F32)
    for t in range(weights.shape[0]):
        taken = jnp.where(which == t, rounded, 0.0).astype(jnp.bfloat16)
        total_sums = total_sums + jnp.dot(taken, weights[t], preferred_element_type=F32)
    chosen = lax.dot_general(
        select, jnp.concatenate([total_sums[c * blocks:(c + 1) * blocks] for c in range(3)], axis=1),
        (((0,), (0,)), ((), ())), precision=HIGHEST, preferred_element_type=F32,
    )
    for c in range(3):
        for o in range(owners):
            slots_ref[o, c] = chosen[CAP * o:CAP * (o + 1), c * ny:(c + 1) * ny]

    pl.semaphore_wait(barrier, (ngx - 1) * ngy + len(peers))

    def remote(source, target, index, device, arrival=None):
        return pltpu.make_async_remote_copy(
            src_ref=source, dst_ref=target, send_sem=send_sem.at[index],
            recv_sem=recv_sem.at[index if arrival is None else arrival],
            device_id=device, device_id_type=pl.DeviceIdType.MESH,
        )

    x_up, x_down = wrap(gx + 1, ngx), wrap(gx - 1, ngx)
    y_up, y_down = wrap(gy + 1, ngy), wrap(gy - 1, ngy)
    to_down = remote(stiff_edge.at[0], stiff_x.at[0], 0, at(x_down, gy, gz))
    to_up = remote(stiff_edge.at[1], stiff_x.at[1], 1, at(x_up, gy, gz))
    to_other = remote(depths.at[own_layers, :], depths.at[own_layers, :], 2, at(gx, gy, other))
    to_other.start()

    to_down.start()
    to_up.start()
    def post(j, first):
        for k in range(first, ngy):
            y = wrap(gy + k, ngy)
            o = j * ngy + y
            for message, (source, target) in enumerate(((slots_ref, got_slots), (choice_ref, got_choice))):
                pltpu.make_async_remote_copy(
                    src_ref=source.at[o], dst_ref=target.at[me],
                    send_sem=send_a2a.at[message], recv_sem=recv_a2a.at[message],
                    device_id=at(j, y, gz), device_id_type=pl.DeviceIdType.MESH,
                ).start()

    def post_pair(i, carry):
        d = ngx // 2 - i
        post(wrap(gx - d, ngx), 0)

        @pl.when(d < ngx // 2)
        def _():
            post(wrap(gx + d, ngx), 0)

        return carry

    lax.fori_loop(0, ngx // 2, post_pair, 0)
    post(gx, 1)

    got_slots[me] = slots_ref[me]
    got_choice[me] = choice_ref[me]

    to_down.wait_recv()
    to_up.wait_recv()
    to_other.wait_recv()
    sent = [to_down, to_up, to_other]
    for z in range(nz):
        wide_stiff[z, 0:nx, :] = stiff_ref[z]
        wide_stiff[z, nx:nx + 4, :] = stiff_x[0, z]
        wide_stiff[z, nx + 4:rows, :] = stiff_x[1, z]
    turned = wide_stiff[...].reshape(nz * rows, ny).T
    strip_out[0] = turned[0:8]
    strip_out[1] = turned[ny - 8:ny]
    strips = [
        remote(strip_out.at[0], strip_in.at[0], 3, at(gx, y_down, gz)),
        remote(strip_out.at[1], strip_in.at[1], 4, at(gx, y_up, gz)),
    ]
    for copy in strips:
        copy.start()

    d = depths[...]
    where_z = iota(d.shape, 0)
    inside = ((where_z >= 8) & (where_z < 8 + 2 * nz)).astype(F32)
    d_up, d_down = ahead(d, 0), behind(d, 0)
    q = 0.5 * (d_up - d_down)
    kept_d, kept_q = inside * d, inside * q
    columns = (
        d,
        0.125 * (d_up + d_down),
        q,
        (1.0 / 32.0) * (ahead(kept_d, 0) - behind(kept_d, 0)),
        (1.0 / 32.0) * (ahead(kept_q, 0) - behind(kept_q, 0)),
    )
    for k, values in enumerate(columns):
        for z in range(2 * nz):
            table[k, z] = values[z + 8:z + 9]

    for copy in strips:
        copy.wait_recv()
    sent = sent + strips
    filler = jnp.zeros((ny - 16, nz * rows), F32)
    beside = jnp.concatenate([strip_in[0], filler, strip_in[1]], axis=0).T.reshape(nz, rows, ny)
    base = nz * gz
    for z in range(nz):
        coef[base + z, :, 0:ny] = 0.125 * wide_stiff[z] - 0.25
        coef[base + z, :, ny:lanes] = 0.125 * beside[z] - 0.25
    passed = pl.ds((nz - 4) + 4 * gz, 4)
    layers = remote(coef.at[passed], coef.at[passed], 5, at(gx, gy, other))
    layers.start()

    for message, buffer in enumerate((got_slots, got_choice)):
        part = buffer.at[pl.ds(0, owners - 1)]
        pltpu.make_async_copy(part, part, recv_a2a.at[message]).wait()
    own_slot = iota((CAP, ny), 1) // (ny // CAP) == iota((CAP, ny), 0)
    for o in range(owners):
        for c in range(3):
            flat_slots[CAP * o:CAP * (o + 1), c * ny:(c + 1) * ny] = got_slots[o, c]
        flat_choice[CAP * o:CAP * (o + 1), :] = jnp.where(own_slot, got_choice[o], 0.0)
    picked = flat_choice[...]
    spread = lax.dot_general(
        picked, flat_slots[...], (((0,), (0,)), ((), ())), precision=HIGHEST, preferred_element_type=F32
    )
    depth_places = ny // CAP
    tiles = []
    for c in range(3):
        placed = spread[0:depth_places, c * ny:(c + 1) * ny]
        for j in range(1, CAP):
            placed = placed + spread[j * depth_places:(j + 1) * depth_places, c * ny:(c + 1) * ny]
        tiles.append(placed)
    tile = jnp.concatenate(tiles, axis=0)
    sub = lax.rem(iota(tile.shape, 0), 8)
    chunk = iota(tile.shape, 1) // PATCH_Y
    for bit in (1, 2, 4):
        row_set, chunk_set = (sub // bit) % 2 == 1, (chunk // bit) % 2 == 1
        from_below = roll(roll(tile, -bit, 0), bit * PATCH_Y, 1)
        from_above = roll(roll(tile, bit, 0), -bit * PATCH_Y, 1)
        tile = jnp.where(row_set == chunk_set, tile, jnp.where(row_set, from_above, from_below))
    surf[...] = tile.reshape(3, nx, ny)
    turned = jnp.concatenate([tile, jnp.zeros((ny - 3 * nx, ny), F32)], axis=0).T
    border[0] = turned[0:8]
    border[1] = turned[ny - 8:ny]

    swap = remote(surf, surf_other, 6, at(gx, gy, other))
    swap.start()
    first, last = pl.ds(0, 8), pl.ds(nx - 8, 8)
    ways = (
        (surf.at[:, first, :], halo_x, 0, x_down, gy),
        (surf.at[:, last, :], halo_x, 1, x_up, gy),
        (border.at[0], halo_y, 0, gx, y_down),
        (border.at[1], halo_y, 1, gx, y_up),
        (border.at[0], halo_y, 2, x_down, y_down),
        (border.at[1], halo_y, 3, x_down, y_up),
        (border.at[0], halo_y, 4, x_up, y_down),
        (border.at[1], halo_y, 5, x_up, y_up),
    )
    count = len(ways)
    started = []
    for k in reversed(range(count)):
        source, target, place, x, y = ways[k]
        for i, z in enumerate((gz, other)):
            copy = remote(source, target.at[gz, place], 7 + i * count + k, at(x, y, z), 7 + gz * count + k)
            copy.start()
            started.append(copy)
    swap.wait_recv()
    for k, (source, target, place, x, y) in enumerate(ways):
        for i in range(2):
            remote(source, target.at[i, place], 7 + i * count + k, at(x, y, gz)).wait_recv()
    sent = sent + [swap] + started
    mask_tall = domain(tall)
    mask = domain(rows)
    low_rows = iota((8, lanes), 0) < 4

    def packed(values):
        return jnp.concatenate(
            [values[0:nx], jnp.where(low_rows, values[nx:nx + 8], values[nx + 8:nx + 16])], axis=0
        )

    blank = jnp.zeros((ny - 16, ny), F32)

    def columns_of(place):
        low_side, high_side = halo_y[0, place] + halo_y[1, place], halo_y[0, place + 1] + halo_y[1, place + 1]
        return jnp.concatenate([low_side, blank, high_side], axis=0).T[0:3 * nx].reshape(3, nx, ny)

    near, upper, lower = columns_of(0), columns_of(2), columns_of(4)
    around = []
    for c in range(3):
        main = jnp.concatenate(
            [surf[c] + surf_other[c], halo_x[0, 0, c] + halo_x[1, 0, c], halo_x[0, 1, c] + halo_x[1, 1, c]], axis=0
        )
        side = jnp.concatenate([near[c], upper[c, 0:8], lower[c, nx - 8:nx]], axis=0)
        around.append(mask_tall * jnp.concatenate([main, side], axis=1))
    flux = mask_tall * (
        0.5 * ((ahead(around[0], 0) - behind(around[0], 0)) + (ahead(around[1], 1) - behind(around[1], 1)))
    )
    for c in range(3):
        s = around[c]
        beside_xy = (ahead(s, 0) + behind(s, 0)) + (ahead(s, 1) + behind(s, 1))
        fields[c] = packed(s)
        if c < 2:
            drop = 0.125 * beside_xy + (1.0 / 32.0) * (ahead(flux, c) - behind(flux, c))
            fields[3 + c] = mask * packed(drop)
            fields[6 + c] = mask * packed((1.0 / 32.0) * (ahead(around[2], c) - behind(around[2], c)))
        else:
            fields[3 + c] = mask * packed(0.125 * beside_xy)
    fields[8] = packed(flux)

    layers.wait_recv()
    sent = sent + [layers]

    def first_layer(i, carry):
        z = (nz - 4) * gz + i
        value = [table[k, z] for k in range(5)]
        own = coef[z] * value[0] - value[1]
        for c in range(2):
            w1[c, z + 1] = mask * (fields[c] * own) - value[0] * fields[3 + c] - value[2] * fields[6 + c]
        w1[2, z + 1] = mask * (fields[2] * (own - value[4])) - value[0] * fields[5] - value[3] * fields[8]
        return carry

    pairwise(0, nz + 4, first_layer)

    def spread_of(source, start, amount):
        def layer(i, carry):
            z = start + i
            x, y = source[0, z + 1], source[1, z + 1]
            div[z + 1] = mask * (
                ((ahead(x, 0) - behind(x, 0)) + (ahead(y, 1) - behind(y, 1)))
                + (source[2, z + 2] - source[2, z])
            )
            return carry

        pairwise(0, amount, layer)

    spread_of(w1, (nz - 3) * gz, nz + 3)

    def second_layer(i, carry):
        z = (nz - 2) * gz + i
        own = coef[z]
        here = div[z + 1]
        for c in range(3):
            v = w1[c, z + 1]
            total = (ahead(v, 0) + behind(v, 0)) + (ahead(v, 1) + behind(v, 1))
            total = total + (w1[c, z + 2] + w1[c, z])
            slope = (ahead(here, c) - behind(here, c)) if c < 2 else (div[z + 2] - div[z])
            w2[c, z + 1] = mask * (own * v - 0.125 * total - (1.0 / 64.0) * slope)
        return carry

    pairwise(0, nz + 2, second_layer)

    spread_of(w2, (nz - 1) * gz, nz + 1)

    def folded(values):
        total = values[0:8]
        for k in range(8, nx, 8):
            total = total + values[k:k + 8]
        return total

    def gather_moments(i, sums):
        z = nz * gz + i
        own = coef[z, 0:nx, 0:ny]
        d_now = table[0, z, :, 0:ny]
        here = div[z + 1, 0:nx, 0:ny]
        terms = [None] * MOMENTS
        terms[MOMENTS - 1] = (1.0 / 64.0) * (here * here)
        for c in range(3):
            v = w2[c, z + 1, 0:nx, 0:ny]
            total = ahead(w2[c, z + 1, :, 0:ny], 0)[0:nx] + ahead(w2[c, z + 1, 0:nx, :], 1)[:, 0:ny]
            total = total + w2[c, z + 2, 0:nx, 0:ny]
            zeroth = d_now * fields[c, 0:nx, 0:ny]
            one = w1[c, z + 1, 0:nx, 0:ny]
            for k, term in enumerate(
                (zeroth * zeroth, zeroth * one, one * one, one * v, v * v, v * (own * v - 0.25 * total))
            ):
                terms[k] = term if terms[k] is None else terms[k] + term
        return tuple(s + folded(t) for s, t in zip(sums, terms))

    sums = lax.fori_loop(0, nz, gather_moments, tuple(jnp.zeros((8, ny), F32) for _ in range(MOMENTS)))

    def third_layer(i, carry):
        z = nz * gz + i
        own = coef[z, 0:nx, 0:ny]
        here_x, here_y = div[z + 1, :, 0:ny], div[z + 1, 0:nx, :]
        for c in range(3):
            v = w2[c, z + 1, 0:nx, 0:ny]
            vx, vy = w2[c, z + 1, :, 0:ny], w2[c, z + 1, 0:nx, :]
            total = (ahead(vx, 0) + behind(vx, 0))[0:nx] + (ahead(vy, 1) + behind(vy, 1))[:, 0:ny]
            total = total + (w2[c, z + 2, 0:nx, 0:ny] + w2[c, z, 0:nx, 0:ny])
            if c == 0:
                slope = (ahead(here_x, 0) - behind(here_x, 0))[0:nx]
            elif c == 1:
                slope = (ahead(here_y, 1) - behind(here_y, 1))[:, 0:ny]
            else:
                slope = div[z + 2, 0:nx, 0:ny] - div[z, 0:nx, 0:ny]
            res_ref[c, i] = own * v - 0.125 * total - (1.0 / 64.0) * slope
        return carry

    early_layers = (3 * nz) // 8

    lane = iota((1, ny), 1)
    message = jnp.where(lane == MOMENTS, mass, 0.0) + jnp.where(lane == MOMENTS + 1, weight, 0.0)
    for k in range(MOMENTS):
        amount = jnp.sum(jnp.sum(sums[k], axis=0, keepdims=True), axis=1, keepdims=True)
        message = message + jnp.where(lane == k, amount, 0.0)
    row_out[0] = message
    slot = gy * 2 + gz
    row_in[slot] = message
    base = 7 + 2 * count
    started = []
    for k, (y, z) in enumerate(peers):
        copy = remote(row_out.at[0], row_in.at[slot], base + k, at(gx, y, z))
        copy.start()
        started.append(copy)
    pairwise(0, early_layers, third_layer)
    for copy in started:
        copy.wait_recv()
    sent = sent + started
    message = row_in[0]
    for k in range(1, 2 * ngy):
        message = message + row_in[k]
    row_out[1] = message
    ring_in[gx] = message
    first_index = base + len(peers)
    started = []
    for k in range(1, ngx):
        copy = remote(row_out.at[1], ring_in.at[gx], first_index + k - 1, at(wrap(gx + k, ngx), gy, gz))
        copy.start()
        started.append(copy)
    pairwise(early_layers, nz, third_layer)
    for copy in started:
        copy.wait_recv()
    sent = sent + started
    message = ring_in[0]
    for k in range(1, ngx):
        message = message + ring_in[k]
    parts = [jnp.sum(jnp.where(lane == k, message, 0.0), axis=1, keepdims=True) for k in range(MOMENTS + 2)]

    scale = lax.rsqrt(parts[MOMENTS] / (EPOCHS * parts[MOMENTS + 1]) + EPS) * (1.0 / PRE)
    iterate, residual = conjugate(parts[0:MOMENTS])
    iterate = [scale * value for value in iterate]
    residual = [scale * value for value in residual]

    def finish(i, carry):
        z = nz * gz + i
        d_now = table[0, z, :, 0:ny]
        for c in range(3):
            zeroth = d_now * fields[c, 0:nx, 0:ny]
            one, two = w1[c, z + 1, 0:nx, 0:ny], w2[c, z + 1, 0:nx, 0:ny]
            third = res_ref[c, i]
            adj_ref[c, i] = iterate[0] * zeroth + iterate[1] * one + iterate[2] * two
            res_ref[c, i] = residual[0] * zeroth + residual[1] * one + residual[2] * two + residual[3] * third
        return carry

    pairwise(0, nz, finish)
    for copy in sent:
        copy.wait_send()
    for message, buffer in enumerate((slots_ref, choice_ref)):
        part = buffer.at[pl.ds(0, owners - 1)]
        pltpu.make_async_copy(part, part, send_a2a.at[message]).wait()


def per_device(
    observed,
    predicted,
    coherence_mask,
    block_count,
    block_owner,
    block_matrix_choice,
    block_patch,
    look_vector,
    interp_weights,
    depth_kernel,
    stiffness,
):
    blocks, epochs, pixels = observed.shape
    cells = PATCH_X * PATCH_Y
    ngx, ngy = lax.axis_size("gx"), lax.axis_size("gy")
    owners = ngx * ngy
    nz, nx, ny = stiffness.shape

    rows, lanes = nx + 8, 2 * ny
    out = pltpu.VMEM((3, nz, nx, ny), F32)
    vmem = pl.BlockSpec(memory_space=pltpu.VMEM)
    far = pl.BlockSpec(memory_space=pltpu.HBM)
    copies = 23 + (2 * ngy - 1) + (ngx - 1)
    return pl.pallas_call(
        kernel,
        out_shape=(out, out),
        in_specs=[far] * 11,
        out_specs=(vmem, vmem),
        scratch_shapes=[
            pltpu.VMEM(observed.shape, F32),
            pltpu.VMEM(predicted.shape, F32),
            pltpu.VMEM(coherence_mask.shape, jnp.int32),
            pltpu.SMEM((blocks,), jnp.int32),
            pltpu.SMEM((blocks,), jnp.int32),
            pltpu.SMEM((blocks,), jnp.int32),
            pltpu.SMEM((blocks,), jnp.int32),
            pltpu.SMEM(look_vector.shape, F32),
            pltpu.VMEM(interp_weights.shape, interp_weights.dtype),
            pltpu.SMEM((nz,), F32),
            pltpu.VMEM(stiffness.shape, F32),
            pltpu.VMEM((4, blocks, ny), jnp.int32),
            pltpu.VMEM((blocks, pixels), F32),
            pltpu.VMEM((epochs * blocks, pixels), F32),
            pltpu.VMEM((3 * blocks, pixels), F32),
            pltpu.VMEM((owners, 3, CAP, cells), F32),
            pltpu.VMEM((owners, 1, cells), F32),
            pltpu.VMEM((owners, 3, CAP, cells), F32),
            pltpu.VMEM((owners, 1, cells), F32),
            pltpu.VMEM((owners * CAP, 3 * cells), F32),
            pltpu.VMEM((owners * CAP, cells), F32),
            pltpu.VMEM((3, nx, ny), F32),
            pltpu.VMEM((3, nx, ny), F32),
            pltpu.VMEM((2, 8, ny), F32),
            pltpu.VMEM((2, 2, 3, 8, ny), F32),
            pltpu.VMEM((2, 6, 8, ny), F32),
            pltpu.VMEM((2, nz, 4, ny), F32),
            pltpu.VMEM((2, nz, 4, ny), F32),
            pltpu.VMEM((nz, rows, ny), F32),
            pltpu.VMEM((2, 8, nz * rows), F32),
            pltpu.VMEM((2, 8, nz * rows), F32),
            pltpu.VMEM((2 * nz, rows, lanes), F32),
            pltpu.VMEM((2 * nz + 16, lanes), F32),
            pltpu.VMEM((5, 2 * nz, 1, lanes), F32),
            pltpu.VMEM((9, rows, lanes), F32),
            pltpu.VMEM((3, 2 * nz + 2, rows, lanes), F32),
            pltpu.VMEM((3, 2 * nz + 2, rows, lanes), F32),
            pltpu.VMEM((2 * nz + 2, rows, lanes), F32),
            pltpu.VMEM((2, 1, ny), F32),
            pltpu.VMEM((2 * ngy, 1, ny), F32),
            pltpu.VMEM((ngx, 1, ny), F32),
            pltpu.SemaphoreType.DMA((2,)),
            pltpu.SemaphoreType.DMA((2,)),
            pltpu.SemaphoreType.DMA((copies,)),
            pltpu.SemaphoreType.DMA((copies,)),
            pltpu.SemaphoreType.DMA((11,)),
        ],
        compiler_params=pltpu.CompilerParams(
            collective_id=0, has_side_effects=True, vmem_limit_bytes=60000000
        ),
    )(
        observed, predicted, coherence_mask, block_count, block_owner[:, 0], block_matrix_choice, block_patch,
        look_vector, interp_weights, depth_kernel, stiffness,
    )


def solution(mesh):
    in_specs = (
        P(("grp", "gx", "gy", "gz"), None, None),
        P(("grp", "gx", "gy", "gz"), None, None),
        P(("grp", "gx", "gy", "gz"), None),
        P(("grp", "gx", "gy", "gz")),
        P(("grp", "gx", "gy", "gz"), None),
        P(("grp", "gx", "gy", "gz")),
        P(("grp", "gx", "gy", "gz")),
        P(),
        P(),
        P(("grp", "gz")),
        P(("grp", "gz"), "gx", "gy"),
    )
    out_specs = (P(None, ("grp", "gz"), "gx", "gy"), P(None, ("grp", "gz"), "gx", "gy"))
    return jax.shard_map(
        per_device, mesh=mesh, in_specs=in_specs, out_specs=out_specs, check_vma=False
    )
```

```python
import jax
import jax.numpy as jnp
from jax import lax
from jax.experimental import pallas as pl
from jax.experimental.pallas import tpu as pltpu
from jax.sharding import PartitionSpec as P

EPOCHS = 4
PATCH_X = 8
PATCH_Y = 16
CAP = 4
EPS = 1e-06

SHIFT = 8.0
PRE = 1024.0
MOMENTS = 6

HIGHEST = lax.Precision.HIGHEST
F32 = jnp.float32


def roll(values, shift, axis):
    return pltpu.roll(values, shift % values.shape[axis], axis)


def ahead(values, axis):
    return roll(values, -1, axis)


def behind(values, axis):
    return roll(values, 1, axis)


def iota(shape, axis):
    return lax.broadcasted_iota(jnp.int32, shape, axis)


def pairwise(start, stop, body):
    def trip(k, carry):
        body(start + 2 * k, None)
        body(start + 2 * k + 1, None)
        return carry

    lax.fori_loop(0, (stop - start) // 2, trip, 0)
    if (stop - start) % 2:
        body(stop - 1, None)


def product(first, second, moments):
    total = None
    for i, f in enumerate(first):
        for j, g in enumerate(second):
            term = f * g * moments[i + j]
            total = term if total is None else total + term
    return total


def combined(first, factor, second):
    size = max(len(first), len(second))
    out = []
    for i in range(size):
        value = first[i] if i < len(first) else None
        if i < len(second):
            term = factor * second[i]
            value = term if value is None else value + term
        out.append(value)
    return out


def applied(poly):
    out = []
    for i in range(len(poly) + 1):
        value = None
        for j in (i, i - 1):
            if 0 <= j < len(poly):
                value = poly[j] if value is None else value + poly[j]
        out.append(SHIFT * value)
    return out


def conjugate(moments):
    one = jnp.ones_like(moments[0])
    residual, direction, iterate = [one], [one], []
    now = moments[0]
    for step in range(3):
        image = applied(direction)
        alpha = now / product(direction, image, moments)
        scaled = [alpha * d for d in direction]
        iterate = scaled if not iterate else combined(iterate, one, scaled)
        residual = combined(residual, -alpha, image)
        if step < 2:
            new = product(residual, residual, moments)
            direction = combined(residual, new / now, direction)
            now = new
    return iterate, residual


def kernel(
    observed_hbm, predicted_hbm, coherence_hbm, count_hbm, owner_hbm, table_hbm, patch_hbm, look_hbm,
    weights_hbm, depth_hbm, stiff_hbm,
    adj_ref, res_ref,
    observed_ref, predicted_ref, coherence_ref, count_ref, owner_ref, table_ref, patch_ref, look_ref,
    weights, depth_ref, stiff_ref,
    numbers, valid, resid, coeffs, slots_ref, choice_ref,
    got_slots, got_choice, flat_slots, flat_choice,
    surf, surf_other, border, halo_x, halo_y,
    stiff_edge, stiff_x, wide_stiff, strip_out, strip_in, coef,
    depths, table,
    fields, w1, w2, div,
    row_out, row_in, ring_in,
    send_a2a, recv_a2a, send_sem, recv_sem, local_sem,
):
    pairs = (
        (depth_hbm, depth_ref), (count_hbm, count_ref), (owner_hbm, owner_ref), (table_hbm, table_ref),
        (patch_hbm, patch_ref), (look_hbm, look_ref), (coherence_hbm, coherence_ref),
        (predicted_hbm, predicted_ref), (observed_hbm, observed_ref), (weights_hbm, weights), (stiff_hbm, stiff_ref),
    )
    fetches = [pltpu.make_async_copy(a, b, local_sem.at[i]) for i, (a, b) in enumerate(pairs)]
    for fetch in fetches:
        fetch.start()
    gx, gy, gz = lax.axis_index("gx"), lax.axis_index("gy"), lax.axis_index("gz")
    ngx, ngy = lax.axis_size("gx"), lax.axis_size("gy")
    owners = ngx * ngy
    me = gx * ngy + gy
    nz, nx, ny = stiff_ref.shape
    other = 1 - gz
    rows, lanes = nx + 8, 2 * ny
    tall = nx + 16

    def at(x, y, z):
        return {"gx": x, "gy": y, "gz": z}

    def wrap(value, count):
        return lax.rem(value + count, count)

    depths[...] = jnp.zeros(depths.shape, F32)

    barrier = pltpu.get_barrier_semaphore()
    peers = [(wrap(gy + k, ngy), gz) for k in range(1, ngy)] + [(wrap(gy + k, ngy), other) for k in range(ngy)]

    def greet(k, carry):
        j = wrap(gx - k, ngx)
        for y in range(ngy):
            pl.semaphore_signal(barrier, inc=1, device_id=at(j, y, gz))
        return carry

    lax.fori_loop(1, ngx, greet, 0)
    for y, z in peers:
        pl.semaphore_signal(barrier, inc=1, device_id=at(gx, y, z))

    own_layers = pl.ds(pl.multiple_of(8 + nz * gz, 8), nz)
    fetches[0].wait()
    layer = iota((nz, lanes), 0)
    own_depths = jnp.zeros((nz, lanes), F32)
    for z in range(nz):
        own_depths = jnp.where(layer == z, PRE * depth_ref[z], own_depths)
    depths[own_layers, :] = own_depths

    def domain(count):
        r, c = iota((count, lanes), 0), iota((count, lanes), 1)
        half = (count - nx) // 2
        in_x = (r < nx) | ((r < nx + half) & (gx < ngx - 1)) | ((r >= nx + half) & (gx > 0))
        in_y = (c < ny) | ((c < ny + ny // 2) & (gy < ngy - 1)) | ((c >= ny + ny // 2) & (gy > 0))
        return (in_x & in_y).astype(F32)

    zero_plane = jnp.zeros((rows, lanes), F32)
    for edge in (0, 2 * nz + 1):
        div[edge] = zero_plane
        for c in range(3):
            w1[c, edge] = zero_plane
            w2[c, edge] = zero_plane
    blocks, epochs, pixels = observed_ref.shape
    for fetch in fetches[1:9]:
        fetch.wait()

    for b in range(blocks):
        for k, source in enumerate((count_ref, table_ref, patch_ref, owner_ref)):
            numbers[k, b:b + 1, :] = jnp.full((1, ny), source[b], jnp.int32)
    in_scene = iota((blocks, ny), 1)
    for k in range(0, pixels, ny):
        kept = (in_scene + k < numbers[0]).astype(F32)
        valid[:, k:k + ny] = coherence_ref[:, k:k + ny].astype(F32) * kept
    for b in range(blocks):
        resid[epochs * b:epochs * (b + 1), :] = (predicted_ref[b] - observed_ref[b]) * valid[b:b + 1, :]
    res = resid[...]
    row_block, row_place = iota((blocks, epochs * blocks), 0), iota((blocks, epochs * blocks), 1)
    own_rows = row_place // epochs == row_block
    mixes = []
    for c in range(3):
        mix = jnp.zeros((blocks, epochs * blocks), F32)
        for e in range(epochs):
            mix = jnp.where(own_rows & (row_place % epochs == e), look_ref[e, c], mix)
        mixes.append(mix)
    coeffs[...] = jnp.dot(
        jnp.concatenate(mixes, axis=0), res, precision=HIGHEST, preferred_element_type=F32
    )
    mass = jnp.sum(jnp.sum(res * res, axis=0, keepdims=True), axis=1, keepdims=True)
    weight = jnp.sum(jnp.sum(valid[...], axis=0, keepdims=True), axis=1, keepdims=True)

    lane_owner = iota((blocks, owners), 1)
    at_owner = (lane_owner == numbers[3, :, 0:owners]).astype(F32)
    before = (iota((blocks, blocks), 1) < iota((blocks, blocks), 0)).astype(F32)
    ahead_of = jnp.dot(before, at_owner, preferred_element_type=F32)
    rank = jnp.sum(ahead_of * at_owner, axis=1, keepdims=True).astype(jnp.int32)
    slot_of = numbers[3, :, 0:1] * CAP + rank
    select = (iota((blocks, owners * CAP), 1) == slot_of).astype(F32)
    at_lane = (iota((blocks, ny), 1) == rank * (ny // CAP) + numbers[2]).astype(F32)
    marks = lax.dot_general(at_owner, at_lane, (((0,), (0,)), ((), ())), preferred_element_type=F32)
    for o in range(owners):
        choice_ref[o] = marks[o:o + 1]

    rounded = coeffs[...].astype(jnp.bfloat16).astype(F32)
    which = jnp.concatenate([numbers[1]] * 3, axis=0)
    which = jnp.concatenate([which] * (pixels // ny), axis=1)
    fetches[9].wait()
    fetches[10].wait()
    for z in range(nz):
        stiff_edge[0, z] = stiff_ref[z, 0:4]
        stiff_edge[1, z] = stiff_ref[z, nx - 4:nx]
    total_sums = jnp.zeros((3 * blocks, ny), F32)
    for t in range(weights.shape[0]):
        taken = jnp.where(which == t, rounded, 0.0).astype(jnp.bfloat16)
        total_sums = total_sums + jnp.dot(taken, weights[t], preferred_element_type=F32)
    chosen = lax.dot_general(
        select, jnp.concatenate([total_sums[c * blocks:(c + 1) * blocks] for c in range(3)], axis=1),
        (((0,), (0,)), ((), ())), precision=HIGHEST, preferred_element_type=F32,
    )
    for c in range(3):
        for o in range(owners):
            slots_ref[o, c] = chosen[CAP * o:CAP * (o + 1), c * ny:(c + 1) * ny]

    pl.semaphore_wait(barrier, (ngx - 1) * ngy + len(peers))

    def remote(source, target, index, device, arrival=None):
        return pltpu.make_async_remote_copy(
            src_ref=source, dst_ref=target, send_sem=send_sem.at[index],
            recv_sem=recv_sem.at[index if arrival is None else arrival],
            device_id=device, device_id_type=pl.DeviceIdType.MESH,
        )

    x_up, x_down = wrap(gx + 1, ngx), wrap(gx - 1, ngx)
    y_up, y_down = wrap(gy + 1, ngy), wrap(gy - 1, ngy)
    to_down = remote(stiff_edge.at[0], stiff_x.at[0], 0, at(x_down, gy, gz))
    to_up = remote(stiff_edge.at[1], stiff_x.at[1], 1, at(x_up, gy, gz))
    to_other = remote(depths.at[own_layers, :], depths.at[own_layers, :], 2, at(gx, gy, other))
    to_other.start()

    to_down.start()
    to_up.start()
    def post(j, first):
        for k in range(first, ngy):
            y = wrap(gy + k, ngy)
            o = j * ngy + y
            for message, (source, target) in enumerate(((slots_ref, got_slots), (choice_ref, got_choice))):
                pltpu.make_async_remote_copy(
                    src_ref=source.at[o], dst_ref=target.at[me],
                    send_sem=send_a2a.at[message], recv_sem=recv_a2a.at[message],
                    device_id=at(j, y, gz), device_id_type=pl.DeviceIdType.MESH,
                ).start()

    def post_pair(i, carry):
        d = ngx // 2 - i
        post(wrap(gx - d, ngx), 0)

        @pl.when(d < ngx // 2)
        def _():
            post(wrap(gx + d, ngx), 0)

        return carry

    lax.fori_loop(0, ngx // 2, post_pair, 0)
    post(gx, 1)

    got_slots[me] = slots_ref[me]
    got_choice[me] = choice_ref[me]

    to_down.wait_recv()
    to_up.wait_recv()
    to_other.wait_recv()
    sent = [to_down, to_up, to_other]
    for z in range(nz):
        wide_stiff[z, 0:nx, :] = stiff_ref[z]
        wide_stiff[z, nx:nx + 4, :] = stiff_x[0, z]
        wide_stiff[z, nx + 4:rows, :] = stiff_x[1, z]
    turned = wide_stiff[...].reshape(nz * rows, ny).T
    strip_out[0] = turned[0:8]
    strip_out[1] = turned[ny - 8:ny]
    strips = [
        remote(strip_out.at[0], strip_in.at[0], 3, at(gx, y_down, gz)),
        remote(strip_out.at[1], strip_in.at[1], 4, at(gx, y_up, gz)),
    ]
    for copy in strips:
        copy.start()

    d = depths[...]
    where_z = iota(d.shape, 0)
    inside = ((where_z >= 8) & (where_z < 8 + 2 * nz)).astype(F32)
    d_up, d_down = ahead(d, 0), behind(d, 0)
    q = 0.5 * (d_up - d_down)
    kept_d, kept_q = inside * d, inside * q
    columns = (
        d,
        0.125 * (d_up + d_down),
        q,
        (1.0 / 32.0) * (ahead(kept_d, 0) - behind(kept_d, 0)),
        (1.0 / 32.0) * (ahead(kept_q, 0) - behind(kept_q, 0)),
    )
    for k, values in enumerate(columns):
        for z in range(2 * nz):
            table[k, z] = values[z + 8:z + 9]

    for copy in strips:
        copy.wait_recv()
    sent = sent + strips
    filler = jnp.zeros((ny - 16, nz * rows), F32)
    beside = jnp.concatenate([strip_in[0], filler, strip_in[1]], axis=0).T.reshape(nz, rows, ny)
    base = nz * gz
    for z in range(nz):
        coef[base + z, :, 0:ny] = 0.125 * wide_stiff[z] - 0.25
        coef[base + z, :, ny:lanes] = 0.125 * beside[z] - 0.25
    passed = pl.ds((nz - 4) + 4 * gz, 4)
    layers = remote(coef.at[passed], coef.at[passed], 5, at(gx, gy, other))
    layers.start()

    for message, buffer in enumerate((got_slots, got_choice)):
        part = buffer.at[pl.ds(0, owners - 1)]
        pltpu.make_async_copy(part, part, recv_a2a.at[message]).wait()
    own_slot = iota((CAP, ny), 1) // (ny // CAP) == iota((CAP, ny), 0)
    for o in range(owners):
        for c in range(3):
            flat_slots[CAP * o:CAP * (o + 1), c * ny:(c + 1) * ny] = got_slots[o, c]
        flat_choice[CAP * o:CAP * (o + 1), :] = jnp.where(own_slot, got_choice[o], 0.0)
    picked = flat_choice[...]
    spread = lax.dot_general(
        picked, flat_slots[...], (((0,), (0,)), ((), ())), precision=HIGHEST, preferred_element_type=F32
    )
    depth_places = ny // CAP
    tiles = []
    for c in range(3):
        placed = spread[0:depth_places, c * ny:(c + 1) * ny]
        for j in range(1, CAP):
            placed = placed + spread[j * depth_places:(j + 1) * depth_places, c * ny:(c + 1) * ny]
        tiles.append(placed)
    tile = jnp.concatenate(tiles, axis=0)
    sub = lax.rem(iota(tile.shape, 0), 8)
    chunk = iota(tile.shape, 1) // PATCH_Y
    for bit in (1, 2, 4):
        row_set, chunk_set = (sub // bit) % 2 == 1, (chunk // bit) % 2 == 1
        from_below = roll(roll(tile, -bit, 0), bit * PATCH_Y, 1)
        from_above = roll(roll(tile, bit, 0), -bit * PATCH_Y, 1)
        tile = jnp.where(row_set == chunk_set, tile, jnp.where(row_set, from_above, from_below))
    surf[...] = tile.reshape(3, nx, ny)
    turned = jnp.concatenate([tile, jnp.zeros((ny - 3 * nx, ny), F32)], axis=0).T
    border[0] = turned[0:8]
    border[1] = turned[ny - 8:ny]

    swap = remote(surf, surf_other, 6, at(gx, gy, other))
    swap.start()
    first, last = pl.ds(0, 8), pl.ds(nx - 8, 8)
    ways = (
        (surf.at[:, first, :], halo_x, 0, x_down, gy),
        (surf.at[:, last, :], halo_x, 1, x_up, gy),
        (border.at[0], halo_y, 0, gx, y_down),
        (border.at[1], halo_y, 1, gx, y_up),
        (border.at[0], halo_y, 2, x_down, y_down),
        (border.at[1], halo_y, 3, x_down, y_up),
        (border.at[0], halo_y, 4, x_up, y_down),
        (border.at[1], halo_y, 5, x_up, y_up),
    )
    count = len(ways)
    started = []
    for k in reversed(range(count)):
        source, target, place, x, y = ways[k]
        for i, z in enumerate((gz, other)):
            copy = remote(source, target.at[gz, place], 7 + i * count + k, at(x, y, z), 7 + gz * count + k)
            copy.start()
            started.append(copy)
    swap.wait_recv()
    for k, (source, target, place, x, y) in enumerate(ways):
        for i in range(2):
            remote(source, target.at[i, place], 7 + i * count + k, at(x, y, gz)).wait_recv()
    sent = sent + [swap] + started
    mask_tall = domain(tall)
    mask = domain(rows)
    low_rows = iota((8, lanes), 0) < 4

    def packed(values):
        return jnp.concatenate(
            [values[0:nx], jnp.where(low_rows, values[nx:nx + 8], values[nx + 8:nx + 16])], axis=0
        )

    blank = jnp.zeros((ny - 16, ny), F32)

    def columns_of(place):
        low_side, high_side = halo_y[0, place] + halo_y[1, place], halo_y[0, place + 1] + halo_y[1, place + 1]
        return jnp.concatenate([low_side, blank, high_side], axis=0).T[0:3 * nx].reshape(3, nx, ny)

    near, upper, lower = columns_of(0), columns_of(2), columns_of(4)
    around = []
    for c in range(3):
        main = jnp.concatenate(
            [surf[c] + surf_other[c], halo_x[0, 0, c] + halo_x[1, 0, c], halo_x[0, 1, c] + halo_x[1, 1, c]], axis=0
        )
        side = jnp.concatenate([near[c], upper[c, 0:8], lower[c, nx - 8:nx]], axis=0)
        around.append(mask_tall * jnp.concatenate([main, side], axis=1))
    flux = mask_tall * (
        0.5 * ((ahead(around[0], 0) - behind(around[0], 0)) + (ahead(around[1], 1) - behind(around[1], 1)))
    )
    for c in range(3):
        s = around[c]
        beside_xy = (ahead(s, 0) + behind(s, 0)) + (ahead(s, 1) + behind(s, 1))
        fields[c] = packed(s)
        if c < 2:
            drop = 0.125 * beside_xy + (1.0 / 32.0) * (ahead(flux, c) - behind(flux, c))
            fields[3 + c] = mask * packed(drop)
            fields[6 + c] = mask * packed((1.0 / 32.0) * (ahead(around[2], c) - behind(around[2], c)))
        else:
            fields[3 + c] = mask * packed(0.125 * beside_xy)
    fields[8] = packed(flux)

    layers.wait_recv()
    sent = sent + [layers]

    def first_layer(i, carry):
        z = (nz - 4) * gz + i
        value = [table[k, z] for k in range(5)]
        own = coef[z] * value[0] - value[1]
        for c in range(2):
            w1[c, z + 1] = mask * (fields[c] * own) - value[0] * fields[3 + c] - value[2] * fields[6 + c]
        w1[2, z + 1] = mask * (fields[2] * (own - value[4])) - value[0] * fields[5] - value[3] * fields[8]
        return carry

    pairwise(0, nz + 4, first_layer)

    def spread_of(source, start, amount):
        def layer(i, carry):
            z = start + i
            x, y = source[0, z + 1], source[1, z + 1]
            div[z + 1] = mask * (
                ((ahead(x, 0) - behind(x, 0)) + (ahead(y, 1) - behind(y, 1)))
                + (source[2, z + 2] - source[2, z])
            )
            return carry

        pairwise(0, amount, layer)

    spread_of(w1, (nz - 3) * gz, nz + 3)

    def second_layer(i, carry):
        z = (nz - 2) * gz + i
        own = coef[z]
        here = div[z + 1]
        for c in range(3):
            v = w1[c, z + 1]
            total = (ahead(v, 0) + behind(v, 0)) + (ahead(v, 1) + behind(v, 1))
            total = total + (w1[c, z + 2] + w1[c, z])
            slope = (ahead(here, c) - behind(here, c)) if c < 2 else (div[z + 2] - div[z])
            w2[c, z + 1] = mask * (own * v - 0.125 * total - (1.0 / 64.0) * slope)
        return carry

    pairwise(0, nz + 2, second_layer)

    def folded(values):
        total = values[0:8]
        for k in range(8, nx, 8):
            total = total + values[k:k + 8]
        return total

    def gather_moments(i, sums):
        z = nz * gz + i
        own = coef[z, 0:nx, 0:ny]
        d_now = table[0, z, :, 0:ny]
        terms = [None] * MOMENTS
        here = w2[2, z + 2, 0:nx, 0:ny] - w2[2, z, 0:nx, 0:ny]
        for c in range(3):
            v = w2[c, z + 1, 0:nx, 0:ny]
            vx, vy = w2[c, z + 1, :, 0:ny], w2[c, z + 1, 0:nx, :]
            next_x, next_y = ahead(vx, 0)[0:nx], ahead(vy, 1)[:, 0:ny]
            total = (next_x + next_y) + w2[c, z + 2, 0:nx, 0:ny]
            if c == 0:
                here = here + (next_x - behind(vx, 0)[0:nx])
            elif c == 1:
                here = here + (next_y - behind(vy, 1)[:, 0:ny])
            zeroth = d_now * fields[c, 0:nx, 0:ny]
            one = w1[c, z + 1, 0:nx, 0:ny]
            for k, term in enumerate(
                (zeroth * zeroth, zeroth * one, one * one, one * v, v * v, v * (own * v - 0.25 * total))
            ):
                terms[k] = term if terms[k] is None else terms[k] + term
        terms[MOMENTS - 1] = terms[MOMENTS - 1] + (1.0 / 64.0) * (here * here)
        return tuple(s + folded(t) for s, t in zip(sums, terms))

    sums = lax.fori_loop(
        0, nz // 2, lambda k, sums: gather_moments(2 * k + 1, gather_moments(2 * k, sums)),
        tuple(jnp.zeros((8, ny), F32) for _ in range(MOMENTS)),
    )

    def third_layer(i, carry):
        z = nz * gz + i
        own = coef[z, 0:nx, 0:ny]
        here_x, here_y = div[z + 1, :, 0:ny], div[z + 1, 0:nx, :]
        for c in range(3):
            v = w2[c, z + 1, 0:nx, 0:ny]
            vx, vy = w2[c, z + 1, :, 0:ny], w2[c, z + 1, 0:nx, :]
            total = (ahead(vx, 0) + behind(vx, 0))[0:nx] + (ahead(vy, 1) + behind(vy, 1))[:, 0:ny]
            total = total + (w2[c, z + 2, 0:nx, 0:ny] + w2[c, z, 0:nx, 0:ny])
            if c == 0:
                slope = (ahead(here_x, 0) - behind(here_x, 0))[0:nx]
            elif c == 1:
                slope = (ahead(here_y, 1) - behind(here_y, 1))[:, 0:ny]
            else:
                slope = div[z + 2, 0:nx, 0:ny] - div[z, 0:nx, 0:ny]
            res_ref[c, i] = own * v - 0.125 * total - (1.0 / 64.0) * slope
        return carry

    early_layers = nz // 4

    lane = iota((1, ny), 1)
    message = jnp.where(lane == MOMENTS, mass, 0.0) + jnp.where(lane == MOMENTS + 1, weight, 0.0)
    for k in range(MOMENTS):
        amount = jnp.sum(jnp.sum(sums[k], axis=0, keepdims=True), axis=1, keepdims=True)
        message = message + jnp.where(lane == k, amount, 0.0)
    row_out[0] = message
    slot = gy * 2 + gz
    row_in[slot] = message
    base = 7 + 2 * count
    started = []
    for k, (y, z) in enumerate(peers):
        copy = remote(row_out.at[0], row_in.at[slot], base + k, at(gx, y, z))
        copy.start()
        started.append(copy)
    spread_of(w2, (nz - 1) * gz, nz + 1)
    pairwise(0, early_layers, third_layer)
    for copy in started:
        copy.wait_recv()
    sent = sent + started
    message = row_in[0]
    for k in range(1, 2 * ngy):
        message = message + row_in[k]
    row_out[1] = message
    ring_in[gx] = message
    first_index = base + len(peers)
    started = []
    for k in range(1, ngx):
        copy = remote(row_out.at[1], ring_in.at[gx], first_index + k - 1, at(wrap(gx + k, ngx), gy, gz))
        copy.start()
        started.append(copy)
    pairwise(early_layers, nz, third_layer)
    for copy in started:
        copy.wait_recv()
    sent = sent + started
    message = ring_in[0]
    for k in range(1, ngx):
        message = message + ring_in[k]
    parts = [jnp.sum(jnp.where(lane == k, message, 0.0), axis=1, keepdims=True) for k in range(MOMENTS + 2)]

    scale = lax.rsqrt(parts[MOMENTS] / (EPOCHS * parts[MOMENTS + 1]) + EPS) * (1.0 / PRE)
    iterate, residual = conjugate(parts[0:MOMENTS])
    iterate = [scale * value for value in iterate]
    residual = [scale * value for value in residual]

    def finish(i, carry):
        z = nz * gz + i
        d_now = table[0, z, :, 0:ny]
        for c in range(3):
            zeroth = d_now * fields[c, 0:nx, 0:ny]
            one, two = w1[c, z + 1, 0:nx, 0:ny], w2[c, z + 1, 0:nx, 0:ny]
            third = res_ref[c, i]
            adj_ref[c, i] = iterate[0] * zeroth + iterate[1] * one + iterate[2] * two
            res_ref[c, i] = residual[0] * zeroth + residual[1] * one + residual[2] * two + residual[3] * third
        return carry

    pairwise(0, nz, finish)
    for copy in sent:
        copy.wait_send()
    for message, buffer in enumerate((slots_ref, choice_ref)):
        part = buffer.at[pl.ds(0, owners - 1)]
        pltpu.make_async_copy(part, part, send_a2a.at[message]).wait()


def per_device(
    observed,
    predicted,
    coherence_mask,
    block_count,
    block_owner,
    block_matrix_choice,
    block_patch,
    look_vector,
    interp_weights,
    depth_kernel,
    stiffness,
):
    blocks, epochs, pixels = observed.shape
    cells = PATCH_X * PATCH_Y
    ngx, ngy = lax.axis_size("gx"), lax.axis_size("gy")
    owners = ngx * ngy
    nz, nx, ny = stiffness.shape

    rows, lanes = nx + 8, 2 * ny
    out = pltpu.VMEM((3, nz, nx, ny), F32)
    vmem = pl.BlockSpec(memory_space=pltpu.VMEM)
    far = pl.BlockSpec(memory_space=pltpu.HBM)
    copies = 23 + (2 * ngy - 1) + (ngx - 1)
    return pl.pallas_call(
        kernel,
        out_shape=(out, out),
        in_specs=[far] * 11,
        out_specs=(vmem, vmem),
        scratch_shapes=[
            pltpu.VMEM(observed.shape, F32),
            pltpu.VMEM(predicted.shape, F32),
            pltpu.VMEM(coherence_mask.shape, jnp.int32),
            pltpu.SMEM((blocks,), jnp.int32),
            pltpu.SMEM((blocks,), jnp.int32),
            pltpu.SMEM((blocks,), jnp.int32),
            pltpu.SMEM((blocks,), jnp.int32),
            pltpu.SMEM(look_vector.shape, F32),
            pltpu.VMEM(interp_weights.shape, interp_weights.dtype),
            pltpu.SMEM((nz,), F32),
            pltpu.VMEM(stiffness.shape, F32),
            pltpu.VMEM((4, blocks, ny), jnp.int32),
            pltpu.VMEM((blocks, pixels), F32),
            pltpu.VMEM((epochs * blocks, pixels), F32),
            pltpu.VMEM((3 * blocks, pixels), F32),
            pltpu.VMEM((owners, 3, CAP, cells), F32),
            pltpu.VMEM((owners, 1, cells), F32),
            pltpu.VMEM((owners, 3, CAP, cells), F32),
            pltpu.VMEM((owners, 1, cells), F32),
            pltpu.VMEM((owners * CAP, 3 * cells), F32),
            pltpu.VMEM((owners * CAP, cells), F32),
            pltpu.VMEM((3, nx, ny), F32),
            pltpu.VMEM((3, nx, ny), F32),
            pltpu.VMEM((2, 8, ny), F32),
            pltpu.VMEM((2, 2, 3, 8, ny), F32),
            pltpu.VMEM((2, 6, 8, ny), F32),
            pltpu.VMEM((2, nz, 4, ny), F32),
            pltpu.VMEM((2, nz, 4, ny), F32),
            pltpu.VMEM((nz, rows, ny), F32),
            pltpu.VMEM((2, 8, nz * rows), F32),
            pltpu.VMEM((2, 8, nz * rows), F32),
            pltpu.VMEM((2 * nz, rows, lanes), F32),
            pltpu.VMEM((2 * nz + 16, lanes), F32),
            pltpu.VMEM((5, 2 * nz, 1, lanes), F32),
            pltpu.VMEM((9, rows, lanes), F32),
            pltpu.VMEM((3, 2 * nz + 2, rows, lanes), F32),
            pltpu.VMEM((3, 2 * nz + 2, rows, lanes), F32),
            pltpu.VMEM((2 * nz + 2, rows, lanes), F32),
            pltpu.VMEM((2, 1, ny), F32),
            pltpu.VMEM((2 * ngy, 1, ny), F32),
            pltpu.VMEM((ngx, 1, ny), F32),
            pltpu.SemaphoreType.DMA((2,)),
            pltpu.SemaphoreType.DMA((2,)),
            pltpu.SemaphoreType.DMA((copies,)),
            pltpu.SemaphoreType.DMA((copies,)),
            pltpu.SemaphoreType.DMA((11,)),
        ],
        compiler_params=pltpu.CompilerParams(
            collective_id=0, has_side_effects=True, vmem_limit_bytes=60000000
        ),
    )(
        observed, predicted, coherence_mask, block_count, block_owner[:, 0], block_matrix_choice, block_patch,
        look_vector, interp_weights, depth_kernel, stiffness,
    )


def solution(mesh):
    in_specs = (
        P(("grp", "gx", "gy", "gz"), None, None),
        P(("grp", "gx", "gy", "gz"), None, None),
        P(("grp", "gx", "gy", "gz"), None),
        P(("grp", "gx", "gy", "gz")),
        P(("grp", "gx", "gy", "gz"), None),
        P(("grp", "gx", "gy", "gz")),
        P(("grp", "gx", "gy", "gz")),
        P(),
        P(),
        P(("grp", "gz")),
        P(("grp", "gz"), "gx", "gy"),
    )
    out_specs = (P(None, ("grp", "gz"), "gx", "gy"), P(None, ("grp", "gz"), "gx", "gy"))
    return jax.shard_map(
        per_device, mesh=mesh, in_specs=in_specs, out_specs=out_specs, check_vma=False
    )
```

```python
import jax
import jax.numpy as jnp
from jax import lax
from jax.experimental import pallas as pl
from jax.experimental.pallas import tpu as pltpu
from jax.sharding import PartitionSpec as P

EPOCHS = 4
PATCH_X = 8
PATCH_Y = 16
CAP = 4
EPS = 1e-06

SHIFT = 8.0
PRE = 1024.0
MOMENTS = 6

HIGHEST = lax.Precision.HIGHEST
F32 = jnp.float32


def roll(values, shift, axis):
    return pltpu.roll(values, shift % values.shape[axis], axis)


def ahead(values, axis):
    return roll(values, -1, axis)


def behind(values, axis):
    return roll(values, 1, axis)


def iota(shape, axis):
    return lax.broadcasted_iota(jnp.int32, shape, axis)


def pairwise(start, stop, body):
    def trip(k, carry):
        body(start + 2 * k, None)
        body(start + 2 * k + 1, None)
        return carry

    lax.fori_loop(0, (stop - start) // 2, trip, 0)
    if (stop - start) % 2:
        body(stop - 1, None)


def product(first, second, moments):
    total = None
    for i, f in enumerate(first):
        for j, g in enumerate(second):
            term = f * g * moments[i + j]
            total = term if total is None else total + term
    return total


def combined(first, factor, second):
    size = max(len(first), len(second))
    out = []
    for i in range(size):
        value = first[i] if i < len(first) else None
        if i < len(second):
            term = factor * second[i]
            value = term if value is None else value + term
        out.append(value)
    return out


def applied(poly):
    out = []
    for i in range(len(poly) + 1):
        value = None
        for j in (i, i - 1):
            if 0 <= j < len(poly):
                value = poly[j] if value is None else value + poly[j]
        out.append(SHIFT * value)
    return out


def conjugate(moments):
    one = jnp.ones_like(moments[0])
    residual, direction, iterate = [one], [one], []
    now = moments[0]
    for step in range(3):
        image = applied(direction)
        alpha = now / product(direction, image, moments)
        scaled = [alpha * d for d in direction]
        iterate = scaled if not iterate else combined(iterate, one, scaled)
        residual = combined(residual, -alpha, image)
        if step < 2:
            new = product(residual, residual, moments)
            direction = combined(residual, new / now, direction)
            now = new
    return iterate, residual


def kernel(
    observed_hbm, predicted_hbm, coherence_hbm, count_hbm, owner_hbm, table_hbm, patch_hbm, look_hbm,
    weights_hbm, depth_hbm, stiff_hbm,
    adj_ref, res_ref,
    observed_ref, predicted_ref, coherence_ref, count_ref, owner_ref, table_ref, patch_ref, look_ref,
    weights, depth_ref, stiff_ref,
    numbers, valid, resid, coeffs, slots_ref, choice_ref,
    got_slots, got_choice, flat_slots, flat_choice,
    surf, surf_other, border, halo_x, halo_y,
    stiff_edge, stiff_x, wide_stiff, strip_out, strip_in, coef,
    depths, table,
    fields, w1, w2, div,
    row_out, row_in, ring_in,
    send_a2a, recv_a2a, send_sem, recv_sem, local_sem,
):
    pairs = (
        (depth_hbm, depth_ref), (count_hbm, count_ref), (owner_hbm, owner_ref), (table_hbm, table_ref),
        (patch_hbm, patch_ref), (look_hbm, look_ref), (coherence_hbm, coherence_ref),
        (predicted_hbm, predicted_ref), (observed_hbm, observed_ref), (weights_hbm, weights), (stiff_hbm, stiff_ref),
    )
    fetches = [pltpu.make_async_copy(a, b, local_sem.at[i]) for i, (a, b) in enumerate(pairs)]
    for fetch in fetches:
        fetch.start()
    gx, gy, gz = lax.axis_index("gx"), lax.axis_index("gy"), lax.axis_index("gz")
    ngx, ngy = lax.axis_size("gx"), lax.axis_size("gy")
    owners = ngx * ngy
    me = gx * ngy + gy
    nz, nx, ny = stiff_ref.shape
    other = 1 - gz
    rows, lanes = nx + 8, 2 * ny
    tall = nx + 16

    def at(x, y, z):
        return {"gx": x, "gy": y, "gz": z}

    def wrap(value, count):
        return lax.rem(value + count, count)

    depths[...] = jnp.zeros(depths.shape, F32)

    barrier = pltpu.get_barrier_semaphore()
    far_first = sorted(range(ngy), key=lambda k: -min(k, ngy - k))
    peers = [(wrap(gy + k, ngy), z) for k in far_first for z in (gz, other) if k or z is other]

    def greet(k, carry):
        j = wrap(gx - k, ngx)
        for y in range(ngy):
            pl.semaphore_signal(barrier, inc=1, device_id=at(j, y, gz))
        return carry

    lax.fori_loop(1, ngx, greet, 0)
    for y, z in peers:
        pl.semaphore_signal(barrier, inc=1, device_id=at(gx, y, z))

    own_layers = pl.ds(pl.multiple_of(8 + nz * gz, 8), nz)
    fetches[0].wait()
    layer = iota((nz, lanes), 0)
    own_depths = jnp.zeros((nz, lanes), F32)
    for z in range(nz):
        own_depths = jnp.where(layer == z, PRE * depth_ref[z], own_depths)
    depths[own_layers, :] = own_depths

    def domain(count):
        r, c = iota((count, lanes), 0), iota((count, lanes), 1)
        half = (count - nx) // 2
        in_x = (r < nx) | ((r < nx + half) & (gx < ngx - 1)) | ((r >= nx + half) & (gx > 0))
        in_y = (c < ny) | ((c < ny + ny // 2) & (gy < ngy - 1)) | ((c >= ny + ny // 2) & (gy > 0))
        return (in_x & in_y).astype(F32)

    zero_plane = jnp.zeros((rows, lanes), F32)
    for edge in (0, 2 * nz + 1):
        div[edge] = zero_plane
        for c in range(3):
            w1[c, edge] = zero_plane
            w2[c, edge] = zero_plane
    blocks, epochs, pixels = observed_ref.shape
    for fetch in fetches[1:9]:
        fetch.wait()

    for b in range(blocks):
        for k, source in enumerate((count_ref, table_ref, patch_ref, owner_ref)):
            numbers[k, b:b + 1, :] = jnp.full((1, ny), source[b], jnp.int32)
    in_scene = iota((blocks, ny), 1)
    for k in range(0, pixels, ny):
        kept = (in_scene + k < numbers[0]).astype(F32)
        valid[:, k:k + ny] = coherence_ref[:, k:k + ny].astype(F32) * kept
    for b in range(blocks):
        resid[epochs * b:epochs * (b + 1), :] = (predicted_ref[b] - observed_ref[b]) * valid[b:b + 1, :]
    res = resid[...]
    row_block, row_place = iota((blocks, epochs * blocks), 0), iota((blocks, epochs * blocks), 1)
    own_rows = row_place // epochs == row_block
    mixes = []
    for c in range(3):
        mix = jnp.zeros((blocks, epochs * blocks), F32)
        for e in range(epochs):
            mix = jnp.where(own_rows & (row_place % epochs == e), look_ref[e, c], mix)
        mixes.append(mix)
    coeffs[...] = jnp.dot(
        jnp.concatenate(mixes, axis=0), res, precision=HIGHEST, preferred_element_type=F32
    )
    mass = jnp.sum(jnp.sum(res * res, axis=0, keepdims=True), axis=1, keepdims=True)
    weight = jnp.sum(jnp.sum(valid[...], axis=0, keepdims=True), axis=1, keepdims=True)

    lane_owner = iota((blocks, owners), 1)
    at_owner = (lane_owner == numbers[3, :, 0:owners]).astype(F32)
    before = (iota((blocks, blocks), 1) < iota((blocks, blocks), 0)).astype(F32)
    ahead_of = jnp.dot(before, at_owner, preferred_element_type=F32)
    rank = jnp.sum(ahead_of * at_owner, axis=1, keepdims=True).astype(jnp.int32)
    slot_of = numbers[3, :, 0:1] * CAP + rank
    select = (iota((blocks, owners * CAP), 1) == slot_of).astype(F32)
    at_lane = (iota((blocks, ny), 1) == rank * (ny // CAP) + numbers[2]).astype(F32)
    marks = lax.dot_general(at_owner, at_lane, (((0,), (0,)), ((), ())), preferred_element_type=F32)
    for o in range(owners):
        choice_ref[o] = marks[o:o + 1]

    rounded = coeffs[...].astype(jnp.bfloat16).astype(F32)
    which = jnp.concatenate([numbers[1]] * 3, axis=0)
    which = jnp.concatenate([which] * (pixels // ny), axis=1)
    fetches[9].wait()
    fetches[10].wait()
    for z in range(nz):
        stiff_edge[0, z] = stiff_ref[z, 0:4]
        stiff_edge[1, z] = stiff_ref[z, nx - 4:nx]
    total_sums = jnp.zeros((3 * blocks, ny), F32)
    for t in range(weights.shape[0]):
        taken = jnp.where(which == t, rounded, 0.0).astype(jnp.bfloat16)
        total_sums = total_sums + jnp.dot(taken, weights[t], preferred_element_type=F32)
    chosen = lax.dot_general(
        select, jnp.concatenate([total_sums[c * blocks:(c + 1) * blocks] for c in range(3)], axis=1),
        (((0,), (0,)), ((), ())), precision=HIGHEST, preferred_element_type=F32,
    )
    for c in range(3):
        for o in range(owners):
            slots_ref[o, c] = chosen[CAP * o:CAP * (o + 1), c * ny:(c + 1) * ny]

    pl.semaphore_wait(barrier, (ngx - 1) * ngy + len(peers))

    def remote(source, target, index, device, arrival=None):
        return pltpu.make_async_remote_copy(
            src_ref=source, dst_ref=target, send_sem=send_sem.at[index],
            recv_sem=recv_sem.at[index if arrival is None else arrival],
            device_id=device, device_id_type=pl.DeviceIdType.MESH,
        )

    x_up, x_down = wrap(gx + 1, ngx), wrap(gx - 1, ngx)
    y_up, y_down = wrap(gy + 1, ngy), wrap(gy - 1, ngy)
    to_down = remote(stiff_edge.at[0], stiff_x.at[0], 0, at(x_down, gy, gz))
    to_up = remote(stiff_edge.at[1], stiff_x.at[1], 1, at(x_up, gy, gz))
    to_other = remote(depths.at[own_layers, :], depths.at[own_layers, :], 2, at(gx, gy, other))
    to_other.start()

    to_down.start()
    to_up.start()
    def post(j, first):
        for k in range(first, ngy):
            y = wrap(gy + k, ngy)
            o = j * ngy + y
            for message, (source, target) in enumerate(((slots_ref, got_slots), (choice_ref, got_choice))):
                pltpu.make_async_remote_copy(
                    src_ref=source.at[o], dst_ref=target.at[me],
                    send_sem=send_a2a.at[message], recv_sem=recv_a2a.at[message],
                    device_id=at(j, y, gz), device_id_type=pl.DeviceIdType.MESH,
                ).start()

    def post_pair(i, carry):
        d = ngx // 2 - i
        post(wrap(gx - d, ngx), 0)

        @pl.when(d < ngx // 2)
        def _():
            post(wrap(gx + d, ngx), 0)

        return carry

    lax.fori_loop(0, ngx // 2, post_pair, 0)
    post(gx, 1)

    got_slots[me] = slots_ref[me]
    got_choice[me] = choice_ref[me]

    to_down.wait_recv()
    to_up.wait_recv()
    to_other.wait_recv()
    sent = [to_down, to_up, to_other]
    for z in range(nz):
        wide_stiff[z, 0:nx, :] = stiff_ref[z]
        wide_stiff[z, nx:nx + 4, :] = stiff_x[0, z]
        wide_stiff[z, nx + 4:rows, :] = stiff_x[1, z]
    turned = wide_stiff[...].reshape(nz * rows, ny).T
    strip_out[0] = turned[0:8]
    strip_out[1] = turned[ny - 8:ny]
    strips = [
        remote(strip_out.at[0], strip_in.at[0], 3, at(gx, y_down, gz)),
        remote(strip_out.at[1], strip_in.at[1], 4, at(gx, y_up, gz)),
    ]
    for copy in strips:
        copy.start()

    d = depths[...]
    where_z = iota(d.shape, 0)
    inside = ((where_z >= 8) & (where_z < 8 + 2 * nz)).astype(F32)
    d_up, d_down = ahead(d, 0), behind(d, 0)
    q = 0.5 * (d_up - d_down)
    kept_d, kept_q = inside * d, inside * q
    columns = (
        d,
        0.125 * (d_up + d_down),
        q,
        (1.0 / 32.0) * (ahead(kept_d, 0) - behind(kept_d, 0)),
        (1.0 / 32.0) * (ahead(kept_q, 0) - behind(kept_q, 0)),
    )
    for k, values in enumerate(columns):
        for z in range(2 * nz):
            table[k, z] = values[z + 8:z + 9]

    for copy in strips:
        copy.wait_recv()
    sent = sent + strips
    filler = jnp.zeros((ny - 16, nz * rows), F32)
    beside = jnp.concatenate([strip_in[0], filler, strip_in[1]], axis=0).T.reshape(nz, rows, ny)
    base = nz * gz
    for z in range(nz):
        coef[base + z, :, 0:ny] = 0.125 * wide_stiff[z] - 0.25
        coef[base + z, :, ny:lanes] = 0.125 * beside[z] - 0.25
    passed = pl.ds((nz - 4) + 4 * gz, 4)
    layers = remote(coef.at[passed], coef.at[passed], 5, at(gx, gy, other))
    layers.start()

    for message, buffer in enumerate((got_slots, got_choice)):
        part = buffer.at[pl.ds(0, owners - 1)]
        pltpu.make_async_copy(part, part, recv_a2a.at[message]).wait()
    own_slot = iota((CAP, ny), 1) // (ny // CAP) == iota((CAP, ny), 0)
    for o in range(owners):
        for c in range(3):
            flat_slots[CAP * o:CAP * (o + 1), c * ny:(c + 1) * ny] = got_slots[o, c]
        flat_choice[CAP * o:CAP * (o + 1), :] = jnp.where(own_slot, got_choice[o], 0.0)
    picked = flat_choice[...]
    spread = lax.dot_general(
        picked, flat_slots[...], (((0,), (0,)), ((), ())), precision=HIGHEST, preferred_element_type=F32
    )
    depth_places = ny // CAP
    tiles = []
    for c in range(3):
        placed = spread[0:depth_places, c * ny:(c + 1) * ny]
        for j in range(1, CAP):
            placed = placed + spread[j * depth_places:(j + 1) * depth_places, c * ny:(c + 1) * ny]
        tiles.append(placed)
    tile = jnp.concatenate(tiles, axis=0)
    sub = lax.rem(iota(tile.shape, 0), 8)
    chunk = iota(tile.shape, 1) // PATCH_Y
    for bit in (1, 2, 4):
        row_set, chunk_set = (sub // bit) % 2 == 1, (chunk // bit) % 2 == 1
        from_below = roll(roll(tile, -bit, 0), bit * PATCH_Y, 1)
        from_above = roll(roll(tile, bit, 0), -bit * PATCH_Y, 1)
        tile = jnp.where(row_set == chunk_set, tile, jnp.where(row_set, from_above, from_below))
    surf[...] = tile.reshape(3, nx, ny)
    turned = jnp.concatenate([tile, jnp.zeros((ny - 3 * nx, ny), F32)], axis=0).T
    border[0] = turned[0:8]
    border[1] = turned[ny - 8:ny]

    swap = remote(surf, surf_other, 6, at(gx, gy, other))
    swap.start()
    first, last = pl.ds(0, 8), pl.ds(nx - 8, 8)
    ways = (
        (surf.at[:, first, :], halo_x, 0, x_down, gy),
        (surf.at[:, last, :], halo_x, 1, x_up, gy),
        (border.at[0], halo_y, 0, gx, y_down),
        (border.at[1], halo_y, 1, gx, y_up),
        (border.at[0], halo_y, 2, x_down, y_down),
        (border.at[1], halo_y, 3, x_down, y_up),
        (border.at[0], halo_y, 4, x_up, y_down),
        (border.at[1], halo_y, 5, x_up, y_up),
    )
    count = len(ways)
    started = []
    for k in reversed(range(count)):
        source, target, place, x, y = ways[k]
        for i, z in enumerate((gz, other)):
            copy = remote(source, target.at[gz, place], 7 + i * count + k, at(x, y, z), 7 + gz * count + k)
            copy.start()
            started.append(copy)
    swap.wait_recv()
    for k, (source, target, place, x, y) in enumerate(ways):
        for i in range(2):
            remote(source, target.at[i, place], 7 + i * count + k, at(x, y, gz)).wait_recv()
    sent = sent + [swap] + started
    mask_tall = domain(tall)
    mask = domain(rows)
    low_rows = iota((8, lanes), 0) < 4

    def packed(values):
        return jnp.concatenate(
            [values[0:nx], jnp.where(low_rows, values[nx:nx + 8], values[nx + 8:nx + 16])], axis=0
        )

    blank = jnp.zeros((ny - 16, ny), F32)

    def columns_of(place):
        low_side, high_side = halo_y[0, place] + halo_y[1, place], halo_y[0, place + 1] + halo_y[1, place + 1]
        return jnp.concatenate([low_side, blank, high_side], axis=0).T[0:3 * nx].reshape(3, nx, ny)

    near, upper, lower = columns_of(0), columns_of(2), columns_of(4)
    around = []
    for c in range(3):
        main = jnp.concatenate(
            [surf[c] + surf_other[c], halo_x[0, 0, c] + halo_x[1, 0, c], halo_x[0, 1, c] + halo_x[1, 1, c]], axis=0
        )
        side = jnp.concatenate([near[c], upper[c, 0:8], lower[c, nx - 8:nx]], axis=0)
        around.append(mask_tall * jnp.concatenate([main, side], axis=1))
    flux = mask_tall * (
        0.5 * ((ahead(around[0], 0) - behind(around[0], 0)) + (ahead(around[1], 1) - behind(around[1], 1)))
    )
    for c in range(3):
        s = around[c]
        beside_xy = (ahead(s, 0) + behind(s, 0)) + (ahead(s, 1) + behind(s, 1))
        fields[c] = packed(s)
        if c < 2:
            drop = 0.125 * beside_xy + (1.0 / 32.0) * (ahead(flux, c) - behind(flux, c))
            fields[3 + c] = mask * packed(drop)
            fields[6 + c] = mask * packed((1.0 / 32.0) * (ahead(around[2], c) - behind(around[2], c)))
        else:
            fields[3 + c] = mask * packed(0.125 * beside_xy)
    fields[8] = packed(flux)

    layers.wait_recv()
    sent = sent + [layers]

    def first_layer(i, carry):
        z = (nz - 4) * gz + i
        value = [table[k, z] for k in range(5)]
        own = coef[z] * value[0] - value[1]
        for c in range(2):
            w1[c, z + 1] = mask * (fields[c] * own) - value[0] * fields[3 + c] - value[2] * fields[6 + c]
        w1[2, z + 1] = mask * (fields[2] * (own - value[4])) - value[0] * fields[5] - value[3] * fields[8]
        return carry

    pairwise(0, nz + 4, first_layer)

    def spread_of(source, start, amount):
        def layer(i, carry):
            z = start + i
            x, y = source[0, z + 1], source[1, z + 1]
            div[z + 1] = mask * (
                ((ahead(x, 0) - behind(x, 0)) + (ahead(y, 1) - behind(y, 1)))
                + (source[2, z + 2] - source[2, z])
            )
            return carry

        pairwise(0, amount, layer)

    spread_of(w1, (nz - 3) * gz, nz + 3)

    def second_layer(i, carry):
        z = (nz - 2) * gz + i
        own = coef[z]
        here = div[z + 1]
        for c in range(3):
            v = w1[c, z + 1]
            total = (ahead(v, 0) + behind(v, 0)) + (ahead(v, 1) + behind(v, 1))
            total = total + (w1[c, z + 2] + w1[c, z])
            slope = (ahead(here, c) - behind(here, c)) if c < 2 else (div[z + 2] - div[z])
            w2[c, z + 1] = mask * (own * v - 0.125 * total - (1.0 / 64.0) * slope)
        return carry

    pairwise(0, nz + 2, second_layer)

    def folded(values):
        total = values[0:8]
        for k in range(8, nx, 8):
            total = total + values[k:k + 8]
        return total

    def gather_moments(i, sums):
        z = nz * gz + i
        own = coef[z, 0:nx, 0:ny]
        d_now = table[0, z, :, 0:ny]
        terms = [None] * MOMENTS
        here = w2[2, z + 2, 0:nx, 0:ny] - w2[2, z, 0:nx, 0:ny]
        for c in range(3):
            v = w2[c, z + 1, 0:nx, 0:ny]
            vx, vy = w2[c, z + 1, :, 0:ny], w2[c, z + 1, 0:nx, :]
            next_x, next_y = ahead(vx, 0)[0:nx], ahead(vy, 1)[:, 0:ny]
            total = (next_x + next_y) + w2[c, z + 2, 0:nx, 0:ny]
            if c == 0:
                here = here + (next_x - behind(vx, 0)[0:nx])
            elif c == 1:
                here = here + (next_y - behind(vy, 1)[:, 0:ny])
            zeroth = d_now * fields[c, 0:nx, 0:ny]
            one = w1[c, z + 1, 0:nx, 0:ny]
            for k, term in enumerate(
                (zeroth * zeroth, zeroth * one, one * one, one * v, v * v, v * (own * v - 0.25 * total))
            ):
                terms[k] = term if terms[k] is None else terms[k] + term
        terms[MOMENTS - 1] = terms[MOMENTS - 1] + (1.0 / 64.0) * (here * here)
        return tuple(s + folded(t) for s, t in zip(sums, terms))

    sums = lax.fori_loop(
        0, nz // 2, lambda k, sums: gather_moments(2 * k + 1, gather_moments(2 * k, sums)),
        tuple(jnp.zeros((8, ny), F32) for _ in range(MOMENTS)),
    )

    def third_layer(i, carry):
        z = nz * gz + i
        own = coef[z, 0:nx, 0:ny]
        here_x, here_y = div[z + 1, :, 0:ny], div[z + 1, 0:nx, :]
        for c in range(3):
            v = w2[c, z + 1, 0:nx, 0:ny]
            vx, vy = w2[c, z + 1, :, 0:ny], w2[c, z + 1, 0:nx, :]
            total = (ahead(vx, 0) + behind(vx, 0))[0:nx] + (ahead(vy, 1) + behind(vy, 1))[:, 0:ny]
            total = total + (w2[c, z + 2, 0:nx, 0:ny] + w2[c, z, 0:nx, 0:ny])
            if c == 0:
                slope = (ahead(here_x, 0) - behind(here_x, 0))[0:nx]
            elif c == 1:
                slope = (ahead(here_y, 1) - behind(here_y, 1))[:, 0:ny]
            else:
                slope = div[z + 2, 0:nx, 0:ny] - div[z, 0:nx, 0:ny]
            res_ref[c, i] = own * v - 0.125 * total - (1.0 / 64.0) * slope
        return carry

    early_layers = nz // 4

    lane = iota((1, ny), 1)
    message = jnp.where(lane == MOMENTS, mass, 0.0) + jnp.where(lane == MOMENTS + 1, weight, 0.0)
    for k in range(MOMENTS):
        amount = jnp.sum(jnp.sum(sums[k], axis=0, keepdims=True), axis=1, keepdims=True)
        message = message + jnp.where(lane == k, amount, 0.0)
    row_out[0] = message
    slot = gy * 2 + gz
    row_in[slot] = message
    base = 7 + 2 * count
    started = []
    for k, (y, z) in enumerate(peers):
        copy = remote(row_out.at[0], row_in.at[slot], base + k, at(gx, y, z))
        copy.start()
        started.append(copy)
    spread_of(w2, (nz - 1) * gz, nz + 1)
    pairwise(0, early_layers, third_layer)
    for copy in started:
        copy.wait_recv()
    sent = sent + started
    message = row_in[0]
    for k in range(1, 2 * ngy):
        message = message + row_in[k]
    row_out[1] = message
    ring_in[gx] = message
    first_index = base + len(peers)
    started = []
    for k in sorted(range(1, ngx), key=lambda k: -min(k, ngx - k)):
        copy = remote(row_out.at[1], ring_in.at[gx], first_index + k - 1, at(wrap(gx + k, ngx), gy, gz))
        copy.start()
        started.append(copy)
    pairwise(early_layers, nz, third_layer)
    for copy in started:
        copy.wait_recv()
    sent = sent + started
    message = ring_in[0]
    for k in range(1, ngx):
        message = message + ring_in[k]
    parts = [jnp.sum(jnp.where(lane == k, message, 0.0), axis=1, keepdims=True) for k in range(MOMENTS + 2)]

    scale = lax.rsqrt(parts[MOMENTS] / (EPOCHS * parts[MOMENTS + 1]) + EPS) * (1.0 / PRE)
    iterate, residual = conjugate(parts[0:MOMENTS])
    iterate = [scale * value for value in iterate]
    residual = [scale * value for value in residual]

    def finish(i, carry):
        z = nz * gz + i
        d_now = table[0, z, :, 0:ny]
        for c in range(3):
            zeroth = d_now * fields[c, 0:nx, 0:ny]
            one, two = w1[c, z + 1, 0:nx, 0:ny], w2[c, z + 1, 0:nx, 0:ny]
            third = res_ref[c, i]
            adj_ref[c, i] = iterate[0] * zeroth + iterate[1] * one + iterate[2] * two
            res_ref[c, i] = residual[0] * zeroth + residual[1] * one + residual[2] * two + residual[3] * third
        return carry

    pairwise(0, nz, finish)
    for copy in sent:
        copy.wait_send()
    for message, buffer in enumerate((slots_ref, choice_ref)):
        part = buffer.at[pl.ds(0, owners - 1)]
        pltpu.make_async_copy(part, part, send_a2a.at[message]).wait()


def per_device(
    observed,
    predicted,
    coherence_mask,
    block_count,
    block_owner,
    block_matrix_choice,
    block_patch,
    look_vector,
    interp_weights,
    depth_kernel,
    stiffness,
):
    blocks, epochs, pixels = observed.shape
    cells = PATCH_X * PATCH_Y
    ngx, ngy = lax.axis_size("gx"), lax.axis_size("gy")
    owners = ngx * ngy
    nz, nx, ny = stiffness.shape

    rows, lanes = nx + 8, 2 * ny
    out = pltpu.VMEM((3, nz, nx, ny), F32)
    vmem = pl.BlockSpec(memory_space=pltpu.VMEM)
    far = pl.BlockSpec(memory_space=pltpu.HBM)
    copies = 23 + (2 * ngy - 1) + (ngx - 1)
    return pl.pallas_call(
        kernel,
        out_shape=(out, out),
        in_specs=[far] * 11,
        out_specs=(vmem, vmem),
        scratch_shapes=[
            pltpu.VMEM(observed.shape, F32),
            pltpu.VMEM(predicted.shape, F32),
            pltpu.VMEM(coherence_mask.shape, jnp.int32),
            pltpu.SMEM((blocks,), jnp.int32),
            pltpu.SMEM((blocks,), jnp.int32),
            pltpu.SMEM((blocks,), jnp.int32),
            pltpu.SMEM((blocks,), jnp.int32),
            pltpu.SMEM(look_vector.shape, F32),
            pltpu.VMEM(interp_weights.shape, interp_weights.dtype),
            pltpu.SMEM((nz,), F32),
            pltpu.VMEM(stiffness.shape, F32),
            pltpu.VMEM((4, blocks, ny), jnp.int32),
            pltpu.VMEM((blocks, pixels), F32),
            pltpu.VMEM((epochs * blocks, pixels), F32),
            pltpu.VMEM((3 * blocks, pixels), F32),
            pltpu.VMEM((owners, 3, CAP, cells), F32),
            pltpu.VMEM((owners, 1, cells), F32),
            pltpu.VMEM((owners, 3, CAP, cells), F32),
            pltpu.VMEM((owners, 1, cells), F32),
            pltpu.VMEM((owners * CAP, 3 * cells), F32),
            pltpu.VMEM((owners * CAP, cells), F32),
            pltpu.VMEM((3, nx, ny), F32),
            pltpu.VMEM((3, nx, ny), F32),
            pltpu.VMEM((2, 8, ny), F32),
            pltpu.VMEM((2, 2, 3, 8, ny), F32),
            pltpu.VMEM((2, 6, 8, ny), F32),
            pltpu.VMEM((2, nz, 4, ny), F32),
            pltpu.VMEM((2, nz, 4, ny), F32),
            pltpu.VMEM((nz, rows, ny), F32),
            pltpu.VMEM((2, 8, nz * rows), F32),
            pltpu.VMEM((2, 8, nz * rows), F32),
            pltpu.VMEM((2 * nz, rows, lanes), F32),
            pltpu.VMEM((2 * nz + 16, lanes), F32),
            pltpu.VMEM((5, 2 * nz, 1, lanes), F32),
            pltpu.VMEM((9, rows, lanes), F32),
            pltpu.VMEM((3, 2 * nz + 2, rows, lanes), F32),
            pltpu.VMEM((3, 2 * nz + 2, rows, lanes), F32),
            pltpu.VMEM((2 * nz + 2, rows, lanes), F32),
            pltpu.VMEM((2, 1, ny), F32),
            pltpu.VMEM((2 * ngy, 1, ny), F32),
            pltpu.VMEM((ngx, 1, ny), F32),
            pltpu.SemaphoreType.DMA((2,)),
            pltpu.SemaphoreType.DMA((2,)),
            pltpu.SemaphoreType.DMA((copies,)),
            pltpu.SemaphoreType.DMA((copies,)),
            pltpu.SemaphoreType.DMA((11,)),
        ],
        compiler_params=pltpu.CompilerParams(
            collective_id=0, has_side_effects=True, vmem_limit_bytes=60000000
        ),
    )(
        observed, predicted, coherence_mask, block_count, block_owner[:, 0], block_matrix_choice, block_patch,
        look_vector, interp_weights, depth_kernel, stiffness,
    )


def solution(mesh):
    in_specs = (
        P(("grp", "gx", "gy", "gz"), None, None),
        P(("grp", "gx", "gy", "gz"), None, None),
        P(("grp", "gx", "gy", "gz"), None),
        P(("grp", "gx", "gy", "gz")),
        P(("grp", "gx", "gy", "gz"), None),
        P(("grp", "gx", "gy", "gz")),
        P(("grp", "gx", "gy", "gz")),
        P(),
        P(),
        P(("grp", "gz")),
        P(("grp", "gz"), "gx", "gy"),
    )
    out_specs = (P(None, ("grp", "gz"), "gx", "gy"), P(None, ("grp", "gz"), "gx", "gy"))
    return jax.shard_map(
        per_device, mesh=mesh, in_specs=in_specs, out_specs=out_specs, check_vma=False
    )
```
